32 devices in a mesh: dp: 1 (over z), tp: 4 (over y), ep: 8 (over x, core).
Axes of the slice: x: 4, y: 4, z: 1, core: 2. Of those that a mesh axis runs over, the one named last changes fastest.
The devices are a block of a 4x4x8 slice.
Arguments:
- hidden_in: bfloat16 [8, 1024, 4096], P(('dp', 'ep'))
- expert_ids: int32 [8, 1024, 4], P(('dp', 'ep'))
- slot_ids: int32 [8, 1024, 4], P(('dp', 'ep'))
- attn_gain: bfloat16 [4096], replicated
- w_query: bfloat16 [4096, 32, 128], P(None, 'tp')
- w_key: bfloat16 [4096, 32, 128], P(None, 'tp')
- w_value: bfloat16 [4096, 32, 128], P(None, 'tp')
- w_out: bfloat16 [32, 128, 4096], P('tp')
- ffn_gain: bfloat16 [4096], replicated
- w_gate: bfloat16 [4096, 11008], P(None, 'tp')
- w_up: bfloat16 [4096, 11008], P(None, 'tp')
- w_down: bfloat16 [11008, 4096], P('tp')
- moe_gain: bfloat16 [4096], replicated
- w_router: bfloat16 [4096, 16], replicated
- exp_gate: bfloat16 [16, 4096, 688], P('ep')
- exp_up: bfloat16 [16, 4096, 688], P('ep')
- exp_down: bfloat16 [16, 688, 4096], P('ep')
Outputs:
- output: bfloat16 [8, 1024, 4096], P(('dp', 'ep'))
All inputs are finite; a program needn't handle non-finite values.
Results may differ from the reference program's by a relative error of at most 0.00899844.
Values are sent between devices in bfloat16 or wider.
A program may use at most 768 MiB of HBM per device.

```python
import math
import jax
import jax.numpy as jnp
from jax import lax

D = 4096
HEADS = 32
HEAD = 128
FF = 11008
EXPERTS = 16
TOP = 4
FE = 688
SEQ = 1024
SEQS_DEV = 1
GROUP = 8
TOK_DEV = SEQS_DEV * SEQ
TOKENS = GROUP * TOK_DEV
MEAN_LOAD = TOK_DEV * TOP // EXPERTS
CAP = 3 * MEAN_LOAD // 2
EPS = 1e-6
ROPE_BASE = 10000.0


def rms_norm(x_val, gain):
    x_f32 = x_val.astype(jnp.float32)
    inv_rms = lax.rsqrt(jnp.mean(x_f32 * x_f32, axis=-1, keepdims=True) + EPS)
    return (x_f32 * inv_rms * gain.astype(jnp.float32)).astype(jnp.bfloat16)


def rope_tables():
    inv_freq = ROPE_BASE ** (-jnp.arange(HEAD // 2, dtype=jnp.float32) * (2.0 / HEAD))
    angle = jnp.arange(SEQ, dtype=jnp.float32)[:, None] * inv_freq[None, :]
    return jnp.cos(angle), jnp.sin(angle)


def apply_rope(x_val, cos_tab, sin_tab):
    half_dim = x_val.shape[-1] // 2
    lower = x_val[..., :half_dim]
    upper = x_val[..., half_dim:]
    cos_b = cos_tab[:, None, :]
    sin_b = sin_tab[:, None, :]
    return jnp.concatenate([lower * cos_b - upper * sin_b, upper * cos_b + lower * sin_b], axis=-1)


def dense_sequence(h_seq, attn_gain, w_query, w_key, w_value, w_out, ffn_gain, w_gate, w_up, w_down):
    width = HEADS * HEAD
    cos_tab, sin_tab = rope_tables()
    x_norm = rms_norm(h_seq, attn_gain)
    q_f32 = jnp.dot(x_norm, w_query.reshape(D, width), preferred_element_type=jnp.float32).reshape(SEQ, HEADS, HEAD)
    k_f32 = jnp.dot(x_norm, w_key.reshape(D, width), preferred_element_type=jnp.float32).reshape(SEQ, HEADS, HEAD)
    query = apply_rope(q_f32, cos_tab, sin_tab).astype(jnp.bfloat16)
    key_proj = apply_rope(k_f32, cos_tab, sin_tab).astype(jnp.bfloat16)
    value_proj = jnp.dot(x_norm, w_value.reshape(D, width), preferred_element_type=jnp.float32).astype(jnp.bfloat16).reshape(SEQ, HEADS, HEAD)
    scores = jnp.einsum('qhe,khe->hqk', query.astype(jnp.float32), key_proj.astype(jnp.float32)) * HEAD ** -0.5
    causal = jnp.arange(SEQ)[:, None] >= jnp.arange(SEQ)[None, :]
    attn_prob = jax.nn.softmax(jnp.where(causal[None], scores, -1e30), axis=-1).astype(jnp.bfloat16)
    context = jnp.einsum('hqk,khe->qhe', attn_prob.astype(jnp.float32), value_proj.astype(jnp.float32)).astype(jnp.bfloat16)
    attn_out = jnp.dot(context.reshape(SEQ, width), w_out.reshape(width, D), preferred_element_type=jnp.float32)
    after_attn = (h_seq.astype(jnp.float32) + attn_out).astype(jnp.bfloat16)
    f_norm = rms_norm(after_attn, ffn_gain)
    gate_pre = jnp.dot(f_norm, w_gate, preferred_element_type=jnp.float32)
    up_pre = jnp.dot(f_norm, w_up, preferred_element_type=jnp.float32)
    hidden_act = (jax.nn.silu(gate_pre) * up_pre).astype(jnp.bfloat16)
    ffn_out = jnp.dot(hidden_act, w_down, preferred_element_type=jnp.float32)
    return after_attn.astype(jnp.float32) + ffn_out


def source_routing(key):
    key_shift, key_label, key_token = jax.random.split(key, 3)
    shift = jax.random.randint(key_shift, (EXPERTS // 2,), 0, MEAN_LOAD // 2 + 1)
    shift = shift.at[0].set(MEAN_LOAD // 2)
    paired = jnp.stack([MEAN_LOAD + shift, MEAN_LOAD - shift], axis=1).reshape(EXPERTS)
    counts = paired[jax.random.permutation(key_label, EXPERTS)]
    ends = jnp.cumsum(counts)
    starts = ends - counts
    position = jnp.arange(TOK_DEV * TOP, dtype=jnp.int32)
    owner = jnp.sum((position[:, None] >= ends[None, :]).astype(jnp.int32), axis=1)
    slot_row = position - starts[owner]
    column = jax.random.permutation(key_token, TOK_DEV)
    expert_col = owner.reshape(TOP, TOK_DEV)[:, column].T
    slot_col = slot_row.reshape(TOP, TOK_DEV)[:, column].T
    return expert_col.astype(jnp.int32), slot_col.astype(jnp.int32)


def draw_routing(key):
    expert_all, slot_all = lax.map(source_routing, jax.random.split(key, GROUP))
    out_shape = (GROUP * SEQS_DEV, SEQ, TOP)
    return expert_all.reshape(out_shape), slot_all.reshape(out_shape)


def normal_weight(key, shape, scale):
    return (jax.random.normal(key, shape, jnp.float32) * scale).astype(jnp.bfloat16)


def gain_vector(key):
    return (1.0 + 0.3 * jax.random.normal(key, (D,), jnp.float32)).astype(jnp.bfloat16)


def setup_inputs(seed: int = 0, part: int = 0) -> dict:
    root = jax.random.key(seed)
    part_key = jax.random.fold_in(root, part)
    key_hidden, key_route = jax.random.split(part_key, 2)
    weight_keys = jax.random.split(root, 14)
    width = HEADS * HEAD
    query_scale = math.sqrt(math.log(SEQ) / 2.0) * D ** -0.5
    expert_ids, slot_ids = draw_routing(key_route)
    return {
        'hidden_in': normal_weight(key_hidden, (GROUP * SEQS_DEV, SEQ, D), 1.0),
        'expert_ids': expert_ids,
        'slot_ids': slot_ids,
        'attn_gain': gain_vector(weight_keys[0]),
        'w_query': normal_weight(weight_keys[1], (D, HEADS, HEAD), query_scale),
        'w_key': normal_weight(weight_keys[2], (D, HEADS, HEAD), D ** -0.5),
        'w_value': normal_weight(weight_keys[3], (D, HEADS, HEAD), D ** -0.5),
        'w_out': normal_weight(weight_keys[4], (HEADS, HEAD, D), 2.0 * width ** -0.5),
        'ffn_gain': gain_vector(weight_keys[5]),
        'w_gate': normal_weight(weight_keys[6], (D, FF), D ** -0.5),
        'w_up': normal_weight(weight_keys[7], (D, FF), D ** -0.5),
        'w_down': normal_weight(weight_keys[8], (FF, D), FF ** -0.5),
        'moe_gain': gain_vector(weight_keys[9]),
        'w_router': normal_weight(weight_keys[10], (D, EXPERTS), 2.0 * D ** -0.5),
        'exp_gate': normal_weight(weight_keys[11], (EXPERTS, D, FE), D ** -0.5),
        'exp_up': normal_weight(weight_keys[12], (EXPERTS, D, FE), D ** -0.5),
        'exp_down': normal_weight(weight_keys[13], (EXPERTS, FE, D), 2.0 * FE ** -0.5),
    }


def reference(hidden_in, expert_ids, slot_ids, attn_gain, w_query, w_key, w_value, w_out, ffn_gain, w_gate, w_up, w_down, moe_gain, w_router, exp_gate, exp_up, exp_down):
    tokens = hidden_in.reshape(TOKENS, D)
    route_ids = expert_ids.reshape(TOKENS, TOP)
    slots = slot_ids.reshape(TOKENS, TOP)
    u_norm = rms_norm(tokens, moe_gain)
    logits = jnp.dot(u_norm, w_router, preferred_element_type=jnp.float32)
    gates = jax.nn.softmax(jnp.take_along_axis(logits, route_ids, axis=1), axis=-1)
    token_of = jnp.broadcast_to(jnp.arange(TOKENS, dtype=jnp.int32)[:, None], (TOKENS, TOP))
    flat_pos = (((token_of // TOK_DEV) * EXPERTS + route_ids) * CAP + slots).reshape(-1)
    row_token = jnp.full((GROUP * EXPERTS * CAP,), TOKENS, jnp.int32).at[flat_pos].set(token_of.reshape(-1))
    row_gate = jnp.zeros((GROUP * EXPERTS * CAP,), jnp.float32).at[flat_pos].set(gates.reshape(-1))
    row_token = row_token.reshape(GROUP, EXPERTS, CAP).transpose(1, 0, 2).reshape(EXPERTS, GROUP * CAP)
    row_gate = row_gate.reshape(GROUP, EXPERTS, CAP).transpose(1, 0, 2).reshape(EXPERTS, GROUP * CAP)

    def expert_step(moe_acc, slab):
        rows, gate_rows, w_one, w_three, w_two = slab
        x_rows = jnp.take(u_norm, rows, axis=0, mode='fill', fill_value=0)
        gate_pre = jnp.dot(x_rows, w_one, preferred_element_type=jnp.float32)
        up_pre = jnp.dot(x_rows, w_three, preferred_element_type=jnp.float32)
        hidden_act = (jax.nn.silu(gate_pre) * up_pre).astype(jnp.bfloat16)
        expert_out = jnp.dot(hidden_act, w_two, preferred_element_type=jnp.float32).astype(jnp.bfloat16)
        return moe_acc.at[rows].add(gate_rows[:, None] * expert_out.astype(jnp.float32), mode='drop'), None

    moe_sum = lax.scan(expert_step, jnp.zeros((TOKENS, D), jnp.float32), (row_token, row_gate, exp_gate, exp_up, exp_down))[0]
    dense_out = lax.map(lambda h_seq: dense_sequence(h_seq, attn_gain, w_query, w_key, w_value, w_out, ffn_gain, w_gate, w_up, w_down), hidden_in)
    return (dense_out.reshape(TOKENS, D) + moe_sum).reshape(GROUP * SEQS_DEV, SEQ, D).astype(jnp.bfloat16)
```

```python
import jax
import jax.numpy as jnp
from jax import lax
from jax.sharding import PartitionSpec as P

EPS = 1e-6
ROPE_BASE = 10000.0
F32 = jnp.float32
BF16 = jnp.bfloat16


def rms_norm(x_val, gain):
    x_f32 = x_val.astype(F32)
    inv_rms = lax.rsqrt(jnp.mean(x_f32 * x_f32, axis=-1, keepdims=True) + EPS)
    return (x_f32 * inv_rms * gain.astype(F32)).astype(BF16)


def rope_tables(seq_len, head_dim):
    inv_freq = ROPE_BASE ** (-jnp.arange(head_dim // 2, dtype=F32) * (2.0 / head_dim))
    angle = jnp.arange(seq_len, dtype=F32)[:, None] * inv_freq[None, :]
    return jnp.cos(angle), jnp.sin(angle)


def apply_rope(x_val, cos_tab, sin_tab):
    half_dim = x_val.shape[-1] // 2
    lower = x_val[..., :half_dim]
    upper = x_val[..., half_dim:]
    cos_b = cos_tab[:, None, :]
    sin_b = sin_tab[:, None, :]
    return jnp.concatenate([lower * cos_b - upper * sin_b, upper * cos_b + lower * sin_b], axis=-1)


def attention(hidden, attn_gain, w_query, w_key, w_value):
    num_seqs, seq_len, d_model = hidden.shape
    head_dim = w_query.shape[2]
    x_norm = rms_norm(hidden, attn_gain)
    cos_tab, sin_tab = rope_tables(seq_len, head_dim)
    query = apply_rope(jnp.einsum('bsd,dhe->bshe', x_norm, w_query, preferred_element_type=F32), cos_tab, sin_tab).astype(BF16)
    key_proj = apply_rope(jnp.einsum('bsd,dhe->bshe', x_norm, w_key, preferred_element_type=F32), cos_tab, sin_tab).astype(BF16)
    value_proj = jnp.einsum('bsd,dhe->bshe', x_norm, w_value, preferred_element_type=F32).astype(BF16)
    scores = jnp.einsum('bqhe,bkhe->bhqk', query, key_proj, preferred_element_type=F32) * head_dim ** -0.5
    causal = jnp.arange(seq_len)[:, None] >= jnp.arange(seq_len)[None, :]
    attn_prob = jax.nn.softmax(jnp.where(causal, scores, -1e30), axis=-1).astype(BF16)
    context = jnp.einsum('bhqk,bkhe->bqhe', attn_prob, value_proj, preferred_element_type=F32).astype(BF16)
    return context


def moe_partial(tokens, ids, moe_gain, w_router, exp_gate, exp_up, exp_down):
    experts = w_router.shape[1]
    local = exp_gate.shape[0]
    u_norm = rms_norm(tokens, moe_gain)
    logits = jnp.dot(u_norm, w_router, preferred_element_type=F32)
    hot = ids[:, :, None] == jnp.arange(experts, dtype=jnp.int32)[None, None, :]
    picked = jnp.sum(jnp.where(hot, logits[:, None, :], 0.0), axis=-1)
    gates = jax.nn.softmax(picked, axis=-1)
    first = lax.axis_index('ep') * local
    total = None
    for k in range(local):
        mine = ids == first + k
        weight = jnp.sum(jnp.where(mine, gates, 0.0), axis=1, keepdims=True)
        chosen = jnp.any(mine, axis=1, keepdims=True)
        gate_pre = jnp.dot(u_norm, exp_gate[k], preferred_element_type=F32)
        up_pre = jnp.dot(u_norm, exp_up[k], preferred_element_type=F32)
        act = (jax.nn.silu(gate_pre) * up_pre).astype(BF16)
        y_out = jnp.dot(act, exp_down[k], preferred_element_type=F32).astype(BF16)
        term = jnp.where(chosen, weight * y_out.astype(F32), 0.0)
        total = term if total is None else total + term
    return total


def solution(mesh):
    tok_spec = P(('dp', 'ep'), None, None)
    col_spec = P(None, 'tp', None)
    exp_spec = P('ep', None, None)
    in_specs = (tok_spec, tok_spec, tok_spec, P(None), col_spec, col_spec, col_spec, P('tp', None, None), P(None), P(None, 'tp'), P(None, 'tp'), P('tp', None), P(None), P(None, None), exp_spec, exp_spec, exp_spec)
    tp = mesh.shape['tp']
    ep = mesh.shape['ep']

    def layer_local(hidden_in, expert_ids, slot_ids, attn_gain, w_query, w_key, w_value, w_out, ffn_gain, w_gate, w_up, w_down, moe_gain, w_router, exp_gate, exp_up, exp_down):
        num_seqs, seq_len, d_model = hidden_in.shape
        tokens = num_seqs * seq_len
        top_k = expert_ids.shape[2]
        heads, head_dim = w_out.shape[0], w_out.shape[1]
        quarter = tokens // tp
        t_idx = lax.axis_index('tp')
        e_idx = lax.axis_index('ep')
        flat = hidden_in.reshape(tokens, d_model)
        own = lax.dynamic_slice_in_dim(flat, t_idx * quarter, quarter, 0)
        own_ids = lax.dynamic_slice_in_dim(expert_ids.reshape(tokens, top_k), t_idx * quarter, quarter, 0)
        gathered = lax.all_gather(own, 'ep', axis=0, tiled=True)
        gathered_ids = lax.all_gather(own_ids, 'ep', axis=0, tiled=True)
        per_ep = heads // ep
        rows = lax.dynamic_slice_in_dim(w_out, e_idx * per_ep, per_ep, 0).reshape(per_ep * head_dim, d_model)
        cols = lax.all_to_all(rows, 'tp', 1, 0, tiled=True)
        w_out_cols = lax.all_gather(cols, 'ep', axis=0, tiled=True)

        context = attention(hidden_in, attn_gain, w_query, w_key, w_value)
        ctx_all = lax.all_gather(context, 'tp', axis=0, tiled=False)
        ctx_all = ctx_all.reshape(tp, tokens, ep, per_ep * head_dim)
        w_cols = w_out_cols.reshape(ep, tp, per_ep * head_dim, d_model // tp)
        o_cols = jnp.einsum('tsef,etfd->sd', ctx_all, w_cols, preferred_element_type=F32)
        width = d_model // tp
        x_cols = lax.dynamic_slice_in_dim(flat, t_idx * width, width, 1)
        a_cols = (x_cols.astype(F32) + o_cols).astype(BF16)
        after_attn = lax.all_gather(a_cols, 'tp', axis=1, tiled=True)

        part = moe_partial(gathered, gathered_ids, moe_gain, w_router, exp_gate, exp_up, exp_down)
        moe_own = lax.psum_scatter(part, 'ep', scatter_dimension=0, tiled=True)

        f_norm = rms_norm(after_attn, ffn_gain)
        gate_pre = jnp.dot(f_norm, w_gate, preferred_element_type=F32)
        up_pre = jnp.dot(f_norm, w_up, preferred_element_type=F32)
        act = (jax.nn.silu(gate_pre) * up_pre).astype(BF16)
        ffn_part = jnp.dot(act, w_down, preferred_element_type=F32)
        ffn_own = lax.psum_scatter(ffn_part, 'tp', scatter_dimension=0, tiled=True)
        a_own = lax.dynamic_slice_in_dim(after_attn, t_idx * quarter, quarter, 0)
        out_own = ((a_own.astype(F32) + ffn_own) + moe_own).astype(BF16)
        return lax.all_gather(out_own, 'tp', axis=0, tiled=True).reshape(hidden_in.shape)

    return jax.shard_map(layer_local, mesh=mesh, in_specs=in_specs, out_specs=tok_spec, check_vma=False)
```

```python
import functools
import jax
import jax.numpy as jnp
from jax import lax
from jax.experimental import pallas as pl
from jax.experimental.pallas import tpu as pltpu
from jax.sharding import PartitionSpec as P

F32 = jnp.float32
BF16 = jnp.bfloat16
EPS = 1e-6
ROPE_BASE = 10000.0
MESH = pl.DeviceIdType.MESH
NT = (((1,), (1,)), ((), ()))


def rcopy(src, dst, ssem, rsem, dev):
    return pltpu.make_async_remote_copy(src_ref=src, dst_ref=dst, send_sem=ssem, recv_sem=rsem, device_id=dev, device_id_type=MESH)


def entry_barrier(neighbours):
    barrier = pltpu.get_barrier_semaphore()
    for dev in neighbours:
        pl.semaphore_signal(barrier, inc=1, device_id=dev, device_id_type=MESH)
    pl.semaphore_wait(barrier, len(neighbours))


def norm_rows(src, dst, gain, rows, step):
    def one(r, carry):
        sl = pl.ds(pl.multiple_of(r * step, step), step)
        x = src[sl, :].astype(F32)
        inv = lax.rsqrt(jnp.mean(x * x, axis=-1, keepdims=True) + EPS)
        dst[sl, :] = (x * inv * gain[...].astype(F32)).astype(BF16)
        return carry
    lax.fori_loop(0, rows // step, one, 0)


def ffn_body(fb, a_ref, wg, wu, wd, gain, m_ref, out_ref,
             a_buf, n2, h, wbuf, dbuf, p1, p2, yrecv, xrecv, mbuf,
             asem, wsem, dsem, msem, osem, ys, yr, xs, xr, gs, gr, fs, fr):
    t = lax.axis_index('tp')
    e = lax.axis_index('ep')
    big = lax.rem(e, 2)
    xc = e // 2
    q = a_buf.shape[1]
    d_model = a_buf.shape[2]
    f_loc = wg.shape[0]
    cw = d_model // 8
    hw = cw // 2
    nf = f_loc // fb
    tail = f_loc - nf * fb
    yright, yleft = {'tp': lax.rem(t + 1, 4)}, {'tp': lax.rem(t + 3, 4)}
    xright, xleft = {'ep': lax.rem(xc + 1, 4) * 2 + big}, {'ep': lax.rem(xc + 3, 4) * 2 + big}

    def cols(cb):
        return pl.ds(pl.multiple_of(cb * cw, cw), cw)

    def chunk(c):
        return lax.rem(c + 8, 4)

    def rows(c):
        return pl.ds(pl.multiple_of(chunk(c) * q, q), q)

    def a_load(c, slot):
        return pltpu.make_async_copy(a_ref.at[rows(c)], a_buf.at[slot], asem.at[slot])

    def w_load(i, slot, size):
        sl = pl.ds(pl.multiple_of(i * fb, fb), size)
        return (pltpu.make_async_copy(wg.at[sl], wbuf.at[slot, 0, pl.ds(0, size)], wsem.at[slot, 0]),
                pltpu.make_async_copy(wu.at[sl], wbuf.at[slot, 1, pl.ds(0, size)], wsem.at[slot, 1]))

    def w_start(i):
        slot = lax.rem(i, 2)

        @pl.when(i < nf)
        def _():
            for c in w_load(i, slot, fb):
                c.start()

        @pl.when(i == nf)
        def _():
            for c in w_load(nf, slot, tail):
                c.start()

    def col_of(j):
        return lax.rem(j, 2) * 4 + j // 2

    def d_load(jj):
        slot = lax.rem(jj, 2)
        start = pl.multiple_of(col_of(jj // 2) * cw + slot * hw, hw)
        return pltpu.make_async_copy(wd.at[:, pl.ds(start, hw)], dbuf.at[slot], dsem.at[slot])

    def m_load(k):
        s, j = k // 8 + 1, lax.rem(k, 8)
        side = lax.rem(j, 2)
        c = lax.rem(xc + (2 * side - 1) * (1 + s) + 8, 4)
        slot = lax.rem(k, 2)
        return pltpu.make_async_copy(m_ref.at[c, :, cols(col_of(j))], mbuf.at[slot], msem.at[slot])

    def send(buf, ssem, rsem, src, right, left, side, step, i):
        @pl.when(side == 0)
        def _():
            rcopy(src, buf.at[0, step, i], ssem.at[0, step, i], rsem.at[0, step, i], right).start()

        @pl.when(side == 1)
        def _():
            rcopy(src, buf.at[1, step, i], ssem.at[1, step, i], rsem.at[1, step, i], left).start()

    def ysend(src, side, step, i):
        send(yrecv, ys, yr, src, yright, yleft, side, step, i)

    def xsend(src, side, step, i):
        send(xrecv, xs, xr, src, xright, xleft, side, step, i)

    def arrived(buf, ssem, rsem, side, step, i, dev):
        rcopy(buf.at[side, step, i], buf.at[side, step, i], ssem.at[side, step, i], rsem.at[side, step, i], dev).wait_recv()

    def sent(buf, ssem, rsem, side, step, i, dev):
        rcopy(buf.at[side, step, i], buf.at[side, step, i], ssem.at[side, step, i], rsem.at[side, step, i], dev).wait_send()

    def xserve(k):
        s, j = k // 8, lax.rem(k, 8)
        side, i = lax.rem(j, 2), j // 2
        m_load(k + 1).start()
        m_load(k).wait()
        arrived(xrecv, xs, xr, side, s, i, xright)
        xrecv[side, s, i] = xrecv[side, s, i] + mbuf[lax.rem(k, 2)]
        xsend(xrecv.at[side, s, i], side, s + 1, i)

    def gate_up(serve):
        def block(i, size):
            slot = lax.rem(i, 2)
            for c in w_load(i, slot, size):
                c.wait()
            g = lax.dot_general(n2[...], wbuf[slot, 0, pl.ds(0, size)], NT, preferred_element_type=F32)
            u = lax.dot_general(n2[...], wbuf[slot, 1, pl.ds(0, size)], NT, preferred_element_type=F32)
            h[:, pl.ds(pl.multiple_of(i * fb, fb), size)] = (jax.nn.silu(g) * u).astype(BF16)

        def one(i, carry):
            block(i, fb)
            w_start(i + 2)
            serve(i)
            return carry
        lax.fori_loop(0, nf, one, 0)
        block(nf, tail)

    def down(use):
        def one(jj, carry):
            sub = lax.rem(jj, 2)
            d_load(jj).wait()
            r = jnp.dot(h[...], dbuf[sub], preferred_element_type=F32)

            @pl.when(jj + 2 < 16)
            def _():
                d_load(jj + 2).start()
            use(jj // 2, sub, pl.ds(pl.multiple_of(sub * hw, hw), hw), r)
            return carry
        lax.fori_loop(0, 16, one, 0)

    a_load(t - 1, 0).start()
    a_load(t + 1, 1).start()
    w_start(0)
    w_start(1)
    entry_barrier((yright, yleft, xright, xleft))

    def x_first(i, carry):
        xsend(m_ref.at[chunk(xc - 1), :, cols(i)], 0, 0, i)
        xsend(m_ref.at[chunk(xc + 1), :, cols(4 + i)], 1, 0, i)
        return carry
    lax.fori_loop(0, 4, x_first, 0)
    d_load(0).start()
    d_load(1).start()
    m_load(0).start()

    for slot in range(2):
        a_load(t, slot).wait()
        norm_rows(a_buf.at[slot], n2.at[pl.ds(slot * q, q)], gain, q, 16)
    a_load(t + 2, 0).start()
    a_load(t, 1).start()
    gate_up(lambda i: None)
    w_start(0)
    w_start(1)

    def use1(j, sub, part, r):
        p1[col_of(j), :, part] = r
        side, i = lax.rem(j, 2), j // 2

        @pl.when(sub == 1)
        def _():
            ysend(p1.at[col_of(j), pl.ds(pl.multiple_of(side * q, q), q)], side, 0, i)
    down(use1)
    d_load(0).start()
    d_load(1).start()

    for slot in range(2):
        a_load(t, slot).wait()
        norm_rows(a_buf.at[slot], n2.at[pl.ds(slot * q, q)], gain, q, 16)

    def serve2(i):
        @pl.when(i < 8)
        def _():
            xserve(i)
    gate_up(serve2)
    for k in range(min(nf, 8), 8):
        xserve(k)

    def use2(j, sub, part, r):
        side, i = lax.rem(j, 2), j // 2
        p2[col_of(j), :, part] = r[q:]

        @pl.when(sub == 0)
        def _():
            arrived(yrecv, ys, yr, side, 0, i, yright)
        yrecv[side, 0, i, :, part] = yrecv[side, 0, i, :, part] + r[:q]

        @pl.when(sub == 1)
        def _():
            ysend(yrecv.at[side, 0, i], side, 1, i)
    down(use2)

    def third(j, carry):
        side, i = lax.rem(j, 2), j // 2
        xserve(8 + j)
        arrived(yrecv, ys, yr, side, 1, i, yright)
        yrecv[side, 1, i] = yrecv[side, 1, i] + p1[col_of(j), pl.ds(pl.multiple_of((1 - side) * q, q), q)]
        ysend(yrecv.at[side, 1, i], side, 2, i)
        return carry
    lax.fori_loop(0, 8, third, 0)

    def out_local(cb):
        return pltpu.make_async_copy(n2.at[pl.ds(0, q), cols(cb)], out_ref.at[rows(t), cols(cb)], osem.at[cb])

    def gather(cb, side, dev):
        return rcopy(n2.at[pl.ds(0, q), cols(cb)], out_ref.at[rows(t), cols(cb)], gs.at[side, cb], gr.at[side, cb], dev)

    def last(j, carry):
        side, i = lax.rem(j, 2), j // 2
        cb = col_of(j)
        k = 16 + j

        @pl.when(j + 1 < 8)
        def _():
            m_load(k + 1).start()
        m_load(k).wait()
        arrived(xrecv, xs, xr, side, 2, i, xright)
        arrived(yrecv, ys, yr, side, 2, i, yright)
        b_val = a_buf[1, :, cols(cb)].astype(F32) + (yrecv[side, 2, i] + p2[cb])
        n2[pl.ds(0, q), cols(cb)] = (b_val + (xrecv[side, 2, i] + mbuf[lax.rem(k, 2)])).astype(BF16)
        out_local(cb).start()
        gather(cb, 0, yright).start()
        gather(cb, 1, yleft).start()
        return carry
    lax.fori_loop(0, 8, last, 0)

    half = q // 2

    def half_rows(c, which):
        return pl.ds(pl.multiple_of(chunk(c) * q + which * half, half), half)

    def forward(c, which, cb, dev):
        ref = out_ref.at[half_rows(c, which), cols(cb)]
        return rcopy(ref, ref, fs.at[which, cb], fr.at[which, cb], dev)

    def pass_on(j, carry):
        cb = col_of(j)
        gather(cb, 0, yright).wait_recv()
        forward(t - 1, 0, cb, yright).start()
        gather(cb, 1, yleft).wait_recv()
        forward(t + 1, 1, cb, yleft).start()
        return carry
    lax.fori_loop(0, 8, pass_on, 0)

    def finish(j, carry):
        cb = col_of(j)
        out_local(cb).wait()
        for which in range(2):
            gather(cb, which, yright).wait_send()
            forward(t, which, cb, yright).wait_send()
            forward(t, which, cb, yright).wait_recv()
        return carry
    lax.fori_loop(0, 8, finish, 0)

    def drain(k, carry):
        step, j = k // 8, lax.rem(k, 8)
        sent(yrecv, ys, yr, lax.rem(j, 2), step, j // 2, yright)
        sent(xrecv, xs, xr, lax.rem(j, 2), step, j // 2, yright)
        return carry
    lax.fori_loop(0, 24, drain, 0)


def ffn_call(after_attn, wg_t, wu_t, w_down, gain, m_part, fb=256):
    tokens, d_model = after_attn.shape
    f_loc = wg_t.shape[0]
    q = tokens // 4
    cw = d_model // 8
    hbm = pl.BlockSpec(memory_space=pl.ANY)
    vmem = pl.BlockSpec(memory_space=pltpu.VMEM)
    dma = pltpu.SemaphoreType.DMA
    flops = 2 * tokens * d_model * f_loc * 3
    return pl.pallas_call(
        functools.partial(ffn_body, fb),
        out_shape=jax.ShapeDtypeStruct((tokens, d_model), BF16),
        in_specs=[hbm, hbm, hbm, hbm, vmem, hbm],
        out_specs=hbm,
        scratch_shapes=[
            pltpu.VMEM((2, q, d_model), BF16),
            pltpu.VMEM((2 * q, d_model), BF16),
            pltpu.VMEM((2 * q, f_loc), BF16),
            pltpu.VMEM((2, 2, fb, d_model), BF16),
            pltpu.VMEM((2, f_loc, cw // 2), BF16),
            pltpu.VMEM((8, 2 * q, cw), F32),
            pltpu.VMEM((8, q, cw), F32),
            pltpu.VMEM((2, 3, 4, q, cw), F32),
            pltpu.VMEM((2, 3, 4, q, cw), F32),
            pltpu.VMEM((2, q, cw), F32),
            dma((2,)), dma((2, 2)), dma((2,)), dma((2,)), dma((8,)),
            dma((2, 3, 4)), dma((2, 3, 4)), dma((2, 3, 4)), dma((2, 3, 4)),
            dma((2, 8)), dma((2, 8)), dma((2, 8)), dma((2, 8)),
        ],
        compiler_params=pltpu.CompilerParams(collective_id=2, has_side_effects=True, vmem_limit_bytes=67043328),
        cost_estimate=pl.CostEstimate(flops=flops, bytes_accessed=4 * tokens * d_model + 12 * f_loc * d_model, transcendentals=tokens * f_loc),
        name='ffn_ring',
    )(after_attn, wg_t, wu_t, w_down, gain, m_part)


def rms_norm(x_val, gain):
    x_f32 = x_val.astype(F32)
    inv_rms = lax.rsqrt(jnp.mean(x_f32 * x_f32, axis=-1, keepdims=True) + EPS)
    return (x_f32 * inv_rms * gain.astype(F32)).astype(BF16)


def rope_tables(seq_len, head_dim):
    inv_freq = ROPE_BASE ** (-jnp.arange(head_dim // 2, dtype=F32) * (2.0 / head_dim))
    angle = jnp.arange(seq_len, dtype=F32)[:, None] * inv_freq[None, :]
    return jnp.cos(angle), jnp.sin(angle)


def apply_rope(x_val, cos_tab, sin_tab):
    half_dim = x_val.shape[-1] // 2
    lower = x_val[..., :half_dim]
    upper = x_val[..., half_dim:]
    cos_b = cos_tab[:, None, :]
    sin_b = sin_tab[:, None, :]
    return jnp.concatenate([lower * cos_b - upper * sin_b, upper * cos_b + lower * sin_b], axis=-1)


def attention(hidden, attn_gain, w_query, w_key, w_value):
    num_seqs, seq_len, d_model = hidden.shape
    head_dim = w_query.shape[2]
    x_norm = rms_norm(hidden, attn_gain)
    cos_tab, sin_tab = rope_tables(seq_len, head_dim)
    query = apply_rope(jnp.einsum('bsd,dhe->bshe', x_norm, w_query, preferred_element_type=F32), cos_tab, sin_tab).astype(BF16)
    key_proj = apply_rope(jnp.einsum('bsd,dhe->bshe', x_norm, w_key, preferred_element_type=F32), cos_tab, sin_tab).astype(BF16)
    value_proj = jnp.einsum('bsd,dhe->bshe', x_norm, w_value, preferred_element_type=F32).astype(BF16)
    scores = jnp.einsum('bqhe,bkhe->bhqk', query, key_proj, preferred_element_type=F32) * head_dim ** -0.5
    causal = jnp.arange(seq_len)[:, None] >= jnp.arange(seq_len)[None, :]
    attn_prob = jax.nn.softmax(jnp.where(causal, scores, -1e30), axis=-1).astype(BF16)
    context = jnp.einsum('bhqk,bkhe->bqhe', attn_prob, value_proj, preferred_element_type=F32).astype(BF16)
    return context


def moe_partial(tokens, ids, first, moe_gain, w_router, exp_gate, exp_up, exp_down):
    experts = w_router.shape[1]
    local = len(exp_gate)
    u_norm = rms_norm(tokens, moe_gain)
    logits = jnp.dot(u_norm, w_router, preferred_element_type=F32)
    hot = ids[:, :, None] == jnp.arange(experts, dtype=jnp.int32)[None, None, :]
    picked = jnp.sum(jnp.where(hot, logits[:, None, :], 0.0), axis=-1)
    gates = jax.nn.softmax(picked, axis=-1)
    total = None
    for k in range(local):
        mine = ids == first[k]
        weight = jnp.sum(jnp.where(mine, gates, 0.0), axis=1, keepdims=True)
        chosen = jnp.any(mine, axis=1, keepdims=True)
        gate_pre = jnp.dot(u_norm, exp_gate[k], preferred_element_type=F32)
        up_pre = jnp.dot(u_norm, exp_up[k], preferred_element_type=F32)
        act = (jax.nn.silu(gate_pre) * up_pre).astype(BF16)
        y_out = jnp.dot(act, exp_down[k], preferred_element_type=F32).astype(BF16)
        term = jnp.where(chosen, weight * y_out.astype(F32), 0.0)
        total = term if total is None else total + term
    return total


def solution(mesh):
    tok_spec = P(('dp', 'ep'), None, None)
    col_spec = P(None, 'tp', None)
    exp_spec = P('ep', None, None)
    in_specs = (tok_spec, tok_spec, tok_spec, P(None), col_spec, col_spec, col_spec, P('tp', None, None), P(None), P(None, 'tp'), P(None, 'tp'), P('tp', None), P(None), P(None, None), exp_spec, exp_spec, exp_spec)
    tp = mesh.shape['tp']
    ep = mesh.shape['ep']

    def layer_local(hidden_in, expert_ids, slot_ids, attn_gain, w_query, w_key, w_value, w_out, ffn_gain, w_gate, w_up, w_down, moe_gain, w_router, exp_gate, exp_up, exp_down):
        num_seqs, seq_len, d_model = hidden_in.shape
        tokens = num_seqs * seq_len
        top_k = expert_ids.shape[2]
        heads, head_dim = w_out.shape[0], w_out.shape[1]
        quarter = tokens // tp
        t_idx = lax.axis_index('tp')
        e_idx = lax.axis_index('ep')
        flat = hidden_in.reshape(tokens, d_model)
        core = lax.rem(e_idx, 2)
        own = lax.dynamic_slice_in_dim(flat, t_idx * quarter, quarter, 0)
        own_ids = lax.dynamic_slice_in_dim(expert_ids.reshape(tokens, top_k), t_idx * quarter, quarter, 0)
        gathered = lax.all_gather(own, 'ep', axis=0, tiled=False).reshape(ep // 2, 2, quarter, d_model)
        gathered = lax.dynamic_index_in_dim(gathered, core, 1, keepdims=False).reshape(ep // 2 * quarter, d_model)
        gathered_ids = lax.all_gather(own_ids, 'ep', axis=0, tiled=False).reshape(ep // 2, 2, quarter, top_k)
        gathered_ids = lax.dynamic_index_in_dim(gathered_ids, core, 1, keepdims=False).reshape(ep // 2 * quarter, top_k)
        swap = [(k, k + 1 - 2 * (k % 2)) for k in range(ep)]
        other = [lax.ppermute(w, 'ep', swap) for w in (exp_gate, exp_up, exp_down)]
        per_ep = heads // ep
        rows = lax.dynamic_slice_in_dim(w_out, e_idx * per_ep, per_ep, 0).reshape(per_ep * head_dim, d_model)
        cols = lax.all_to_all(rows, 'tp', 1, 0, tiled=True)
        w_out_cols = lax.all_gather(cols, 'ep', axis=0, tiled=True)

        context = attention(hidden_in, attn_gain, w_query, w_key, w_value)
        ctx_all = lax.all_gather(context, 'tp', axis=0, tiled=False)
        ctx_all = ctx_all.reshape(tp, tokens, ep, per_ep * head_dim)
        w_cols = w_out_cols.reshape(ep, tp, per_ep * head_dim, d_model // tp)
        o_cols = jnp.einsum('tsef,etfd->sd', ctx_all, w_cols, preferred_element_type=F32)
        width = d_model // tp
        x_cols = lax.dynamic_slice_in_dim(flat, t_idx * width, width, 1)
        a_cols = (x_cols.astype(F32) + o_cols).astype(BF16)
        after_attn = lax.all_gather(a_cols, 'tp', axis=1, tiled=True)

        local = exp_gate.shape[0]
        other_e = e_idx + 1 - 2 * core
        first = [e_idx * local + k for k in range(local)] + [other_e * local + k for k in range(local)]
        weights = [[w[k] for k in range(local)] + [v[k] for k in range(local)] for w, v in zip((exp_gate, exp_up, exp_down), other)]
        part = moe_partial(gathered, gathered_ids, first, moe_gain, w_router, *weights)
        out = ffn_call(after_attn, w_gate.T, w_up.T, w_down, ffn_gain.reshape(1, d_model), part.reshape(ep // 2, quarter, d_model))
        return out.reshape(hidden_in.shape)

    return jax.shard_map(layer_local, mesh=mesh, in_specs=in_specs, out_specs=tok_spec, check_vma=False)
```

```python
import functools

import jax
import jax.numpy as jnp
from jax import lax
from jax.experimental import pallas as pl
from jax.experimental.pallas import tpu as pltpu
from jax.sharding import PartitionSpec as P

F32 = jnp.float32
BF16 = jnp.bfloat16
EPS = 1e-6
ROPE_BASE = 10000.0
VMEM_LIMIT = 67043328
MESH = pl.DeviceIdType.MESH
NT = (((1,), (1,)), ((), ()))


RING = 4
SIDES = (0, 1)


def odd(k):
    return lax.rem(k, 2)


def turn(side):
    return 1 - 2 * side


def loop(count, body):
    def step(k, carry):
        body(k)
        return carry
    lax.fori_loop(0, count, step, 0)


def window(index, size):
    return pl.ds(pl.multiple_of(index * size, size), size)


def rcopy(src, dst, ssem, rsem, dev):
    return pltpu.make_async_remote_copy(src_ref=src, dst_ref=dst, send_sem=ssem, recv_sem=rsem, device_id=dev, device_id_type=MESH)


def entry_barrier(neighbours):
    barrier = pltpu.get_barrier_semaphore()
    for dev in neighbours:
        pl.semaphore_signal(barrier, inc=1, device_id=dev, device_id_type=MESH)
    pl.semaphore_wait(barrier, len(neighbours))


def norm_rows(src, dst, gain, rows, step):
    def one(r):
        sl = window(r, step)
        x = src[sl, :].astype(F32)
        inv = lax.rsqrt(jnp.mean(x * x, axis=-1, keepdims=True) + EPS)
        dst[sl, :] = (x * inv * gain[...].astype(F32)).astype(BF16)
    loop(rows // step, one)


def ffn_body(fb, a_ref, wg, wu, wd, gain, m_ref, out_ref,
             a_buf, n2, h, wbuf, dbuf, p1, p2, yrecv, xrecv, mbuf,
             asem, wsem, dsem, msem, osem, ys, yr, xs, xr, gs, gr, fs, fr):
    t = lax.axis_index('tp')
    e = lax.axis_index('ep')
    big = odd(e)
    xc = e // 2
    q = a_buf.shape[1]
    d_model = a_buf.shape[2]
    f_loc = wg.shape[0]
    cw = d_model // 8
    hw = cw // 2
    nf = f_loc // fb
    tail = f_loc - nf * fb
    yright, yleft = {'tp': lax.rem(t + 1, RING)}, {'tp': lax.rem(t + 3, RING)}
    xright, xleft = {'ep': lax.rem(xc + 1, RING) * 2 + big}, {'ep': lax.rem(xc + 3, RING) * 2 + big}

    def cols(cb):
        return window(cb, cw)

    def chunk(c):
        return lax.rem(c + 8, RING)

    def rows(c):
        return window(chunk(c), q)

    def a_load(c, slot):
        return pltpu.make_async_copy(a_ref.at[rows(c)], a_buf.at[slot], asem.at[slot])

    def w_load(i, slot, size):
        sl = pl.ds(pl.multiple_of(i * fb, fb), size)
        return (pltpu.make_async_copy(wg.at[sl], wbuf.at[slot, 0, pl.ds(0, size)], wsem.at[slot, 0]),
                pltpu.make_async_copy(wu.at[sl], wbuf.at[slot, 1, pl.ds(0, size)], wsem.at[slot, 1]))

    def w_start(i):
        slot = odd(i)

        @pl.when(i < nf)
        def _():
            for c in w_load(i, slot, fb):
                c.start()

        @pl.when(i == nf)
        def _():
            for c in w_load(nf, slot, tail):
                c.start()

    def col_of(j):
        return odd(j) * 4 + j // 2

    def d_load(jj):
        slot = odd(jj)
        start = pl.multiple_of(col_of(jj // 2) * cw + slot * hw, hw)
        return pltpu.make_async_copy(wd.at[:, pl.ds(start, hw)], dbuf.at[slot], dsem.at[slot])

    def m_load(k):
        s, j = k // 8 + 1, lax.rem(k, 8)
        side = odd(j)
        c = lax.rem(xc + (2 * side - 1) * (1 + s) + 8, RING)
        slot = odd(k)
        return pltpu.make_async_copy(m_ref.at[c, :, cols(col_of(j))], mbuf.at[slot], msem.at[slot])

    def send(buf, ssem, rsem, src, right, left, side, step, i):
        @pl.when(side == 0)
        def _():
            rcopy(src, buf.at[0, step, i], ssem.at[0, step, i], rsem.at[0, step, i], right).start()

        @pl.when(side == 1)
        def _():
            rcopy(src, buf.at[1, step, i], ssem.at[1, step, i], rsem.at[1, step, i], left).start()

    def ysend(src, side, step, i):
        send(yrecv, ys, yr, src, yright, yleft, side, step, i)

    def xsend(src, side, step, i):
        send(xrecv, xs, xr, src, xright, xleft, side, step, i)

    def arrived(buf, ssem, rsem, side, step, i, dev):
        rcopy(buf.at[side, step, i], buf.at[side, step, i], ssem.at[side, step, i], rsem.at[side, step, i], dev).wait_recv()

    def sent(buf, ssem, rsem, side, step, i, dev):
        rcopy(buf.at[side, step, i], buf.at[side, step, i], ssem.at[side, step, i], rsem.at[side, step, i], dev).wait_send()

    def xserve(k):
        s, j = k // 8, lax.rem(k, 8)
        side, i = odd(j), j // 2
        m_load(k + 1).start()
        m_load(k).wait()
        arrived(xrecv, xs, xr, side, s, i, xright)
        xrecv[side, s, i] = xrecv[side, s, i] + mbuf[odd(k)]
        xsend(xrecv.at[side, s, i], side, s + 1, i)

    def gate_up(serve):
        def block(i, size):
            slot = odd(i)
            for c in w_load(i, slot, size):
                c.wait()
            g = lax.dot_general(n2[...], wbuf[slot, 0, pl.ds(0, size)], NT, preferred_element_type=F32)
            u = lax.dot_general(n2[...], wbuf[slot, 1, pl.ds(0, size)], NT, preferred_element_type=F32)
            h[:, pl.ds(pl.multiple_of(i * fb, fb), size)] = (jax.nn.silu(g) * u).astype(BF16)

        def one(i):
            block(i, fb)
            w_start(i + 2)
            serve(i)
        loop(nf, one)
        block(nf, tail)

    def down(use):
        def one(jj):
            sub = odd(jj)
            d_load(jj).wait()
            r = jnp.dot(h[...], dbuf[sub], preferred_element_type=F32)

            @pl.when(jj + 2 < 16)
            def _():
                d_load(jj + 2).start()
            use(jj // 2, sub, window(sub, hw), r)
        loop(16, one)

    a_load(t - 1, 0).start()
    a_load(t + 1, 1).start()
    w_start(0)
    w_start(1)
    entry_barrier((yright, yleft, xright, xleft))

    def x_first(i):
        xsend(m_ref.at[chunk(xc - 1), :, cols(i)], 0, 0, i)
        xsend(m_ref.at[chunk(xc + 1), :, cols(4 + i)], 1, 0, i)
    loop(4, x_first)
    d_load(0).start()
    d_load(1).start()
    m_load(0).start()

    for slot in SIDES:
        a_load(t, slot).wait()
        norm_rows(a_buf.at[slot], n2.at[pl.ds(slot * q, q)], gain, q, 16)
    a_load(t + 2, 0).start()
    a_load(t, 1).start()
    gate_up(lambda i: None)
    w_start(0)
    w_start(1)

    def use1(j, sub, part, r):
        p1[col_of(j), :, part] = r
        side, i = odd(j), j // 2

        @pl.when(sub == 1)
        def _():
            ysend(p1.at[col_of(j), window(side, q)], side, 0, i)
    down(use1)
    d_load(0).start()
    d_load(1).start()

    for slot in SIDES:
        a_load(t, slot).wait()
        norm_rows(a_buf.at[slot], n2.at[pl.ds(slot * q, q)], gain, q, 16)

    def serve2(i):
        @pl.when(i < 8)
        def _():
            xserve(i)
    gate_up(serve2)
    for k in range(min(nf, 8), 8):
        xserve(k)

    def use2(j, sub, part, r):
        side, i = odd(j), j // 2
        p2[col_of(j), :, part] = r[q:]

        @pl.when(sub == 0)
        def _():
            arrived(yrecv, ys, yr, side, 0, i, yright)
        yrecv[side, 0, i, :, part] = yrecv[side, 0, i, :, part] + r[:q]

        @pl.when(sub == 1)
        def _():
            ysend(yrecv.at[side, 0, i], side, 1, i)
    down(use2)

    def third(j):
        side, i = odd(j), j // 2
        xserve(8 + j)
        arrived(yrecv, ys, yr, side, 1, i, yright)
        yrecv[side, 1, i] = yrecv[side, 1, i] + p1[col_of(j), window((1 - side), q)]
        ysend(yrecv.at[side, 1, i], side, 2, i)
    loop(8, third)

    def out_local(cb):
        return pltpu.make_async_copy(n2.at[pl.ds(0, q), cols(cb)], out_ref.at[rows(t), cols(cb)], osem.at[cb])

    def gather(cb, side, dev):
        return rcopy(n2.at[pl.ds(0, q), cols(cb)], out_ref.at[rows(t), cols(cb)], gs.at[side, cb], gr.at[side, cb], dev)

    def last(j):
        side, i = odd(j), j // 2
        cb = col_of(j)
        k = 16 + j

        @pl.when(j + 1 < 8)
        def _():
            m_load(k + 1).start()
        m_load(k).wait()
        arrived(xrecv, xs, xr, side, 2, i, xright)
        arrived(yrecv, ys, yr, side, 2, i, yright)
        b_val = a_buf[1, :, cols(cb)].astype(F32) + (yrecv[side, 2, i] + p2[cb])
        n2[pl.ds(0, q), cols(cb)] = (b_val + (xrecv[side, 2, i] + mbuf[odd(k)])).astype(BF16)
        out_local(cb).start()
        gather(cb, 0, yright).start()
        gather(cb, 1, yleft).start()
    loop(8, last)

    half = q // 2

    def half_rows(c, which):
        return pl.ds(pl.multiple_of(chunk(c) * q + which * half, half), half)

    def forward(c, which, cb, dev):
        ref = out_ref.at[half_rows(c, which), cols(cb)]
        return rcopy(ref, ref, fs.at[which, cb], fr.at[which, cb], dev)

    def pass_on(j):
        cb = col_of(j)
        gather(cb, 0, yright).wait_recv()
        forward(t - 1, 0, cb, yright).start()
        gather(cb, 1, yleft).wait_recv()
        forward(t + 1, 1, cb, yleft).start()
    loop(8, pass_on)

    def finish(j):
        cb = col_of(j)
        out_local(cb).wait()
        for which in SIDES:
            gather(cb, which, yright).wait_send()
            forward(t, which, cb, yright).wait_send()
            forward(t, which, cb, yright).wait_recv()
    loop(8, finish)

    def drain(k):
        step, j = k // 8, lax.rem(k, 8)
        sent(yrecv, ys, yr, odd(j), step, j // 2, yright)
        sent(xrecv, xs, xr, odd(j), step, j // 2, yright)
    loop(24, drain)


def ffn_call(after_attn, wg_t, wu_t, w_down, gain, m_part, fb=256):
    tokens, d_model = after_attn.shape
    f_loc = wg_t.shape[0]
    q = tokens // 4
    cw = d_model // 8
    hbm = pl.BlockSpec(memory_space=pl.ANY)
    vmem = pl.BlockSpec(memory_space=pltpu.VMEM)
    dma = pltpu.SemaphoreType.DMA
    flops = 2 * tokens * d_model * f_loc * 3
    return pl.pallas_call(
        functools.partial(ffn_body, fb),
        out_shape=jax.ShapeDtypeStruct((tokens, d_model), BF16),
        in_specs=[hbm, hbm, hbm, hbm, vmem, hbm],
        out_specs=hbm,
        scratch_shapes=[
            pltpu.VMEM((2, q, d_model), BF16),
            pltpu.VMEM((2 * q, d_model), BF16),
            pltpu.VMEM((2 * q, f_loc), BF16),
            pltpu.VMEM((2, 2, fb, d_model), BF16),
            pltpu.VMEM((2, f_loc, cw // 2), BF16),
            pltpu.VMEM((8, 2 * q, cw), F32),
            pltpu.VMEM((8, q, cw), F32),
            pltpu.VMEM((2, 3, RING, q, cw), F32),
            pltpu.VMEM((2, 3, RING, q, cw), F32),
            pltpu.VMEM((2, q, cw), F32),
            dma((2,)), dma((2, 2)), dma((2,)), dma((2,)), dma((8,)),
        ] + [dma((2, 3, RING))] * RING + [dma((2, 8))] * RING,
        compiler_params=pltpu.CompilerParams(collective_id=2, has_side_effects=True, vmem_limit_bytes=VMEM_LIMIT),
        cost_estimate=pl.CostEstimate(flops=flops, bytes_accessed=4 * tokens * d_model + 12 * f_loc * d_model, transcendentals=tokens * f_loc),
        name='ffn_ring',
    )(after_attn, wg_t, wu_t, w_down, gain, m_part)


def attn_body(x_ref, wq, wk, wv, wo, eg, eu, ed, gain, cosf, sinf, ids, moe_gain, router,
              ctx_all, hid_all, gates_all, w_cols, og, ou, od,
              xv, xn, raw, wide, wb, qb, kb, vb, ctxb, ub, gbuf,
              lsem, rawsem, cls, cs, cr, cfs, cfr, hs, hr, hfs, hfr, gs, gr, was, war, wxs, wxr, wfs, wfr, wds, wdr, es, er):
    t = lax.axis_index('tp')
    e = lax.axis_index('ep')
    core = odd(e)
    xc = e // 2
    tokens, d_model = xv.shape
    heads, hd = wq.shape[1], wq.shape[2]
    q = tokens // 4
    kblk = raw.shape[1]
    nk = d_model // kblk
    width = d_model // 4
    pair = 2 * hd
    pairs = heads // 2

    def y_dev(k):
        return {'tp': lax.rem(t + k + 4, RING)}

    def x_id(k):
        return lax.rem(xc + k + 4, RING) * 2 + core

    def x_dev(k):
        return {'ep': x_id(k)}
    partner = {'ep': xc * 2 + 1 - core}

    own_rows = window(t, q)
    rots = (x_ref, xv)
    load_x = [pltpu.make_async_copy(x_ref.at[pl.ds(k * q, q)], xv.at[pl.ds(k * q, q)], lsem.at[k]) for k in range(RING)]
    for c in load_x:
        c.start()
    mats = (wq, wk, wv)

    def raw_load(m, k):
        sl = window(k, kblk)
        return pltpu.make_async_copy(mats[m].at[sl], raw.at[odd(k)], rawsem.at[odd(k)])
    raw_load(0, 0).start()
    raw_load(0, 1).start()
    entry_barrier((y_dev(1), y_dev(-1), y_dev(2), x_dev(1), x_dev(-1), x_dev(2), partner))

    head_rows = window(e, hd)

    def col_block(c):
        return window(c, width)
    w_own = pltpu.make_async_copy(wo.at[head_rows, col_block(t)], w_cols.at[e, t], lsem.at[4])
    w_own.start()
    swap = [rcopy(wo.at[head_rows, col_block(lax.rem(t + k, RING))], w_cols.at[e, t], was.at[k - 1], war.at[k - 1], y_dev(k)) for k in (1, 2, 3)]
    for c in swap:
        c.start()
    hid = [rcopy(x_ref.at[own_rows], hid_all.at[xc], hs.at[k], hr.at[k], x_dev(1 - 2 * k)) for k in SIDES]
    for c in hid:
        c.start()
    exp = [rcopy(src, dst, es.at[k], er.at[k], partner) for k, (src, dst) in enumerate(((eg, og), (eu, ou), (ed, od)))]
    for c in exp:
        c.start()

    for k in range(RING):
        load_x[k].wait()
        norm_rows(xv.at[pl.ds(k * q, q)], xn.at[pl.ds(k * q, q)], gain, q, 16)
    hid_own = pltpu.make_async_copy(xv.at[own_rows], hid_all.at[xc], lsem.at[5])
    hid_own.start()

    norm_rows(xv.at[own_rows], ub, moe_gain, q, 16)
    logits = jnp.dot(ub[...], router[...], preferred_element_type=F32)
    lane = lax.broadcasted_iota(jnp.int32, logits.shape, 1)
    own_ids = ids[own_rows, :]
    chosen = lane == own_ids[:, 0:1]
    for j in range(1, ids.shape[1]):
        chosen = jnp.logical_or(chosen, lane == own_ids[:, j:j + 1])
    top = jnp.max(jnp.where(chosen, logits, -jnp.inf), axis=-1, keepdims=True)
    p = jnp.where(chosen, jnp.exp(jnp.where(chosen, logits - top, 0.0)), 0.0)
    gbuf[...] = p / jnp.sum(p, axis=-1, keepdims=True)
    gate_own = pltpu.make_async_copy(gbuf, gates_all.at[xc], lsem.at[6])
    gate_own.start()
    gate_out = [rcopy(gbuf, gates_all.at[xc], gs.at[k - 1], gr.at[k - 1], x_dev(k)) for k in (1, 2, 3)]
    for c in gate_out:
        c.start()

    for m in range(3):
        def one(k, m=m):
            slot = odd(k)
            raw_load(m, k).wait()
            wide[...] = raw[slot].astype(F32).reshape(kblk * heads, hd)

            @pl.when(k + 2 < nk)
            def _():
                raw_load(m, k + 2).start()
            rows = window(k, kblk)
            for h in range(heads):
                wb[m, rows, h * hd:(h + 1) * hd] = wide[pl.ds(h, kblk, stride=heads), :].astype(BF16)
        loop(nk, one)
        if m < 2:
            raw_load(m + 1, 0).start()
            raw_load(m + 1, 1).start()

    w_own.wait()
    for c in swap:
        c.wait_recv()
    wx = [rcopy(w_cols.at[e], w_cols.at[e], wxs.at[k], wxr.at[k], x_dev(1 - 2 * k)) for k in SIDES]
    for c in wx:
        c.start()

    def w_core(k):
        return rcopy(w_cols.at[x_id(k)], w_cols.at[x_id(k)], wds.at[k], wdr.at[k], partner)
    w_core(0).start()

    def ctx_cols(g):
        return window(g, pair)

    def ctx_local(g):
        return pltpu.make_async_copy(ctxb.at[g], ctx_all.at[t, :, ctx_cols(g)], cls.at[g])

    def ctx_send(g, side):
        return rcopy(ctxb.at[g], ctx_all.at[t, :, ctx_cols(g)], cs.at[side, g], cr.at[side, g], y_dev(turn(side)))

    def ctx_forward(g, side):
        src = lax.rem(t + 3 + 2 * side, RING)
        ref = ctx_all.at[src, pl.ds(side * (tokens // 2), tokens // 2), ctx_cols(g)]
        return rcopy(ref, ref, cfs.at[side, g], cfr.at[side, g], y_dev(turn(side)))

    def pass_on(g):
        for side in SIDES:
            ctx_send(g, side).wait_recv()
            ctx_forward(g, side).start()

    scale = hd ** -0.5
    tri = lax.broadcasted_iota(jnp.int32, (q, q), 0) >= lax.broadcasted_iota(jnp.int32, (q, q), 1)

    def heads_of(g):
        cols = ctx_cols(g)
        for m, dst in ((0, qb), (1, kb), (2, vb)):
            r = jnp.dot(xn[...], wb[m, :, cols], preferred_element_type=F32)
            if m == 2:
                dst[...] = r.astype(BF16)
            else:
                for h in SIDES:
                    part = r[:, h * hd:(h + 1) * hd]
                    turned = part * cosf[...] + pltpu.roll(part, hd // 2, 1) * sinf[...]
                    dst[:, h * hd:(h + 1) * hd] = turned.astype(BF16)
        for h in SIDES:
            hc = slice(h * hd, (h + 1) * hd)
            for b in range(RING):
                s = lax.dot_general(qb[b * q:(b + 1) * q, hc], kb[0:(b + 1) * q, hc], NT, preferred_element_type=F32) * scale
                diag = jnp.where(tri, s[:, b * q:], -1e30)
                s = diag if b == 0 else jnp.concatenate([s[:, :b * q], diag], axis=1)
                w = jnp.exp(s - jnp.max(s, axis=-1, keepdims=True))
                prob = (w * (1.0 / jnp.sum(w, axis=-1, keepdims=True))).astype(BF16)
                ctxb[g, b * q:(b + 1) * q, hc] = jnp.dot(prob, vb[0:(b + 1) * q, hc], preferred_element_type=F32).astype(BF16)
        ctx_local(g).start()
        ctx_send(g, 0).start()
        ctx_send(g, 1).start()

        @pl.when(g >= 2)
        def _():
            pass_on(g - 2)
    loop(pairs, heads_of)

    def hid_forward(side):
        ref = hid_all.at[lax.rem(xc + 3 + 2 * side, RING), pl.ds(side * (q // 2), q // 2)]
        return rcopy(ref, ref, hfs.at[side], hfr.at[side], x_dev(turn(side)))

    def w_forward(side):
        ref = w_cols.at[x_id(2 * side - 1), pl.ds(2 * side, 2)]
        return rcopy(ref, ref, wfs.at[side], wfr.at[side], x_dev(turn(side)))
    for side in SIDES:
        hid[side].wait_recv()
        hid_forward(side).start()
    pass_on(pairs - 2)
    for side in SIDES:
        wx[side].wait_recv()
        w_forward(side).start()
    w_core(1).start()
    w_core(3).start()
    pass_on(pairs - 1)
    for side in SIDES:
        w_forward(side).wait_recv()
    w_core(2).start()

    for side in SIDES:
        hid_forward(side).wait()
        hid[side].wait_send()
        wx[side].wait_send()
        w_forward(side).wait_send()
        for g in range(pairs):
            ctx_send(g, side).wait_send()
            ctx_forward(g, side).wait()
    for c in swap:
        c.wait_send()
    for c in gate_out:
        c.wait()
    for c in exp:
        c.wait()
    for k in range(RING):
        w_core(k).wait()
    for g in range(pairs):
        ctx_local(g).wait()
    hid_own.wait()
    gate_own.wait()


def attn_call(x, wq, wk, wv, wo, eg, eu, ed, gain, cosf, sinf, ids, moe_gain, router):
    tokens, d_model = x.shape
    heads, hd = wq.shape[1], wq.shape[2]
    q = tokens // 4
    kblk = min(256, d_model)
    experts = router.shape[1]
    hbm = pl.BlockSpec(memory_space=pl.ANY)
    vmem = pl.BlockSpec(memory_space=pltpu.VMEM)
    dma = pltpu.SemaphoreType.DMA
    two, three = dma((2,)), dma((3,))
    sds = jax.ShapeDtypeStruct
    pairs = heads // 2
    return pl.pallas_call(
        attn_body,
        out_shape=(sds((4, tokens, heads * hd), BF16), sds((4, q, d_model), BF16), sds((4, q, experts), F32),
                   sds((8, 4, hd, d_model // 4), BF16), sds(eg.shape, BF16), sds(eu.shape, BF16), sds(ed.shape, BF16)),
        in_specs=[hbm] * 8 + [vmem] * 6,
        out_specs=(hbm,) * 7,
        scratch_shapes=[
            pltpu.VMEM((tokens, d_model), BF16), pltpu.VMEM((tokens, d_model), BF16),
            pltpu.VMEM((2, kblk, heads, hd), BF16), pltpu.VMEM((kblk * heads, hd), F32),
            pltpu.VMEM((3, d_model, heads * hd), BF16),
            pltpu.VMEM((tokens, 2 * hd), BF16), pltpu.VMEM((tokens, 2 * hd), BF16), pltpu.VMEM((tokens, 2 * hd), BF16),
            pltpu.VMEM((pairs, tokens, 2 * hd), BF16), pltpu.VMEM((q, d_model), BF16), pltpu.VMEM((q, experts), F32),
            dma((7,)), two, dma((pairs,)),
        ] + [dma((2, pairs))] * RING + [two] * RING + [three] * RING + [two] * RING + [dma((RING,))] * 2 + [three] * 2,
        compiler_params=pltpu.CompilerParams(collective_id=0, has_side_effects=True, vmem_limit_bytes=VMEM_LIMIT),
        cost_estimate=pl.CostEstimate(flops=2 * tokens * d_model * heads * hd * 3, bytes_accessed=6 * d_model * heads * hd, transcendentals=heads * tokens * tokens),
        name='attn_gather',
    )(x, wq, wk, wv, wo, eg, eu, ed, gain, cosf, sinf, ids, moe_gain, router)


def moe_body(ctx_all, w_cols, x_ref, hid_all, gates_all, eg, eu, ed, og, ou, od, moe_gain, a_full, m_part,
             wcv, cbuf, xbuf, abuf, u, mv, h, wbuf, dbuf, gbuf,
             lsem, csem, xsem, als, as_, ar, fs, fr, hsem, wsem, dsem, msem):
    t = lax.axis_index('tp')
    e = lax.axis_index('ep')
    core = odd(e)
    tokens, d_model = x_ref.shape
    q = tokens // 4
    width = d_model // 4
    local, fe = eg.shape[0], eg.shape[1]
    fb = wbuf.shape[2]
    nfull = fe // fb
    tail = fe - nfull * fb
    sizes = [fb] * nfull + [tail]
    nb = len(sizes)
    cw = dbuf.shape[2]
    nn = d_model // cw

    def y_dev(k):
        return {'tp': lax.rem(t + k + 4, RING)}
    my_cols = window(t, width)

    def rows(c):
        return window(c, q)

    hk = wcv.shape[1]
    load_w = [pltpu.make_async_copy(w_cols.at[:, k], wcv.at[k], lsem.at[k]) for k in range(RING)]
    load_g = pltpu.make_async_copy(gates_all, gbuf, lsem.at[4])

    def ctx_load(c, slot):
        wide = cbuf.shape[2] // 4
        return [pltpu.make_async_copy(ctx_all.at[k, rows(c)], cbuf.at[slot, :, pl.ds(k * wide, wide)], csem.at[slot, k]) for k in range(RING)]

    def x_load(c, slot):
        return pltpu.make_async_copy(x_ref.at[rows(c), my_cols], xbuf.at[slot], xsem.at[slot])

    def hid_load(k):
        return pltpu.make_async_copy(hid_all.at[k], u.at[pl.ds(k * q, q)], hsem.at[k])

    def w_load(k, b, slot, from_own):
        g_ref, u_ref = (eg, eu) if from_own else (og, ou)
        kk = k if from_own else k - local
        sl = pl.ds(b * fb, sizes[b])
        return (pltpu.make_async_copy(g_ref.at[kk, sl], wbuf.at[slot, 0, pl.ds(0, sizes[b])], wsem.at[slot, 0]),
                pltpu.make_async_copy(u_ref.at[kk, sl], wbuf.at[slot, 1, pl.ds(0, sizes[b])], wsem.at[slot, 1]))

    def w_start(k, b):
        slot = odd(k * nb + b)

        @pl.when(k < local)
        def _():
            for c in w_load(k, b, slot, True):
                c.start()

        @pl.when(jnp.logical_and(k >= local, k < 2 * local))
        def _():
            for c in w_load(k, b, slot, False):
                c.start()

    def d_load(k, n, from_own):
        ref = ed if from_own else od
        kk = k if from_own else k - local
        slot = odd(n)
        return pltpu.make_async_copy(ref.at[kk, :, window(n, cw)], dbuf.at[slot], dsem.at[slot])

    def d_start(k, n):
        @pl.when(k < local)
        def _():
            d_load(k, n, True).start()

        @pl.when(jnp.logical_and(k >= local, k < 2 * local))
        def _():
            d_load(k, n, False).start()

    for c in ctx_load(0, 0):
        c.start()
    for c in load_w:
        c.start()
    x_load(0, 0).start()
    entry_barrier((y_dev(1), y_dev(-1)))
    load_g.start()
    for k in range(RING):
        hid_load(k).start()
    for b in SIDES:
        w_start(jnp.int32(0), b)
        d_start(jnp.int32(0), jnp.int32(b))
    for c in load_w:
        c.wait()

    def a_local(c):
        return pltpu.make_async_copy(abuf.at[c], a_full.at[rows(c), my_cols], als.at[c])

    def a_send(c, side):
        return rcopy(abuf.at[c], a_full.at[rows(c), my_cols], as_.at[side, c], ar.at[side, c], y_dev(turn(side)))

    def a_forward(c, side):
        src = lax.rem(t + 3 + 2 * side, RING)
        ref = a_full.at[pl.ds(pl.multiple_of(c * q + side * (q // 2), q // 2), q // 2), window(src, width)]
        return rcopy(ref, ref, fs.at[side, c], fr.at[side, c], y_dev(turn(side)))

    def o_chunk(c):
        slot = odd(c)

        @pl.when(c + 1 < 4)
        def _():
            for d in ctx_load(c + 1, 1 - slot):
                d.start()
            x_load(c + 1, 1 - slot).start()
        for d in ctx_load(c, slot):
            d.wait()
        x_load(c, slot).wait()
        o = jnp.dot(cbuf[slot], wcv[...].reshape(4 * hk * wcv.shape[2], width), preferred_element_type=F32)
        abuf[c] = (xbuf[slot].astype(F32) + o).astype(BF16)
        a_local(c).start()
        a_send(c, 0).start()
        a_send(c, 1).start()
    loop(4, o_chunk)

    for k in range(RING):
        hid_load(k).wait()
        norm_rows(u.at[pl.ds(k * q, q)], u.at[pl.ds(k * q, q)], moe_gain, q, 16)
    load_g.wait()

    def pass_on(c):
        for side in SIDES:
            a_send(c, side).wait_recv()
            a_forward(c, side).start()

    def m_out(n):
        cols = window(n, cw)
        return pltpu.make_async_copy(mv.at[n], m_part.at[:, cols], msem.at[n])

    def expert(k):
        which = jnp.where(k < local, e * local + k, (xc2 + 1 - core) * local + k - local)
        gate_all = gbuf[...].reshape(tokens, gbuf.shape[2])
        lane = lax.broadcasted_iota(jnp.int32, gate_all.shape, 1)
        weight = jnp.sum(jnp.where(lane == which, gate_all, 0.0), axis=1, keepdims=True)
        for b, size in enumerate(sizes):
            slot = odd(k * nb + b)
            for c in w_load(0, b, slot, True):
                c.wait()
            g = lax.dot_general(u[...], wbuf[slot, 0, 0:size], NT, preferred_element_type=F32)
            v = lax.dot_general(u[...], wbuf[slot, 1, 0:size], NT, preferred_element_type=F32)
            h[:, b * fb:b * fb + size] = (jax.nn.silu(g) * v).astype(BF16)
            nxt = b + 2
            w_start(k + nxt // nb, nxt % nb)

        def block(n):
            d_load(0, n, True).wait()
            y = jnp.dot(h[...], dbuf[odd(n)], preferred_element_type=F32).astype(BF16)
            term = jnp.where(weight > 0.0, weight * y.astype(F32), 0.0)

            @pl.when(n + 2 < nn)
            def _():
                d_start(k, n + 2)

            @pl.when(n + 2 >= nn)
            def _():
                d_start(k + 1, n + 2 - nn)

            @pl.when(k == 0)
            def _():
                mv[n] = term

            @pl.when(k > 0)
            def _():
                mv[n] = mv[n] + term

            @pl.when(k == 2 * local - 1)
            def _():
                m_out(n).start()
        loop(nn, block)

        @pl.when(k >= 0)
        def _():
            pass_on(k)
    xc2 = e - core
    loop(2 * local, expert)

    for c in range(RING):
        a_local(c).wait()
        for side in SIDES:
            a_send(c, side).wait_send()
            a_forward(c, side).wait()

    def finish(n):
        m_out(n).wait()
    loop(nn, finish)


def moe_call(ctx_all, w_cols, x, hid_all, gates_all, eg, eu, ed, og, ou, od, moe_gain, fb=256, cw=512):
    tokens, d_model = x.shape
    q = tokens // 4
    width = d_model // 4
    hd = w_cols.shape[2]
    local, fe = eg.shape[0], eg.shape[1]
    assert 2 * local == 4
    hbm = pl.BlockSpec(memory_space=pl.ANY)
    vmem = pl.BlockSpec(memory_space=pltpu.VMEM)
    dma = pltpu.SemaphoreType.DMA
    sds = jax.ShapeDtypeStruct
    nn = d_model // cw
    return pl.pallas_call(
        moe_body,
        out_shape=(sds((tokens, d_model), BF16), sds((tokens, d_model), F32)),
        in_specs=[hbm] * 11 + [vmem],
        out_specs=(hbm, hbm),
        scratch_shapes=[
            pltpu.VMEM((4, 8, hd, width), BF16), pltpu.VMEM((2, q, 4 * 8 * hd), BF16), pltpu.VMEM((2, q, width), BF16),
            pltpu.VMEM((4, q, width), BF16), pltpu.VMEM((tokens, d_model), BF16),
            pltpu.VMEM((nn, tokens, cw), F32), pltpu.VMEM((tokens, fe), BF16), pltpu.VMEM((2, 2, fb, d_model), BF16),
            pltpu.VMEM((2, fe, cw), BF16), pltpu.VMEM(gates_all.shape, F32),
            dma((5,)), dma((2, RING)), dma((2,)), dma((RING,)),
        ] + [dma((2, RING))] * RING + [dma((RING,)), dma((2, 2)), dma((2,)), dma((nn,))],
        compiler_params=pltpu.CompilerParams(collective_id=1, has_side_effects=True, vmem_limit_bytes=VMEM_LIMIT),
        cost_estimate=pl.CostEstimate(flops=2 * tokens * d_model * fe * 3 * 4, bytes_accessed=24 * fe * d_model, transcendentals=4 * tokens * fe),
        name='moe_gather',
    )(ctx_all, w_cols, x, hid_all, gates_all, eg, eu, ed, og, ou, od, moe_gain)


def rope_tables(seq_len, head_dim):
    inv_freq = ROPE_BASE ** (-jnp.arange(head_dim // 2, dtype=F32) * (2.0 / head_dim))
    angle = jnp.arange(seq_len, dtype=F32)[:, None] * inv_freq[None, :]
    return jnp.cos(angle), jnp.sin(angle)


def solution(mesh, fb=256, cw=512):
    tok_spec = P(('dp', 'ep'), None, None)
    col_spec = P(None, 'tp', None)
    exp_spec = P('ep', None, None)
    in_specs = (tok_spec, tok_spec, tok_spec, P(None), col_spec, col_spec, col_spec, P('tp', None, None), P(None), P(None, 'tp'), P(None, 'tp'), P('tp', None), P(None), P(None, None), exp_spec, exp_spec, exp_spec)

    def layer_local(hidden_in, expert_ids, slot_ids, attn_gain, w_query, w_key, w_value, w_out, ffn_gain, w_gate, w_up, w_down, moe_gain, w_router, exp_gate, exp_up, exp_down):
        num_seqs, seq_len, d_model = hidden_in.shape
        tokens = num_seqs * seq_len
        heads, head_dim = w_out.shape[0], w_out.shape[1]
        x = hidden_in.reshape(tokens, d_model)
        ids = expert_ids.reshape(tokens, expert_ids.shape[2])
        cos_tab, sin_tab = rope_tables(seq_len, head_dim)
        cosf = jnp.concatenate([cos_tab, cos_tab], axis=1)
        sinf = jnp.concatenate([-sin_tab, sin_tab], axis=1)
        eg, eu = jnp.swapaxes(exp_gate, 1, 2), jnp.swapaxes(exp_up, 1, 2)
        row = lambda g: g.reshape(1, d_model)
        ctx_all, hid_all, gates_all, w_cols, og, ou, od = attn_call(
            x, w_query, w_key, w_value, w_out.reshape(heads * head_dim, d_model), eg, eu, exp_down,
            row(attn_gain), cosf, sinf, ids, row(moe_gain), w_router)
        after_attn, m_part = moe_call(ctx_all, w_cols, x, hid_all, gates_all, eg, eu, exp_down, og, ou, od, row(moe_gain), fb=fb, cw=cw)
        out = ffn_call(after_attn, w_gate.T, w_up.T, w_down, row(ffn_gain), m_part.reshape(4, tokens // 4, d_model), fb=fb)
        return out.reshape(hidden_in.shape)

    return jax.shard_map(layer_local, mesh=mesh, in_specs=in_specs, out_specs=tok_spec, check_vma=False)
```

```python
import functools

import jax
import jax.numpy as jnp
import numpy as np
from jax import lax
from jax.experimental import pallas as pl
from jax.experimental.pallas import tpu as pltpu
from jax.sharding import PartitionSpec as P

F32 = jnp.float32
BF16 = jnp.bfloat16
EPS = 1e-6
ROPE_BASE = 10000.0
VMEM_LIMIT = 67043328
MESH = pl.DeviceIdType.MESH
NT = (((1,), (1,)), ((), ()))


RING = 4
SIDES = (0, 1)


def odd(k):
    return lax.rem(k, 2)


def turn(side):
    return 1 - 2 * side


def loop(count, body):
    def step(k, carry):
        body(k)
        return carry
    lax.fori_loop(0, count, step, 0)


def window(index, size):
    return pl.ds(pl.multiple_of(index * size, size), size)


def rcopy(src, dst, ssem, rsem, dev):
    return pltpu.make_async_remote_copy(src_ref=src, dst_ref=dst, send_sem=ssem, recv_sem=rsem, device_id=dev, device_id_type=MESH)


def entry_barrier(neighbours):
    barrier = pltpu.get_barrier_semaphore()
    for dev in neighbours:
        pl.semaphore_signal(barrier, inc=1, device_id=dev, device_id_type=MESH)
    pl.semaphore_wait(barrier, len(neighbours))


def norm_rows(src, dst, gain, rows, step):
    def one(r):
        sl = window(r, step)
        x = src[sl, :].astype(F32)
        inv = lax.rsqrt(jnp.mean(x * x, axis=-1, keepdims=True) + EPS)
        dst[sl, :] = (x * inv * gain[...].astype(F32).reshape(1, -1)).astype(BF16)
    loop(rows // step, one)


def ffn_body(fb, a_ref, wg, wu, wd, gain, m_ref, out_ref,
             a_buf, n2, h, wbuf, dbuf, p1, p2, yrecv, xrecv, mbuf,
             asem, wsem, dsem, msem, osem, ys, yr, xs, xr, gs, gr, fs, fr):
    t = lax.axis_index('tp')
    e = lax.axis_index('ep')
    big = odd(e)
    xc = e // 2
    q = a_buf.shape[1]
    d_model = a_buf.shape[2]
    f_loc = wg.shape[0]
    cw = d_model // 8
    hw = cw // 2
    nf = f_loc // fb
    tail = f_loc - nf * fb
    yright, yleft = {'tp': lax.rem(t + 1, RING)}, {'tp': lax.rem(t + 3, RING)}
    xright, xleft = {'ep': lax.rem(xc + 1, RING) * 2 + big}, {'ep': lax.rem(xc + 3, RING) * 2 + big}

    def cols(cb):
        return window(cb, cw)

    def chunk(c):
        return lax.rem(c + 8, RING)

    def rows(c):
        return window(chunk(c), q)

    def a_load(c, slot):
        return pltpu.make_async_copy(a_ref.at[rows(c)], a_buf.at[slot], asem.at[slot])

    def w_load(i, slot, size):
        sl = pl.ds(pl.multiple_of(i * fb, fb), size)
        return (pltpu.make_async_copy(wg.at[sl], wbuf.at[slot, 0, pl.ds(0, size)], wsem.at[slot, 0]),
                pltpu.make_async_copy(wu.at[sl], wbuf.at[slot, 1, pl.ds(0, size)], wsem.at[slot, 1]))

    def w_start(i):
        slot = odd(i)

        @pl.when(i < nf)
        def _():
            for c in w_load(i, slot, fb):
                c.start()

        @pl.when(i == nf)
        def _():
            for c in w_load(nf, slot, tail):
                c.start()

    def col_of(j):
        return odd(j) * 4 + j // 2

    def d_load(jj):
        slot = odd(jj)
        start = pl.multiple_of(col_of(jj // 2) * cw + slot * hw, hw)
        return pltpu.make_async_copy(wd.at[:, pl.ds(start, hw)], dbuf.at[slot], dsem.at[slot])

    def m_load(k):
        s, j = k // 8 + 1, lax.rem(k, 8)
        side = odd(j)
        c = lax.rem(xc + (2 * side - 1) * (1 + s) + 8, RING)
        slot = odd(k)
        return pltpu.make_async_copy(m_ref.at[c, :, cols(col_of(j))], mbuf.at[slot], msem.at[slot])

    def send(buf, ssem, rsem, src, right, left, side, step, i):
        @pl.when(side == 0)
        def _():
            rcopy(src, buf.at[0, step, i], ssem.at[0, step, i], rsem.at[0, step, i], right).start()

        @pl.when(side == 1)
        def _():
            rcopy(src, buf.at[1, step, i], ssem.at[1, step, i], rsem.at[1, step, i], left).start()

    def ysend(src, side, step, i):
        send(yrecv, ys, yr, src, yright, yleft, side, step, i)

    def xsend(src, side, step, i):
        send(xrecv, xs, xr, src, xright, xleft, side, step, i)

    def arrived(buf, ssem, rsem, side, step, i, dev):
        rcopy(buf.at[side, step, i], buf.at[side, step, i], ssem.at[side, step, i], rsem.at[side, step, i], dev).wait_recv()

    def sent(buf, ssem, rsem, side, step, i, dev):
        rcopy(buf.at[side, step, i], buf.at[side, step, i], ssem.at[side, step, i], rsem.at[side, step, i], dev).wait_send()

    def xserve(k):
        s, j = k // 8, lax.rem(k, 8)
        side, i = odd(j), j // 2
        m_load(k + 1).start()
        m_load(k).wait()
        arrived(xrecv, xs, xr, side, s, i, xright)
        xrecv[side, s, i] = xrecv[side, s, i] + mbuf[odd(k)]
        xsend(xrecv.at[side, s, i], side, s + 1, i)

    def gate_up(serve):
        def block(i, size):
            slot = odd(i)
            for c in w_load(i, slot, size):
                c.wait()
            g = lax.dot_general(n2[...], wbuf[slot, 0, pl.ds(0, size)], NT, preferred_element_type=F32)
            u = lax.dot_general(n2[...], wbuf[slot, 1, pl.ds(0, size)], NT, preferred_element_type=F32)
            h[:, pl.ds(pl.multiple_of(i * fb, fb), size)] = (jax.nn.silu(g) * u).astype(BF16)

        def one(i):
            block(i, fb)
            w_start(i + 2)
            serve(i)
        loop(nf, one)
        block(nf, tail)

    def down(use):
        def one(jj):
            sub = odd(jj)
            d_load(jj).wait()
            r = jnp.dot(h[...], dbuf[sub], preferred_element_type=F32)

            @pl.when(jj + 2 < 16)
            def _():
                d_load(jj + 2).start()
            use(jj // 2, sub, window(sub, hw), r)
        loop(16, one)

    a_load(t - 1, 0).start()
    a_load(t + 1, 1).start()
    w_start(0)
    w_start(1)
    entry_barrier((yright, yleft, xright, xleft))

    def x_first(i):
        xsend(m_ref.at[chunk(xc - 1), :, cols(i)], 0, 0, i)
        xsend(m_ref.at[chunk(xc + 1), :, cols(4 + i)], 1, 0, i)
    loop(4, x_first)
    d_load(0).start()
    d_load(1).start()
    m_load(0).start()

    for slot in SIDES:
        a_load(t, slot).wait()
        norm_rows(a_buf.at[slot], n2.at[pl.ds(slot * q, q)], gain, q, 16)
    a_load(t + 2, 0).start()
    a_load(t, 1).start()
    gate_up(lambda i: None)
    w_start(0)
    w_start(1)

    def use1(j, sub, part, r):
        p1[col_of(j), :, part] = r
        side, i = odd(j), j // 2

        @pl.when(sub == 1)
        def _():
            ysend(p1.at[col_of(j), window(side, q)], side, 0, i)
    down(use1)
    d_load(0).start()
    d_load(1).start()

    for slot in SIDES:
        a_load(t, slot).wait()
        norm_rows(a_buf.at[slot], n2.at[pl.ds(slot * q, q)], gain, q, 16)

    def serve2(i):
        @pl.when(i < 8)
        def _():
            xserve(i)
    gate_up(serve2)
    for k in range(min(nf, 8), 8):
        xserve(k)

    def use2(j, sub, part, r):
        side, i = odd(j), j // 2
        p2[col_of(j), :, part] = r[q:]

        @pl.when(sub == 0)
        def _():
            arrived(yrecv, ys, yr, side, 0, i, yright)
        yrecv[side, 0, i, :, part] = yrecv[side, 0, i, :, part] + r[:q]

        @pl.when(sub == 1)
        def _():
            ysend(yrecv.at[side, 0, i], side, 1, i)
    down(use2)

    def third(j):
        side, i = odd(j), j // 2
        xserve(8 + j)
        arrived(yrecv, ys, yr, side, 1, i, yright)
        yrecv[side, 1, i] = yrecv[side, 1, i] + p1[col_of(j), window((1 - side), q)]
        ysend(yrecv.at[side, 1, i], side, 2, i)
    loop(8, third)

    def out_local(cb):
        return pltpu.make_async_copy(n2.at[pl.ds(0, q), cols(cb)], out_ref.at[rows(t), cols(cb)], osem.at[cb])

    def gather(cb, side, dev):
        return rcopy(n2.at[pl.ds(0, q), cols(cb)], out_ref.at[rows(t), cols(cb)], gs.at[side, cb], gr.at[side, cb], dev)

    def last(j):
        side, i = odd(j), j // 2
        cb = col_of(j)
        k = 16 + j

        @pl.when(j + 1 < 8)
        def _():
            m_load(k + 1).start()
        m_load(k).wait()
        arrived(xrecv, xs, xr, side, 2, i, xright)
        arrived(yrecv, ys, yr, side, 2, i, yright)
        b_val = a_buf[1, :, cols(cb)].astype(F32) + (yrecv[side, 2, i] + p2[cb])
        n2[pl.ds(0, q), cols(cb)] = (b_val + (xrecv[side, 2, i] + mbuf[odd(k)])).astype(BF16)
        out_local(cb).start()
        gather(cb, 0, yright).start()
        gather(cb, 1, yleft).start()
    loop(8, last)

    half = q // 2

    def half_rows(c, which):
        return pl.ds(pl.multiple_of(chunk(c) * q + which * half, half), half)

    def forward(c, which, cb, dev):
        ref = out_ref.at[half_rows(c, which), cols(cb)]
        return rcopy(ref, ref, fs.at[which, cb], fr.at[which, cb], dev)

    def pass_on(j):
        cb = col_of(j)
        gather(cb, 0, yright).wait_recv()
        forward(t - 1, 0, cb, yright).start()
        gather(cb, 1, yleft).wait_recv()
        forward(t + 1, 1, cb, yleft).start()
    loop(8, pass_on)

    def finish(j):
        cb = col_of(j)
        out_local(cb).wait()
        for which in SIDES:
            gather(cb, which, yright).wait_send()
            forward(t, which, cb, yright).wait_send()
            forward(t, which, cb, yright).wait_recv()
    loop(8, finish)

    def drain(k):
        step, j = k // 8, lax.rem(k, 8)
        sent(yrecv, ys, yr, odd(j), step, j // 2, yright)
        sent(xrecv, xs, xr, odd(j), step, j // 2, yright)
    loop(24, drain)


def ffn_call(after_attn, wg_t, wu_t, w_down, gain, m_part):
    tokens, d_model = after_attn.shape
    f_loc = wg_t.shape[0]
    fb = 256 if f_loc > 512 else 128
    q = tokens // 4
    cw = d_model // 8
    hbm = pl.BlockSpec(memory_space=pl.ANY)
    vmem = pl.BlockSpec(memory_space=pltpu.VMEM)
    dma = pltpu.SemaphoreType.DMA
    flops = 2 * tokens * d_model * f_loc * 3
    return pl.pallas_call(
        functools.partial(ffn_body, fb),
        out_shape=jax.ShapeDtypeStruct((tokens, d_model), BF16),
        in_specs=[hbm, hbm, hbm, hbm, vmem, hbm],
        out_specs=hbm,
        scratch_shapes=[
            pltpu.VMEM((2, q, d_model), BF16),
            pltpu.VMEM((2 * q, d_model), BF16),
            pltpu.VMEM((2 * q, f_loc), BF16),
            pltpu.VMEM((2, 2, fb, d_model), BF16),
            pltpu.VMEM((2, f_loc, cw // 2), BF16),
            pltpu.VMEM((8, 2 * q, cw), F32),
            pltpu.VMEM((8, q, cw), F32),
            pltpu.VMEM((2, 3, RING, q, cw), F32),
            pltpu.VMEM((2, 3, RING, q, cw), F32),
            pltpu.VMEM((2, q, cw), F32),
            dma((2,)), dma((2, 2)), dma((2,)), dma((2,)), dma((8,)),
        ] + [dma((2, 3, RING))] * RING + [dma((2, 8))] * RING,
        compiler_params=pltpu.CompilerParams(collective_id=2, has_side_effects=True, vmem_limit_bytes=VMEM_LIMIT),
        cost_estimate=pl.CostEstimate(flops=flops, bytes_accessed=4 * tokens * d_model + 12 * f_loc * d_model, transcendentals=tokens * f_loc),
        name='ffn_ring',
    )(after_attn, wg_t, wu_t, w_down, gain, m_part)


def front_body(x_ref, wq, wk, wv, wo, eg, eu, ed, attn_gain, moe_gain, freq, ids, router,
               a_full, m_part, ctx_all, hid_all, ids_all, w_cols, og, ou, od,
               xn, ctxb, abuf, gate, idf, rope,
               lsem, rawsem, cls, als, cs, cr, cfs, cfr, as_, ar, afs, afr, hs, hr, hfs, hfr, ws, wr, wxs, wxr, wfs, wfr,
               wds, wdr, ins, inr, es, er, csem, xsem, usem, wsem, dsem, msem):
    t = lax.axis_index('tp')
    e = lax.axis_index('ep')
    core = odd(e)
    xc = e // 2
    tokens, d_model = xn.shape
    heads, hd = wq.shape[1], wq.shape[2]
    q = tokens // RING
    half = q // 2
    width = d_model // RING
    kblk = min(256, d_model)
    nk = d_model // kblk
    pair = 2 * hd
    pairs = heads // 2
    local, fe = eg.shape[0], eg.shape[1]
    top_k = ids.shape[0]
    partner = {'ep': xc * 2 + 1 - core}

    def ring(k):
        return lax.rem(k + RING, RING)

    def y_dev(k):
        return {'tp': ring(t + k)}

    def x_id(k):
        return ring(xc + k) * 2 + core

    def x_dev(k):
        return {'ep': x_id(k)}

    def w_swap(k):
        return rcopy(wo.at[window(e, hd), window(ring(t + k), width)], w_cols.at[e, t], ws.at[k - 1], wr.at[k - 1], y_dev(k))

    def w_round(side):
        return rcopy(w_cols.at[e], w_cols.at[e], wxs.at[side], wxr.at[side], x_dev(turn(side)))

    def w_forward(side):
        ref = w_cols.at[x_id(2 * side - 1), pl.ds(2 * side, 2)]
        return rcopy(ref, ref, wfs.at[side], wfr.at[side], x_dev(turn(side)))

    def w_core(k):
        return rcopy(w_cols.at[x_id(k)], w_cols.at[x_id(k)], wds.at[k], wdr.at[k], partner)

    def hid_send(part, side):
        rows = pl.ds(pl.multiple_of(t * q + part * half, half), half)
        return rcopy(x_ref.at[rows], hid_all.at[xc, part], hs.at[part, side], hr.at[part, side], x_dev(turn(side)))

    def hid_forward(part, side):
        ref = hid_all.at[ring(xc + 2 * side - 1), part, pl.ds(side * (half // 2), half // 2)]
        return rcopy(ref, ref, hfs.at[part, side], hfr.at[part, side], x_dev(turn(side)))

    def ids_send(k):
        return rcopy(ids.at[:, window(t, q)], ids_all.at[xc], ins.at[k - 1], inr.at[k - 1], x_dev(k))

    mats = ((eg, og), (eu, ou), (ed, od))

    def swap_mat(k, i):
        return rcopy(mats[i][0].at[k], mats[i][1].at[k], es.at[k, i], er.at[k, i], partner)

    def ctx_local(g):
        return pltpu.make_async_copy(ctxb.at[g], ctx_all.at[t, :, window(g, pair)], cls.at[g])

    def ctx_send(g, side):
        return rcopy(ctxb.at[g], ctx_all.at[t, :, window(g, pair)], cs.at[side, g], cr.at[side, g], y_dev(turn(side)))

    def ctx_forward(g, side):
        ref = ctx_all.at[ring(t + 2 * side - 1), pl.ds(side * (tokens // 2), tokens // 2), window(g, pair)]
        return rcopy(ref, ref, cfs.at[side, g], cfr.at[side, g], y_dev(turn(side)))

    def ctx_pass(g):
        for side in SIDES:
            ctx_send(g, side).wait_recv()
            ctx_forward(g, side).start()

    def a_local(c):
        return pltpu.make_async_copy(abuf.at[c], a_full.at[window(c, q), window(t, width)], als.at[c])

    def a_send(c, side):
        return rcopy(abuf.at[c], a_full.at[window(c, q), window(t, width)], as_.at[side, c], ar.at[side, c], y_dev(turn(side)))

    def a_forward(c, side):
        rows = pl.ds(pl.multiple_of(c * q + side * half, half), half)
        ref = a_full.at[rows, window(ring(t + 2 * side - 1), width)]
        return rcopy(ref, ref, afs.at[side, c], afr.at[side, c], y_dev(turn(side)))

    def a_pass(c):
        for side in SIDES:
            a_send(c, side).wait_recv()
            a_forward(c, side).start()

    load_x = [pltpu.make_async_copy(x_ref.at[pl.ds(k * q, q)], xn.at[pl.ds(k * q, q)], lsem.at[k]) for k in range(RING)]
    for c in load_x:
        c.start()
    w_own = pltpu.make_async_copy(wo.at[window(e, hd), window(t, width)], w_cols.at[e, t], lsem.at[RING])
    ids_own = pltpu.make_async_copy(ids.at[:, window(t, q)], ids_all.at[xc], lsem.at[RING + 1])

    def attention(raw, wide, wb, qb, kb, vb):
        proj = (wq, wk, wv)

        def raw_load(m, k):
            return pltpu.make_async_copy(proj[m].at[window(k, kblk)], raw.at[odd(k)], rawsem.at[odd(k)])
        for k in SIDES:
            raw_load(0, k).start()
        entry_barrier((y_dev(1), y_dev(-1), y_dev(2), x_dev(1), x_dev(-1), x_dev(2), partner))
        w_own.start()
        ids_own.start()
        for k in range(1, RING):
            w_swap(k).start()
            ids_send(k).start()
        for side in SIDES:
            hid_send(0, side).start()
        for i in range(len(mats)):
            swap_mat(0, i).start()

        sign = jnp.where(lax.broadcasted_iota(jnp.int32, (1, hd), 1) < hd // 2, -1.0, 1.0)
        steps = min(128, tokens)

        def angles(k):
            angle = (lax.broadcasted_iota(jnp.int32, (steps, 1), 0) + k * steps).astype(F32) * freq[...]
            rope[0, window(k, steps)] = jnp.cos(angle)
            rope[1, window(k, steps)] = jnp.sin(angle) * sign
        loop(tokens // steps, angles)

        for k in range(RING):
            load_x[k].wait()
            norm_rows(xn.at[pl.ds(k * q, q)], xn.at[pl.ds(k * q, q)], attn_gain, q, 16)

        for m in range(len(proj)):
            def one(k, m=m):
                raw_load(m, k).wait()
                wide[...] = raw[odd(k)].astype(F32).reshape(kblk * heads, hd)

                @pl.when(k + 2 < nk)
                def _():
                    raw_load(m, k + 2).start()
                for h in range(heads):
                    wb[m, window(k, kblk), h * hd:(h + 1) * hd] = wide[pl.ds(h, kblk, stride=heads), :].astype(BF16)
            loop(nk, one)
            if m + 1 < len(proj):
                for k in SIDES:
                    raw_load(m + 1, k).start()

        w_own.wait()
        for k in range(1, RING):
            w_swap(k).wait_recv()
        for side in SIDES:
            w_round(side).start()
        w_core(0).start()

        scale = hd ** -0.5
        tri = lax.broadcasted_iota(jnp.int32, (q, q), 0) >= lax.broadcasted_iota(jnp.int32, (q, q), 1)

        def heads_of(g):
            for m, dst in enumerate((qb, kb, vb)):
                r = jnp.dot(xn[...], wb[m, :, window(g, pair)], preferred_element_type=F32)
                if dst is vb:
                    dst[...] = r.astype(BF16)
                else:
                    for h in SIDES:
                        part = r[:, h * hd:(h + 1) * hd]
                        turned = part * rope[0] + pltpu.roll(part, hd // 2, 1) * rope[1]
                        dst[:, h * hd:(h + 1) * hd] = turned.astype(BF16)
            for h in SIDES:
                hc = slice(h * hd, (h + 1) * hd)
                for b in range(RING):
                    s = lax.dot_general(qb[b * q:(b + 1) * q, hc], kb[0:(b + 1) * q, hc], NT, preferred_element_type=F32) * scale
                    diag = jnp.where(tri, s[:, b * q:], -1e30)
                    s = diag if b == 0 else jnp.concatenate([s[:, :b * q], diag], axis=1)
                    w = jnp.exp(s - jnp.max(s, axis=-1, keepdims=True))
                    prob = (w * (1.0 / jnp.sum(w, axis=-1, keepdims=True))).astype(BF16)
                    ctxb[g, b * q:(b + 1) * q, hc] = jnp.dot(prob, vb[0:(b + 1) * q, hc], preferred_element_type=F32).astype(BF16)
            ctx_local(g).start()
            for side in SIDES:
                ctx_send(g, side).start()

            @pl.when(g == 0)
            def _():
                for side in SIDES:
                    hid_send(0, side).wait_recv()
                    hid_forward(0, side).start()

            @pl.when(g >= 2)
            def _():
                ctx_pass(g - 2)

            @pl.when(g == 2)
            def _():
                for side in SIDES:
                    w_round(side).wait_recv()
                    w_forward(side).start()
                w_core(1).start()
                w_core(RING - 1).start()

            @pl.when(g == pairs - 1)
            def _():
                for side in SIDES:
                    hid_send(1, side).start()
        loop(pairs, heads_of)

    pl.run_scoped(attention, pltpu.VMEM((2, kblk, heads, hd), BF16), pltpu.VMEM((kblk * heads, hd), F32),
                  pltpu.VMEM((len(SIDES) + 1, d_model, heads * hd), BF16), *[pltpu.VMEM((tokens, pair), BF16)] * (len(SIDES) + 1))

    def experts(wcv, cbuf, xbuf, mv, act, wbuf, dbuf):
        fb = wbuf.shape[2]
        sizes = [fb] * (fe // fb) + [fe % fb]
        nb = len(sizes)
        cw = dbuf.shape[2]
        nn = d_model // cw
        passes = 4 * local
        last = passes - 2

        def expert_of(p):
            late = p // last
            return (1 - late) * lax.rem(p, 3) + late * 3

        def half_of(p):
            late = p // last
            return (1 - late) * (p // 3) + late * (p - last)

        def w_load(k, b, slot, own):
            k = k if own else k - local
            rows = pl.ds(b * fb, sizes[b])
            return [pltpu.make_async_copy(ref.at[k, rows], wbuf.at[slot, i, pl.ds(0, sizes[b])], wsem.at[slot, i])
                    for i, ref in enumerate((eg, eu) if own else (og, ou))]

        def d_load(k, n, own):
            return pltpu.make_async_copy((ed if own else od).at[k if own else k - local, :, window(n, cw)], dbuf.at[odd(n)], dsem.at[odd(n)])

        def either(p, start):
            k = expert_of(p)

            @pl.when(jnp.logical_and(p < passes, k < local))
            def _():
                start(k, True)

            @pl.when(jnp.logical_and(p < passes, k >= local))
            def _():
                start(k, False)

        def w_start(p, b):
            def go(k, own):
                for c in w_load(k, b, odd(p * nb + b), own):
                    c.start()
            either(p, go)

        def d_start(p, n):
            either(p, lambda k, own: d_load(k, n, own).start())

        def u_rows(part, k):
            return xn.at[pl.ds(pl.multiple_of((part * RING + k) * half, half), half)]

        def u_ready(part):
            for k in range(RING):
                @pl.when(k == xc)
                def _():
                    rows = pl.ds(pl.multiple_of(t * q + part * half, half), half)
                    pltpu.make_async_copy(x_ref.at[rows], u_rows(part, k), usem.at[k]).start()

                @pl.when(k != xc)
                def _():
                    pltpu.make_async_copy(hid_all.at[k, part], u_rows(part, k), usem.at[k]).start()
            for k in range(RING):
                pltpu.make_async_copy(hid_all.at[k, part], u_rows(part, k), usem.at[k]).wait()
            rows = RING * half
            u = xn.at[pl.ds(part * rows, rows)]
            norm_rows(u, u, moe_gain, rows, 16)
            logits = lax.dot_general(u[...], router[...], NT, preferred_element_type=F32)
            lane = lax.broadcasted_iota(jnp.int32, logits.shape, 1).astype(F32)
            picks = jnp.concatenate([idf[k, :, part * half:(part + 1) * half].astype(F32) for k in range(RING)], axis=1).T
            chosen = lane == picks[:, 0:1]
            for j in range(1, top_k):
                chosen = jnp.logical_or(chosen, lane == picks[:, j:j + 1])
            top = jnp.max(jnp.where(chosen, logits, -jnp.inf), axis=-1, keepdims=True)
            w = jnp.where(chosen, jnp.exp(jnp.where(chosen, logits - top, 0.0)), 0.0)
            gate[part] = w / jnp.sum(w, axis=-1, keepdims=True)

        def ctx_load(c):
            return [pltpu.make_async_copy(ctx_all.at[k, window(c, q)], cbuf.at[odd(c), :, pl.ds(k * heads * hd, heads * hd)], csem.at[odd(c), k]) for k in range(RING)]

        def x_load(c):
            return pltpu.make_async_copy(x_ref.at[window(c, q), window(t, width)], xbuf.at[odd(c)], xsem.at[odd(c)])

        load_w = [pltpu.make_async_copy(w_cols.at[:, k], wcv.at[k], lsem.at[k]) for k in range(RING)]

        def attention_out():
            for side in SIDES:
                for g in range(pairs):
                    ctx_forward(g, side).wait_recv()
            for g in range(pairs):
                ctx_local(g).wait()
            for c in ctx_load(jnp.int32(0)):
                c.start()
            x_load(jnp.int32(0)).start()
            for c in load_w:
                c.wait()

            def chunk(c):
                @pl.when(c + 1 < RING)
                def _():
                    for d in ctx_load(c + 1):
                        d.start()
                    x_load(c + 1).start()
                for d in ctx_load(c):
                    d.wait()
                x_load(c).wait()
                o = jnp.dot(cbuf[odd(c)], wcv[...].reshape(RING * heads * hd, width), preferred_element_type=F32)
                abuf[c] = (xbuf[odd(c)].astype(F32) + o).astype(BF16)
                a_local(c).start()
                for side in SIDES:
                    a_send(c, side).start()
            loop(RING, chunk)

        def m_out(part, n):
            return pltpu.make_async_copy(mv.at[part, n], m_part.at[:, part, :, window(n, cw)], msem.at[part, n])

        for b in SIDES:
            w_start(jnp.int32(0), b)
            d_start(jnp.int32(0), jnp.int32(b))
        ids_own.wait()
        for k in range(1, RING):
            ids_send(k).wait_recv()
        load_i = pltpu.make_async_copy(ids_all, idf.at[:, pl.ds(0, top_k)], lsem.at[RING + 1])
        load_i.start()
        for side in SIDES:
            hid_forward(0, side).wait_recv()
        load_i.wait()
        u_ready(0)

        def one_pass(p):
            @pl.when(p == 1)
            def _():
                ctx_pass(pairs - 2)
                for side in SIDES:
                    w_forward(side).wait_recv()
                w_core(2).start()
                for i in range(len(mats)):
                    swap_mat(1, i).start()

            @pl.when(p == 2)
            def _():
                for k in range(RING):
                    w_core(k).wait_recv()
                for c in load_w:
                    c.start()

            @pl.when(p == 3)
            def _():
                ctx_pass(pairs - 1)
                for side in SIDES:
                    hid_send(1, side).wait_recv()
                    hid_forward(1, side).start()
                attention_out()
                for side in SIDES:
                    hid_forward(1, side).wait_recv()
                u_ready(1)

            @pl.when(p >= RING)
            def _():
                a_pass(p - RING)
            k, part = expert_of(p), half_of(p)
            which = (k // local) * ((e + 1 - 2 * core) * local + k - local) + (1 - k // local) * (e * local + k)
            rows = RING * half
            u = xn.at[pl.ds(pl.multiple_of(part * rows, rows), rows)]
            lane = lax.broadcasted_iota(jnp.int32, gate.shape[1:], 1)
            weight = jnp.sum(jnp.where(lane == which, gate[part], 0.0), axis=1, keepdims=True)

            def arrived(which_mats):
                for late, when in enumerate((1, last - 1)):
                    @pl.when(p == when)
                    def _():
                        for i in which_mats:
                            swap_mat(late, i).wait_recv()
            for b, size in enumerate(sizes):
                slot = odd(p * nb + b)
                for c in w_load(0, b, slot, True):
                    c.wait()
                g = lax.dot_general(u[...], wbuf[slot, 0, 0:size], NT, preferred_element_type=F32)
                v = lax.dot_general(u[...], wbuf[slot, 1, 0:size], NT, preferred_element_type=F32)
                act[:, b * fb:b * fb + size] = (jax.nn.silu(g) * v).astype(BF16)
                nxt = b + 2
                if nxt == nb:
                    arrived(SIDES)
                w_start(p + nxt // nb, nxt % nb)

            def block(n):
                d_load(0, n, True).wait()
                y = jnp.dot(act[...], dbuf[odd(n)], preferred_element_type=F32).astype(BF16)
                term = jnp.where(weight > 0.0, weight * y.astype(F32), 0.0).reshape(mv.shape[2:])

                @pl.when(n + 2 < nn)
                def _():
                    d_start(p, n + 2)

                @pl.when(n + 2 == nn)
                def _():
                    arrived((2,))

                @pl.when(n + 2 >= nn)
                def _():
                    d_start(p + 1, n + 2 - nn)

                @pl.when(k == 0)
                def _():
                    mv[part, n] = term

                @pl.when(k > 0)
                def _():
                    mv[part, n] = mv[part, n] + term

                @pl.when(p >= last)
                def _():
                    m_out(part, n).start()
            loop(nn, block)
        loop(passes, one_pass)

        def finish(n):
            for part in SIDES:
                m_out(part, n).wait()
        loop(nn, finish)

    fb = 256 if fe > 512 else 128
    cw = min(512, d_model // 4)
    pl.run_scoped(experts, pltpu.VMEM((RING, 8, hd, width), BF16), pltpu.VMEM((2, q, RING * heads * hd), BF16), pltpu.VMEM((2, q, width), BF16),
                  pltpu.VMEM((2, d_model // cw, RING, half, cw), F32), pltpu.VMEM((RING * half, fe), BF16),
                  pltpu.VMEM((2, 2, fb, d_model), BF16), pltpu.VMEM((2, fe, cw), BF16))

    for side in SIDES:
        w_round(side).wait_send()
        w_forward(side).wait_send()
        for part in SIDES:
            hid_send(part, side).wait_send()
            hid_forward(part, side).wait_send()
        for g in range(pairs):
            ctx_send(g, side).wait_send()
            ctx_forward(g, side).wait_send()
        for c in range(RING):
            a_send(c, side).wait_send()
            a_forward(c, side).wait()
    for k in range(1, RING):
        w_swap(k).wait_send()
        ids_send(k).wait_send()
    for k in SIDES:
        for i in range(len(mats)):
            swap_mat(k, i).wait_send()
    for k in range(RING):
        w_core(k).wait_send()
        a_local(k).wait()


def front_call(x, wq, wk, wv, wo, eg, eu, ed, attn_gain, moe_gain, ids, router):
    tokens, d_model = x.shape
    heads, hd = wq.shape[1], wq.shape[2]
    q = tokens // RING
    local, fe = eg.shape[0], eg.shape[1]
    experts = router.shape[0]
    pairs = heads // 2
    hbm = pl.BlockSpec(memory_space=pl.ANY)
    vmem = pl.BlockSpec(memory_space=pltpu.VMEM)
    dma = pltpu.SemaphoreType.DMA
    sds = jax.ShapeDtypeStruct
    freq = ROPE_BASE ** (np.arange(hd) % (hd // 2) * (-2.0 / hd))
    freq = jnp.asarray(freq.astype(np.float32).reshape(1, hd))
    two, three, four = dma((2,)), dma((3,)), dma((RING,))
    by_pair, by_chunk, square = dma((2, pairs)), dma((2, RING)), dma((2, 2))
    outs = pl.pallas_call(
        front_body,
        out_shape=(sds((tokens, d_model), BF16), sds((RING, 2, q // 2, d_model), F32), sds((RING, tokens, heads * hd), BF16),
                   sds((RING, 2, q // 2, d_model), BF16), sds((RING, ids.shape[0], q), ids.dtype), sds((8, RING, hd, d_model // RING), BF16),
                   sds(eg.shape, BF16), sds(eu.shape, BF16), sds(ed.shape, BF16)),
        in_specs=[hbm] * 8 + [vmem] * 3 + [hbm, vmem],
        out_specs=(hbm,) * 9,
        scratch_shapes=[
            pltpu.VMEM((tokens, d_model), BF16), pltpu.VMEM((pairs, tokens, 2 * hd), BF16), pltpu.VMEM((RING, q, d_model // RING), BF16),
            pltpu.VMEM((2, tokens // 2, experts), F32), pltpu.VMEM((RING, 8, q), ids.dtype),
            pltpu.VMEM((2, tokens, hd), F32),
            dma((RING + 2,)), two, dma((pairs,)), four,
        ] + [by_pair] * RING + [by_chunk] * RING + [square] * RING + [three] * 2 + [two] * RING + [four] * 2 + [three] * 2
          + [dma((2, 3))] * 2 + [by_chunk, two, four, square, two, dma((2, 8))],
        compiler_params=pltpu.CompilerParams(collective_id=0, has_side_effects=True, vmem_limit_bytes=VMEM_LIMIT),
        cost_estimate=pl.CostEstimate(flops=2 * tokens * d_model * (heads * hd * RING + 12 * fe), bytes_accessed=24 * fe * d_model, transcendentals=heads * tokens * tokens),
        name='attn_moe',
    )(x, wq, wk, wv, wo, eg, eu, ed, attn_gain, moe_gain, freq, ids, router)
    return outs[0], outs[1]


def solution(mesh):
    tok_spec = P(('dp', 'ep'))
    col_spec = P(None, 'tp')
    in_specs = (tok_spec,) * 3 + (P(),) + (col_spec,) * 3 + (P('tp'), P(), col_spec, col_spec, P('tp'), P(), P()) + (P('ep'),) * 3

    def layer_local(hidden_in, expert_ids, slot_ids, attn_gain, w_query, w_key, w_value, w_out, ffn_gain, w_gate, w_up, w_down, moe_gain, w_router, exp_gate, exp_up, exp_down):
        num_seqs, seq_len, d_model = hidden_in.shape
        tokens = num_seqs * seq_len
        heads, head_dim = w_out.shape[0], w_out.shape[1]
        x = hidden_in.reshape(tokens, d_model)
        ids = jnp.swapaxes(expert_ids, 1, 2).reshape(expert_ids.shape[2], tokens)
        after_attn, m_part = front_call(
            x, w_query, w_key, w_value, w_out.reshape(heads * head_dim, d_model), jnp.swapaxes(exp_gate, 1, 2), jnp.swapaxes(exp_up, 1, 2), exp_down,
            attn_gain, moe_gain, ids, w_router.T)
        out = ffn_call(after_attn, w_gate.T, w_up.T, w_down, ffn_gain, m_part.reshape(-1, tokens // 4, d_model))
        return out.reshape(hidden_in.shape)

    return jax.shard_map(layer_local, mesh=mesh, in_specs=in_specs, out_specs=tok_spec, check_vma=False)
```

```python
import functools

import jax
import jax.numpy as jnp
import numpy as np
from jax import lax
from jax.experimental import pallas as pl
from jax.experimental.pallas import tpu as pltpu
from jax.sharding import PartitionSpec as P

F32 = jnp.float32
BF16 = jnp.bfloat16
EPS = 1e-6
ROPE_BASE = 10000.0
VMEM_LIMIT = 67043328
MESH = pl.DeviceIdType.MESH
NT = (((1,), (1,)), ((), ()))


RING = 4
SIDES = (0, 1)


def odd(k):
    return lax.rem(k, 2)


def turn(side):
    return 1 - 2 * side


def loop(count, body):
    def step(k, carry):
        body(k)
        return carry
    lax.fori_loop(0, count, step, 0)


def window(index, size):
    return pl.ds(pl.multiple_of(index * size, size), size)


def rcopy(src, dst, ssem, rsem, dev):
    return pltpu.make_async_remote_copy(src_ref=src, dst_ref=dst, send_sem=ssem, recv_sem=rsem, device_id=dev, device_id_type=MESH)


def entry_barrier(neighbours):
    barrier = pltpu.get_barrier_semaphore()
    for dev in neighbours:
        pl.semaphore_signal(barrier, inc=1, device_id=dev, device_id_type=MESH)
    pl.semaphore_wait(barrier, len(neighbours))


def norm_rows(src, dst, gain, rows, step):
    def one(r):
        sl = window(r, step)
        x = src[sl, :].astype(F32)
        inv = lax.rsqrt(jnp.mean(x * x, axis=-1, keepdims=True) + EPS)
        dst[sl, :] = (x * inv * gain[...].astype(F32).reshape(1, -1)).astype(BF16)
    loop(rows // step, one)


def ffn_body(fb, a_ref, wg, wu, wd, gain, m_ref, out_ref,
             a_own, n2, h, wbuf, dbuf, p1, yrecv, xrecv, mbuf,
             asem, wsem, dsem, msem, osem, ys, yr, xs, xr, gs, gr, fs, fr):
    t = lax.axis_index('tp')
    e = lax.axis_index('ep')
    big = odd(e)
    xc = e // 2
    q = a_own.shape[0]
    d_model = a_own.shape[1]
    f_loc = wg.shape[0]
    cw = d_model // 8
    hw = cw // 2
    nf = f_loc // fb
    tail = f_loc - nf * fb
    yright, yleft = {'tp': lax.rem(t + 1, RING)}, {'tp': lax.rem(t + 3, RING)}
    xright, xleft = {'ep': lax.rem(xc + 1, RING) * 2 + big}, {'ep': lax.rem(xc + 3, RING) * 2 + big}

    def cols(cb):
        return window(cb, cw)

    def chunk(c):
        return lax.rem(c + 8, RING)

    def rows(c):
        return window(chunk(c), q)

    def a_load(c, slot):
        return pltpu.make_async_copy(a_ref.at[rows(c)], n2.at[pl.ds(slot * q, q)], asem.at[slot])
    load_own = pltpu.make_async_copy(a_ref.at[rows(t)], a_own, asem.at[2])

    def w_load(i, slot, size):
        sl = pl.ds(pl.multiple_of(i * fb, fb), size)
        return (pltpu.make_async_copy(wg.at[sl], wbuf.at[slot, 0, pl.ds(0, size)], wsem.at[slot, 0]),
                pltpu.make_async_copy(wu.at[sl], wbuf.at[slot, 1, pl.ds(0, size)], wsem.at[slot, 1]))

    def w_start(i):
        slot = lax.rem(i, wbuf.shape[0])

        @pl.when(i < nf)
        def _():
            for c in w_load(i, slot, fb):
                c.start()

        @pl.when(i == nf)
        def _():
            for c in w_load(nf, slot, tail):
                c.start()

    def col_of(j):
        return odd(j) * 4 + j // 2

    def d_load(jj):
        slot = lax.rem(jj, RING)
        start = pl.multiple_of(col_of(jj // 2) * cw + odd(jj) * hw, hw)
        return pltpu.make_async_copy(wd.at[:, pl.ds(start, hw)], dbuf.at[slot], dsem.at[slot])

    def m_load(k):
        s, j = k // 8 + 1, lax.rem(k, 8)
        side = odd(j)
        c = lax.rem(xc + (2 * side - 1) * (1 + s) + 8, RING)
        slot = odd(k)
        return pltpu.make_async_copy(m_ref.at[c, :, cols(col_of(j))], mbuf.at[slot], msem.at[slot])

    def send(buf, ssem, rsem, src, right, left, side, step, i):
        @pl.when(side == 0)
        def _():
            rcopy(src, buf.at[0, step, i], ssem.at[0, step, i], rsem.at[0, step, i], right).start()

        @pl.when(side == 1)
        def _():
            rcopy(src, buf.at[1, step, i], ssem.at[1, step, i], rsem.at[1, step, i], left).start()

    def ysend(src, side, step, i):
        send(yrecv, ys, yr, src, yright, yleft, side, step, i)

    def xsend(src, side, step, i):
        send(xrecv, xs, xr, src, xright, xleft, side, step, i)

    def arrived(buf, ssem, rsem, side, step, i, dev):
        rcopy(buf.at[side, step, i], buf.at[side, step, i], ssem.at[side, step, i], rsem.at[side, step, i], dev).wait_recv()

    def sent(buf, ssem, rsem, side, step, i, dev):
        rcopy(buf.at[side, step, i], buf.at[side, step, i], ssem.at[side, step, i], rsem.at[side, step, i], dev).wait_send()

    def xserve(k):
        s, j = k // 8, lax.rem(k, 8)
        side, i = odd(j), j // 2
        m_load(k + 1).start()
        m_load(k).wait()
        arrived(xrecv, xs, xr, side, s, i, xright)
        xrecv[side, s, i] = xrecv[side, s, i] + mbuf[odd(k)]
        xsend(xrecv.at[side, s, i], side, s + 1, i)

    def gate_up(serve):
        def block(i, size):
            slot = lax.rem(i, wbuf.shape[0])
            w_start(i + 2)
            for c in w_load(i, slot, size):
                c.wait()
            g = lax.dot_general(n2[...], wbuf[slot, 0, pl.ds(0, size)], NT, preferred_element_type=F32)
            u = lax.dot_general(n2[...], wbuf[slot, 1, pl.ds(0, size)], NT, preferred_element_type=F32)
            h[:, pl.ds(pl.multiple_of(i * fb, fb), size)] = (jax.nn.silu(g) * u).astype(BF16)

        def one(i):
            block(i, fb)
            serve(i)
        loop(nf, one)
        block(nf, tail)

    def down(ready, use):
        def one(jj):
            sub = odd(jj)

            @pl.when(jj + RING - 1 < 16)
            def _():
                d_load(jj + RING - 1).start()

            @pl.when(sub == 0)
            def _():
                ready(jj // 2)
            d_load(jj).wait()
            r = jnp.dot(h[...], dbuf[lax.rem(jj, RING)], preferred_element_type=F32)
            use(jj // 2, sub, pl.ds(pl.multiple_of(sub * hw, hw), hw), r)
        loop(16, one)

    def d_first():
        for k in range(RING - 1):
            d_load(jnp.int32(k)).start()

    a_load(t - 1, 0).start()
    a_load(t + 1, 1).start()
    w_start(0)
    w_start(1)
    entry_barrier((yright, yleft, xright, xleft))

    def x_first(i):
        xsend(m_ref.at[chunk(xc - 1), :, cols(i)], 0, 0, i)
        xsend(m_ref.at[chunk(xc + 1), :, cols(4 + i)], 1, 0, i)
    loop(4, x_first)
    d_first()
    m_load(0).start()
    load_own.start()

    for slot in SIDES:
        a_load(t, slot).wait()
        norm_rows(n2.at[pl.ds(slot * q, q)], n2.at[pl.ds(slot * q, q)], gain, q, 16)
    gate_up(lambda i: None)
    a_load(t + 2, 0).start()
    a_load(t, 1).start()
    w_start(0)
    w_start(1)

    def use1(j, sub, part, r):
        p1[col_of(j), :, part] = r
        side, i = odd(j), j // 2

        @pl.when(sub == 1)
        def _():
            ysend(p1.at[col_of(j), window(side, q)], side, 0, i)
    down(lambda j: None, use1)
    d_first()

    for slot in SIDES:
        a_load(t, slot).wait()
        norm_rows(n2.at[pl.ds(slot * q, q)], n2.at[pl.ds(slot * q, q)], gain, q, 16)

    def serve2(i):
        @pl.when(i < 8)
        def _():
            xserve(i)
    gate_up(serve2)
    for k in range(min(nf, 8), 8):
        xserve(k)

    def sent_rows(j):
        return pl.ds(pl.multiple_of(odd(j) * q, q), q)

    def ready2(j):
        arrived(yrecv, ys, yr, odd(j), 0, j // 2, yright)
        sent(yrecv, ys, yr, odd(j), 0, j // 2, yright)

    def use2(j, sub, part, r):
        side, i = odd(j), j // 2
        p1[col_of(j), sent_rows(j), part] = r[q:]
        yrecv[side, 0, i, :, part] = yrecv[side, 0, i, :, part] + r[:q]

        @pl.when(sub == 1)
        def _():
            ysend(yrecv.at[side, 0, i], side, 1, i)
    down(ready2, use2)

    def third(j):
        side, i = odd(j), j // 2
        xserve(8 + j)
        arrived(yrecv, ys, yr, side, 1, i, yright)
        yrecv[side, 1, i] = yrecv[side, 1, i] + p1[col_of(j), window((1 - side), q)]
        ysend(yrecv.at[side, 1, i], side, 2, i)
    loop(8, third)

    def out_local(cb):
        return pltpu.make_async_copy(n2.at[pl.ds(0, q), cols(cb)], out_ref.at[rows(t), cols(cb)], osem.at[cb])

    def gather(cb, side, dev):
        return rcopy(n2.at[pl.ds(0, q), cols(cb)], out_ref.at[rows(t), cols(cb)], gs.at[side, cb], gr.at[side, cb], dev)

    load_own.wait()

    def last(j):
        side, i = odd(j), j // 2
        cb = col_of(j)
        k = 16 + j

        @pl.when(j + 1 < 8)
        def _():
            m_load(k + 1).start()
        m_load(k).wait()
        arrived(xrecv, xs, xr, side, 2, i, xright)
        arrived(yrecv, ys, yr, side, 2, i, yright)
        b_val = a_own[:, cols(cb)].astype(F32) + (yrecv[side, 2, i] + p1[cb, sent_rows(j)])
        n2[pl.ds(0, q), cols(cb)] = (b_val + (xrecv[side, 2, i] + mbuf[odd(k)])).astype(BF16)
        out_local(cb).start()
        gather(cb, 0, yright).start()
        gather(cb, 1, yleft).start()
    loop(8, last)

    half = q // 2

    def half_rows(c, which):
        return pl.ds(pl.multiple_of(chunk(c) * q + which * half, half), half)

    def forward(c, which, cb, dev):
        ref = out_ref.at[half_rows(c, which), cols(cb)]
        return rcopy(ref, ref, fs.at[which, cb], fr.at[which, cb], dev)

    def pass_on(j):
        cb = col_of(j)
        gather(cb, 0, yright).wait_recv()
        forward(t - 1, 0, cb, yright).start()
        gather(cb, 1, yleft).wait_recv()
        forward(t + 1, 1, cb, yleft).start()
    loop(8, pass_on)

    def finish(j):
        cb = col_of(j)
        out_local(cb).wait()
        for which in SIDES:
            gather(cb, which, yright).wait_send()
            forward(t, which, cb, yright).wait_send()
            forward(t, which, cb, yright).wait_recv()
    loop(8, finish)

    def drain(k):
        step, j = k // 8, lax.rem(k, 8)

        @pl.when(step > 0)
        def _():
            sent(yrecv, ys, yr, odd(j), step, j // 2, yright)
        sent(xrecv, xs, xr, odd(j), step, j // 2, yright)
    loop(24, drain)


def ffn_call(after_attn, wg_t, wu_t, w_down, gain, m_part):
    tokens, d_model = after_attn.shape
    f_loc = wg_t.shape[0]
    fb = 256 if f_loc > 512 else 128
    q = tokens // 4
    cw = d_model // 8
    hbm = pl.BlockSpec(memory_space=pl.ANY)
    vmem = pl.BlockSpec(memory_space=pltpu.VMEM)
    dma = pltpu.SemaphoreType.DMA
    flops = 2 * tokens * d_model * f_loc * 3
    return pl.pallas_call(
        functools.partial(ffn_body, fb),
        out_shape=jax.ShapeDtypeStruct((tokens, d_model), BF16),
        in_specs=[hbm, hbm, hbm, hbm, vmem, hbm],
        out_specs=hbm,
        scratch_shapes=[
            pltpu.VMEM((q, d_model), BF16),
            pltpu.VMEM((2 * q, d_model), BF16),
            pltpu.VMEM((2 * q, f_loc), BF16),
            pltpu.VMEM((3, 2, fb, d_model), BF16),
            pltpu.VMEM((RING, f_loc, cw // 2), BF16),
            pltpu.VMEM((8, 2 * q, cw), F32),
            pltpu.VMEM((2, 3, RING, q, cw), F32),
            pltpu.VMEM((2, 3, RING, q, cw), F32),
            pltpu.VMEM((2, q, cw), F32),
            dma((3,)), dma((3, 2)), dma((RING,)), dma((2,)), dma((8,)),
        ] + [dma((2, 3, RING))] * RING + [dma((2, 8))] * RING,
        compiler_params=pltpu.CompilerParams(collective_id=2, has_side_effects=True, vmem_limit_bytes=VMEM_LIMIT),
        cost_estimate=pl.CostEstimate(flops=flops, bytes_accessed=4 * tokens * d_model + 12 * f_loc * d_model, transcendentals=tokens * f_loc),
        name='ffn_ring',
    )(after_attn, wg_t, wu_t, w_down, gain, m_part)


def front_body(x_ref, wq, wk, wv, wo, eg, eu, ed, attn_gain, moe_gain, freq, ids, router,
               a_full, m_part, ctx_all, hid_all, ids_all, w_cols, og, ou, od,
               xn, ctxb, abuf, gate, idf, rope,
               lsem, rawsem, cls, als, cs, cr, cfs, cfr, as_, ar, afs, afr, hs, hr, hfs, hfr, ws, wr, wxs, wxr, wfs, wfr,
               wds, wdr, ins, inr, es, er, csem, xsem, usem, wsem, dsem, msem):
    t = lax.axis_index('tp')
    e = lax.axis_index('ep')
    core = odd(e)
    xc = e // 2
    tokens, d_model = xn.shape
    heads, hd = wq.shape[1], wq.shape[2]
    q = tokens // RING
    half = q // 2
    width = d_model // RING
    kblk = min(256, d_model)
    nk = d_model // kblk
    pair = 2 * hd
    pairs = heads // 2
    local, fe = eg.shape[0], eg.shape[1]
    top_k = ids.shape[0]
    partner = {'ep': xc * 2 + 1 - core}

    def ring(k):
        return lax.rem(k + RING, RING)

    def y_dev(k):
        return {'tp': ring(t + k)}

    def x_id(k):
        return ring(xc + k) * 2 + core

    def x_dev(k):
        return {'ep': x_id(k)}

    def w_swap(k):
        return rcopy(wo.at[window(e, hd), window(ring(t + k), width)], w_cols.at[e, t], ws.at[k - 1], wr.at[k - 1], y_dev(k))

    def w_round(side):
        return rcopy(w_cols.at[e], w_cols.at[e], wxs.at[side], wxr.at[side], x_dev(turn(side)))

    def w_forward(side):
        ref = w_cols.at[x_id(2 * side - 1), pl.ds(2 * side, 2)]
        return rcopy(ref, ref, wfs.at[side], wfr.at[side], x_dev(turn(side)))

    def w_core(k):
        return rcopy(w_cols.at[x_id(k)], w_cols.at[x_id(k)], wds.at[k], wdr.at[k], partner)

    def hid_send(part, side):
        rows = pl.ds(pl.multiple_of(t * q + part * half, half), half)
        return rcopy(x_ref.at[rows], hid_all.at[xc, part], hs.at[part, side], hr.at[part, side], x_dev(turn(side)))

    def hid_forward(part, side):
        ref = hid_all.at[ring(xc + 2 * side - 1), part, pl.ds(side * (half // 2), half // 2)]
        return rcopy(ref, ref, hfs.at[part, side], hfr.at[part, side], x_dev(turn(side)))

    def ids_send(k):
        return rcopy(ids.at[:, window(t, q)], ids_all.at[xc], ins.at[k - 1], inr.at[k - 1], x_dev(k))

    mats = ((eg, og), (eu, ou), (ed, od))

    def swap_mat(k, i):
        return rcopy(mats[i][0].at[k], mats[i][1].at[k], es.at[k, i], er.at[k, i], partner)

    def ctx_local(g):
        return pltpu.make_async_copy(ctxb.at[g], ctx_all.at[t, :, window(g, pair)], cls.at[g])

    def ctx_send(g, side):
        return rcopy(ctxb.at[g], ctx_all.at[t, :, window(g, pair)], cs.at[side, g], cr.at[side, g], y_dev(turn(side)))

    def ctx_forward(g, side):
        ref = ctx_all.at[ring(t + 2 * side - 1), pl.ds(side * (tokens // 2), tokens // 2), window(g, pair)]
        return rcopy(ref, ref, cfs.at[side, g], cfr.at[side, g], y_dev(turn(side)))

    def ctx_pass(g):
        for side in SIDES:
            ctx_send(g, side).wait_recv()
            ctx_forward(g, side).start()

    def a_local(c):
        return pltpu.make_async_copy(abuf.at[c], a_full.at[window(c, q), window(t, width)], als.at[c])

    def a_send(c, side):
        return rcopy(abuf.at[c], a_full.at[window(c, q), window(t, width)], as_.at[side, c], ar.at[side, c], y_dev(turn(side)))

    def a_forward(c, side):
        rows = pl.ds(pl.multiple_of(c * q + side * half, half), half)
        ref = a_full.at[rows, window(ring(t + 2 * side - 1), width)]
        return rcopy(ref, ref, afs.at[side, c], afr.at[side, c], y_dev(turn(side)))

    def a_pass(c):
        for side in SIDES:
            a_send(c, side).wait_recv()
            a_forward(c, side).start()

    load_x = [pltpu.make_async_copy(x_ref.at[pl.ds(k * q, q)], xn.at[pl.ds(k * q, q)], lsem.at[k]) for k in range(RING)]
    for c in load_x:
        c.start()
    w_own = pltpu.make_async_copy(wo.at[window(e, hd), window(t, width)], w_cols.at[e, t], lsem.at[RING])
    ids_own = pltpu.make_async_copy(ids.at[:, window(t, q)], ids_all.at[xc], lsem.at[RING + 1])

    def attention(raw, wide, wb, qb, kb, vb):
        proj = (wq, wk, wv)

        deep = raw.shape[0]

        def raw_load(m, k):
            slot = lax.rem(k, deep)
            return pltpu.make_async_copy(proj[m].at[window(k, kblk)], raw.at[slot], rawsem.at[slot])
        for k in range(deep):
            raw_load(0, k).start()
        entry_barrier((y_dev(1), y_dev(-1), y_dev(2), x_dev(1), x_dev(-1), x_dev(2), partner))
        w_own.start()
        ids_own.start()
        for k in range(1, RING):
            w_swap(k).start()
            ids_send(k).start()
        for side in SIDES:
            hid_send(0, side).start()
        for i in range(len(mats)):
            swap_mat(0, i).start()

        sign = jnp.where(lax.broadcasted_iota(jnp.int32, (1, hd), 1) < hd // 2, -1.0, 1.0)
        steps = min(128, tokens)

        def angles(k):
            angle = (lax.broadcasted_iota(jnp.int32, (steps, 1), 0) + k * steps).astype(F32) * freq[...]
            rope[0, window(k, steps)] = jnp.cos(angle)
            rope[1, window(k, steps)] = jnp.sin(angle) * sign
        loop(tokens // steps, angles)

        for k in range(RING):
            load_x[k].wait()
            norm_rows(xn.at[pl.ds(k * q, q)], xn.at[pl.ds(k * q, q)], attn_gain, q, 16)

        for m in range(len(proj)):
            def one(k, m=m):
                raw_load(m, k).wait()
                wide[...] = raw[lax.rem(k, deep)].astype(F32).reshape(kblk * heads, hd)

                @pl.when(k + deep < nk)
                def _():
                    raw_load(m, k + deep).start()

                if m + 1 < len(proj):
                    @pl.when(k + deep >= nk)
                    def _():
                        raw_load(m + 1, k + deep - nk).start()
                for h in range(heads):
                    wb[m, window(k, kblk), h * hd:(h + 1) * hd] = wide[pl.ds(h, kblk, stride=heads), :].astype(BF16)
            loop(nk, one)

        w_own.wait()
        for k in range(1, RING):
            w_swap(k).wait_recv()
        for side in SIDES:
            w_round(side).start()
        w_core(0).start()

        scale = hd ** -0.5
        tri = lax.broadcasted_iota(jnp.int32, (q, q), 0) >= lax.broadcasted_iota(jnp.int32, (q, q), 1)

        def heads_of(g):
            for m, dst in enumerate((qb, kb, vb)):
                r = jnp.dot(xn[...], wb[m, :, window(g, pair)], preferred_element_type=F32)
                if dst is vb:
                    dst[...] = r.astype(BF16)
                else:
                    for h in SIDES:
                        part = r[:, h * hd:(h + 1) * hd]
                        turned = part * rope[0] + pltpu.roll(part, hd // 2, 1) * rope[1]
                        dst[:, h * hd:(h + 1) * hd] = turned.astype(BF16)
            for h in SIDES:
                hc = slice(h * hd, (h + 1) * hd)
                for b in range(RING):
                    s = lax.dot_general(qb[b * q:(b + 1) * q, hc], kb[0:(b + 1) * q, hc], NT, preferred_element_type=F32) * scale
                    diag = jnp.where(tri, s[:, b * q:], -1e30)
                    s = diag if b == 0 else jnp.concatenate([s[:, :b * q], diag], axis=1)
                    w = jnp.exp(s - jnp.max(s, axis=-1, keepdims=True))
                    prob = (w * (1.0 / jnp.sum(w, axis=-1, keepdims=True))).astype(BF16)
                    ctxb[g, b * q:(b + 1) * q, hc] = jnp.dot(prob, vb[0:(b + 1) * q, hc], preferred_element_type=F32).astype(BF16)
            ctx_local(g).start()
            for side in SIDES:
                ctx_send(g, side).start()

            @pl.when(g == 0)
            def _():
                for side in SIDES:
                    hid_send(0, side).wait_recv()
                    hid_forward(0, side).start()

            @pl.when(g >= 2)
            def _():
                ctx_pass(g - 2)

            @pl.when(g == 2)
            def _():
                for side in SIDES:
                    w_round(side).wait_recv()
                    w_forward(side).start()
                w_core(1).start()
                w_core(RING - 1).start()

            @pl.when(g == pairs - 1)
            def _():
                for side in SIDES:
                    hid_send(1, side).start()
        loop(pairs, heads_of)

    pl.run_scoped(attention, pltpu.VMEM((8, kblk, heads, hd), BF16), pltpu.VMEM((kblk * heads, hd), F32),
                  pltpu.VMEM((len(SIDES) + 1, d_model, heads * hd), BF16), *[pltpu.VMEM((tokens, pair), BF16)] * (len(SIDES) + 1))

    def experts(wcv, cbuf, xbuf, mv, act, wbuf, dbuf):
        fb = wbuf.shape[2]
        sizes = [fb] * (fe // fb) + [fe % fb]
        nb = len(sizes)
        cw = dbuf.shape[2]
        nn = d_model // cw
        passes = 4 * local
        last = passes - 2

        def expert_of(p):
            late = p // last
            return (1 - late) * lax.rem(p, 3) + late * 3

        def half_of(p):
            late = p // last
            return (1 - late) * (p // 3) + late * (p - last)

        def w_load(k, b, slot, own):
            k = k if own else k - local
            rows = pl.ds(b * fb, sizes[b])
            return [pltpu.make_async_copy(ref.at[k, rows], wbuf.at[slot, i, pl.ds(0, sizes[b])], wsem.at[slot, i])
                    for i, ref in enumerate((eg, eu) if own else (og, ou))]

        def d_load(k, n, own):
            return pltpu.make_async_copy((ed if own else od).at[k if own else k - local, :, window(n, cw)], dbuf.at[lax.rem(n, RING)], dsem.at[lax.rem(n, RING)])

        def either(p, start):
            k = expert_of(p)

            @pl.when(jnp.logical_and(p < passes, k < local))
            def _():
                start(k, True)

            @pl.when(jnp.logical_and(p < passes, k >= local))
            def _():
                start(k, False)

        def w_start(p, b):
            def go(k, own):
                for c in w_load(k, b, b, own):
                    c.start()
            either(p, go)

        def d_start(p, n):
            either(p, lambda k, own: d_load(k, n, own).start())

        def u_rows(part, k):
            return xn.at[pl.ds(pl.multiple_of((part * RING + k) * half, half), half)]

        def u_ready(part):
            for k in range(RING):
                @pl.when(k == xc)
                def _():
                    rows = pl.ds(pl.multiple_of(t * q + part * half, half), half)
                    pltpu.make_async_copy(x_ref.at[rows], u_rows(part, k), usem.at[k]).start()

                @pl.when(k != xc)
                def _():
                    pltpu.make_async_copy(hid_all.at[k, part], u_rows(part, k), usem.at[k]).start()
            for k in range(RING):
                pltpu.make_async_copy(hid_all.at[k, part], u_rows(part, k), usem.at[k]).wait()
            rows = RING * half
            u = xn.at[pl.ds(part * rows, rows)]
            norm_rows(u, u, moe_gain, rows, 16)
            logits = lax.dot_general(u[...], router[...], NT, preferred_element_type=F32)
            lane = lax.broadcasted_iota(jnp.int32, logits.shape, 1).astype(F32)
            picks = jnp.concatenate([idf[k, :, part * half:(part + 1) * half].astype(F32) for k in range(RING)], axis=1).T
            chosen = lane == picks[:, 0:1]
            for j in range(1, top_k):
                chosen = jnp.logical_or(chosen, lane == picks[:, j:j + 1])
            top = jnp.max(jnp.where(chosen, logits, -jnp.inf), axis=-1, keepdims=True)
            w = jnp.where(chosen, jnp.exp(jnp.where(chosen, logits - top, 0.0)), 0.0)
            gate[part] = w / jnp.sum(w, axis=-1, keepdims=True)

        def ctx_load(c):
            return [pltpu.make_async_copy(ctx_all.at[k, window(c, q)], cbuf.at[odd(c), :, pl.ds(k * heads * hd, heads * hd)], csem.at[odd(c), k]) for k in range(RING)]

        def x_load(c):
            return pltpu.make_async_copy(x_ref.at[window(c, q), window(t, width)], xbuf.at[odd(c)], xsem.at[odd(c)])

        load_w = [pltpu.make_async_copy(w_cols.at[:, k], wcv.at[k], lsem.at[k]) for k in range(RING)]

        def attention_out():
            for side in SIDES:
                for g in range(pairs):
                    ctx_forward(g, side).wait_recv()
            for g in range(pairs):
                ctx_local(g).wait()
            for c in ctx_load(jnp.int32(0)):
                c.start()
            x_load(jnp.int32(0)).start()
            for c in load_w:
                c.wait()

            def chunk(c):
                @pl.when(c + 1 < RING)
                def _():
                    for d in ctx_load(c + 1):
                        d.start()
                    x_load(c + 1).start()
                for d in ctx_load(c):
                    d.wait()
                x_load(c).wait()
                o = jnp.dot(cbuf[odd(c)], wcv[...].reshape(RING * heads * hd, width), preferred_element_type=F32)
                abuf[c] = (xbuf[odd(c)].astype(F32) + o).astype(BF16)
                a_local(c).start()
                for side in SIDES:
                    a_send(c, side).start()
            loop(RING, chunk)

        def m_out(part, n):
            return pltpu.make_async_copy(mv.at[part, n], m_part.at[:, part, :, window(n, cw)], msem.at[part, n])

        for b in range(nb - 1):
            w_start(jnp.int32(0), b)
        for n in range(RING - 1):
            d_start(jnp.int32(0), jnp.int32(n))
        ids_own.wait()
        for k in range(1, RING):
            ids_send(k).wait_recv()
        load_i = pltpu.make_async_copy(ids_all, idf.at[:, pl.ds(0, top_k)], lsem.at[RING + 1])
        load_i.start()
        for side in SIDES:
            hid_forward(0, side).wait_recv()
        load_i.wait()
        u_ready(0)

        def one_pass(p):
            @pl.when(p == 1)
            def _():
                ctx_pass(pairs - 2)
                for side in SIDES:
                    w_forward(side).wait_recv()
                w_core(2).start()
                for i in range(len(mats)):
                    swap_mat(1, i).start()

            @pl.when(p == 2)
            def _():
                for k in range(RING):
                    w_core(k).wait_recv()
                for c in load_w:
                    c.start()

            @pl.when(p == 3)
            def _():
                ctx_pass(pairs - 1)
                for side in SIDES:
                    hid_send(1, side).wait_recv()
                    hid_forward(1, side).start()
                attention_out()
                for side in SIDES:
                    hid_forward(1, side).wait_recv()
                u_ready(1)

            @pl.when(p >= RING)
            def _():
                a_pass(p - RING)
            k, part = expert_of(p), half_of(p)
            which = (k // local) * ((e + 1 - 2 * core) * local + k - local) + (1 - k // local) * (e * local + k)
            rows = RING * half
            u = xn.at[pl.ds(pl.multiple_of(part * rows, rows), rows)]
            lane = lax.broadcasted_iota(jnp.int32, gate.shape[1:], 1)
            weight = jnp.sum(jnp.where(lane == which, gate[part], 0.0), axis=1, keepdims=True)

            def arrived(which_mats):
                for late, when in enumerate((1, last - 1)):
                    @pl.when(p == when)
                    def _():
                        for i in which_mats:
                            swap_mat(late, i).wait_recv()
            for b, size in enumerate(sizes):
                nxt = b + nb - 1
                if nxt == nb:
                    arrived(SIDES)
                w_start(p + nxt // nb, nxt % nb)
                for c in w_load(0, b, b, True):
                    c.wait()
                g = lax.dot_general(u[...], wbuf[b, 0, 0:size], NT, preferred_element_type=F32)
                v = lax.dot_general(u[...], wbuf[b, 1, 0:size], NT, preferred_element_type=F32)
                act[:, b * fb:b * fb + size] = (jax.nn.silu(g) * v).astype(BF16)

            def block(n):
                ahead = n + RING - 1

                @pl.when(ahead < nn)
                def _():
                    d_start(p, ahead)

                @pl.when(ahead == nn)
                def _():
                    arrived((2,))

                @pl.when(ahead >= nn)
                def _():
                    d_start(p + 1, ahead - nn)
                d_load(0, n, True).wait()
                y = jnp.dot(act[...], dbuf[lax.rem(n, RING)], preferred_element_type=F32).astype(BF16)
                term = jnp.where(weight > 0.0, weight * y.astype(F32), 0.0).reshape(mv.shape[2:])
                mv[part, n] = jnp.where(k == 0, term, mv[part, n] + term)

                @pl.when(p >= last)
                def _():
                    m_out(part, n).start()
            loop(nn, block)
        loop(passes, one_pass)

        def finish(n):
            for part in SIDES:
                m_out(part, n).wait()
        loop(nn, finish)

    fb = 256 if fe > 512 else 128
    cw = min(512, d_model // 4)
    pl.run_scoped(experts, pltpu.VMEM((RING, 8, hd, width), BF16), pltpu.VMEM((2, q, RING * heads * hd), BF16), pltpu.VMEM((2, q, width), BF16),
                  pltpu.VMEM((2, d_model // cw, RING, half, cw), F32), pltpu.VMEM((RING * half, fe), BF16),
                  pltpu.VMEM((fe // fb + 1, 2, fb, d_model), BF16), pltpu.VMEM((RING, fe, cw), BF16))

    for side in SIDES:
        w_round(side).wait_send()
        w_forward(side).wait_send()
        for part in SIDES:
            hid_send(part, side).wait_send()
            hid_forward(part, side).wait_send()
        for g in range(pairs):
            ctx_send(g, side).wait_send()
            ctx_forward(g, side).wait_send()
        for c in range(RING):
            a_send(c, side).wait_send()
            a_forward(c, side).wait()
    for k in range(1, RING):
        w_swap(k).wait_send()
        ids_send(k).wait_send()
    for k in SIDES:
        for i in range(len(mats)):
            swap_mat(k, i).wait_send()
    for k in range(RING):
        w_core(k).wait_send()
        a_local(k).wait()


def front_call(x, wq, wk, wv, wo, eg, eu, ed, attn_gain, moe_gain, ids, router):
    tokens, d_model = x.shape
    heads, hd = wq.shape[1], wq.shape[2]
    q = tokens // RING
    local, fe = eg.shape[0], eg.shape[1]
    experts = router.shape[0]
    pairs = heads // 2
    hbm = pl.BlockSpec(memory_space=pl.ANY)
    vmem = pl.BlockSpec(memory_space=pltpu.VMEM)
    dma = pltpu.SemaphoreType.DMA
    sds = jax.ShapeDtypeStruct
    freq = ROPE_BASE ** (np.arange(hd) % (hd // 2) * (-2.0 / hd))
    freq = jnp.asarray(freq.astype(np.float32).reshape(1, hd))
    two, three, four = dma((2,)), dma((3,)), dma((RING,))
    by_pair, by_chunk, square = dma((2, pairs)), dma((2, RING)), dma((2, 2))
    outs = pl.pallas_call(
        front_body,
        out_shape=(sds((tokens, d_model), BF16), sds((RING, 2, q // 2, d_model), F32), sds((RING, tokens, heads * hd), BF16),
                   sds((RING, 2, q // 2, d_model), BF16), sds((RING, ids.shape[0], q), ids.dtype), sds((8, RING, hd, d_model // RING), BF16),
                   sds(eg.shape, BF16), sds(eu.shape, BF16), sds(ed.shape, BF16)),
        in_specs=[hbm] * 8 + [vmem] * 3 + [hbm, vmem],
        out_specs=(hbm,) * 9,
        scratch_shapes=[
            pltpu.VMEM((tokens, d_model), BF16), pltpu.VMEM((pairs, tokens, 2 * hd), BF16), pltpu.VMEM((RING, q, d_model // RING), BF16),
            pltpu.VMEM((2, tokens // 2, experts), F32), pltpu.VMEM((RING, 8, q), ids.dtype),
            pltpu.VMEM((2, tokens, hd), F32),
            dma((RING + 2,)), dma((8,)), dma((pairs,)), four,
        ] + [by_pair] * RING + [by_chunk] * RING + [square] * RING + [three] * 2 + [two] * RING + [four] * 2 + [three] * 2
          + [dma((2, 3))] * 2 + [by_chunk, two, four, dma((fe // 256 + 1, 2)), four, dma((2, 8))],
        compiler_params=pltpu.CompilerParams(collective_id=0, has_side_effects=True, vmem_limit_bytes=VMEM_LIMIT),
        cost_estimate=pl.CostEstimate(flops=2 * tokens * d_model * (heads * hd * RING + 12 * fe), bytes_accessed=24 * fe * d_model, transcendentals=heads * tokens * tokens),
        name='attn_moe',
    )(x, wq, wk, wv, wo, eg, eu, ed, attn_gain, moe_gain, freq, ids, router)
    return outs[0], outs[1]


def solution(mesh):
    tok_spec = P(('dp', 'ep'))
    col_spec = P(None, 'tp')
    in_specs = (tok_spec,) * 3 + (P(),) + (col_spec,) * 3 + (P('tp'), P(), col_spec, col_spec, P('tp'), P(), P()) + (P('ep'),) * 3

    def layer_local(hidden_in, expert_ids, slot_ids, attn_gain, w_query, w_key, w_value, w_out, ffn_gain, w_gate, w_up, w_down, moe_gain, w_router, exp_gate, exp_up, exp_down):
        num_seqs, seq_len, d_model = hidden_in.shape
        tokens = num_seqs * seq_len
        heads, head_dim = w_out.shape[0], w_out.shape[1]
        x = hidden_in.reshape(tokens, d_model)
        ids = jnp.swapaxes(expert_ids, 1, 2).reshape(expert_ids.shape[2], tokens)
        after_attn, m_part = front_call(
            x, w_query, w_key, w_value, w_out.reshape(heads * head_dim, d_model), jnp.swapaxes(exp_gate, 1, 2), jnp.swapaxes(exp_up, 1, 2), exp_down,
            attn_gain, moe_gain, ids, w_router.T)
        out = ffn_call(after_attn, w_gate.T, w_up.T, w_down, ffn_gain, m_part.reshape(-1, tokens // 4, d_model))
        return out.reshape(hidden_in.shape)

    return jax.shard_map(layer_local, mesh=mesh, in_specs=in_specs, out_specs=tok_spec, check_vma=False)
```

```python
import functools

import jax
import jax.numpy as jnp
import numpy as np
from jax import lax
from jax.experimental import pallas as pl
from jax.experimental.pallas import tpu as pltpu
from jax.sharding import PartitionSpec as P

F32 = jnp.float32
BF16 = jnp.bfloat16
EPS = 1e-6
ROPE_BASE = 10000.0
VMEM_LIMIT = 67043328
MESH = pl.DeviceIdType.MESH
NT = (((1,), (1,)), ((), ()))


RING = 4
SIDES = (0, 1)


def odd(k):
    return lax.rem(k, 2)


def turn(side):
    return 1 - 2 * side


def loop(count, body):
    def step(k, carry):
        body(k)
        return carry
    lax.fori_loop(0, count, step, 0)


def window(index, size):
    return pl.ds(pl.multiple_of(index * size, size), size)


def rcopy(src, dst, ssem, rsem, dev):
    return pltpu.make_async_remote_copy(src_ref=src, dst_ref=dst, send_sem=ssem, recv_sem=rsem, device_id=dev, device_id_type=MESH)


def entry_barrier(neighbours):
    barrier = pltpu.get_barrier_semaphore()
    for dev in neighbours:
        pl.semaphore_signal(barrier, inc=1, device_id=dev, device_id_type=MESH)
    pl.semaphore_wait(barrier, len(neighbours))


def norm_rows(src, dst, gain, rows, step):
    def one(r):
        sl = window(r, step)
        x = src[sl, :].astype(F32)
        inv = lax.rsqrt(jnp.mean(x * x, axis=-1, keepdims=True) + EPS)
        dst[sl, :] = (x * inv * gain[...].astype(F32).reshape(1, -1)).astype(BF16)
    loop(rows // step, one)


def ffn_body(fb, a_ref, wg, wu, wd, gain, m_ref, out_ref,
             a_own, n2, h, wbuf, dbuf, p1, yrecv, xrecv, mbuf,
             asem, wsem, dsem, msem, osem, ys, yr, xs, xr, gs, gr, fs, fr):
    t = lax.axis_index('tp')
    e = lax.axis_index('ep')
    big = odd(e)
    xc = e // 2
    q = a_own.shape[0]
    d_model = a_own.shape[1]
    f_loc = wg.shape[0]
    cw = d_model // 8
    hw = cw // 2
    nf = f_loc // fb
    tail = f_loc - nf * fb
    yright, yleft = {'tp': lax.rem(t + 1, RING)}, {'tp': lax.rem(t + 3, RING)}
    xright, xleft = {'ep': lax.rem(xc + 1, RING) * 2 + big}, {'ep': lax.rem(xc + 3, RING) * 2 + big}

    def cols(cb):
        return window(cb, cw)

    def chunk(c):
        return lax.rem(c + 8, RING)

    def rows(c):
        return window(chunk(c), q)

    def a_load(c, slot):
        return pltpu.make_async_copy(a_ref.at[rows(c)], n2.at[pl.ds(slot * q, q)], asem.at[slot])
    load_own = pltpu.make_async_copy(a_ref.at[rows(t)], a_own, asem.at[2])

    def w_load(i, slot, size):
        sl = pl.ds(pl.multiple_of(i * fb, fb), size)
        return (pltpu.make_async_copy(wg.at[sl], wbuf.at[slot, 0, pl.ds(0, size)], wsem.at[slot, 0]),
                pltpu.make_async_copy(wu.at[sl], wbuf.at[slot, 1, pl.ds(0, size)], wsem.at[slot, 1]))

    def w_start(i):
        slot = lax.rem(i, wbuf.shape[0])

        @pl.when(i < nf)
        def _():
            for c in w_load(i, slot, fb):
                c.start()

        @pl.when(i == nf)
        def _():
            for c in w_load(nf, slot, tail):
                c.start()

    def col_of(j):
        return odd(j) * 4 + j // 2

    def d_load(j):
        start = col_of(j) * cw
        return [pltpu.make_async_copy(wd.at[:, pl.ds(pl.multiple_of(start + sub * hw, hw), hw)], dbuf.at[odd(j), sub], dsem.at[odd(j), sub]) for sub in SIDES]

    def m_load(k):
        s, j = k // 8 + 1, lax.rem(k, 8)
        side = odd(j)
        c = lax.rem(xc + (2 * side - 1) * (1 + s) + 8, RING)
        slot = odd(k)
        return pltpu.make_async_copy(m_ref.at[c, :, cols(col_of(j))], mbuf.at[slot], msem.at[slot])

    def send(buf, ssem, rsem, src, right, left, side, step, i):
        @pl.when(side == 0)
        def _():
            rcopy(src, buf.at[0, step, i], ssem.at[0, step, i], rsem.at[0, step, i], right).start()

        @pl.when(side == 1)
        def _():
            rcopy(src, buf.at[1, step, i], ssem.at[1, step, i], rsem.at[1, step, i], left).start()

    def ysend(src, side, step, i):
        send(yrecv, ys, yr, src, yright, yleft, side, step, i)

    def xsend(src, side, step, i):
        send(xrecv, xs, xr, src, xright, xleft, side, step, i)

    def arrived(buf, ssem, rsem, side, step, i, dev):
        rcopy(buf.at[side, step, i], buf.at[side, step, i], ssem.at[side, step, i], rsem.at[side, step, i], dev).wait_recv()

    def sent(buf, ssem, rsem, side, step, i, dev):
        rcopy(buf.at[side, step, i], buf.at[side, step, i], ssem.at[side, step, i], rsem.at[side, step, i], dev).wait_send()

    def xserve(k):
        s, j = k // 8, lax.rem(k, 8)
        side, i = odd(j), j // 2
        m_load(k + 1).start()
        m_load(k).wait()
        arrived(xrecv, xs, xr, side, s, i, xright)
        xrecv[side, s, i] = xrecv[side, s, i] + mbuf[odd(k)]
        xsend(xrecv.at[side, s, i], side, s + 1, i)

    def gate_up(serve):
        def block(i, size):
            slot = lax.rem(i, wbuf.shape[0])
            w_start(i + 2)
            for c in w_load(i, slot, size):
                c.wait()
            g = lax.dot_general(n2[...], wbuf[slot, 0, pl.ds(0, size)], NT, preferred_element_type=F32)
            u = lax.dot_general(n2[...], wbuf[slot, 1, pl.ds(0, size)], NT, preferred_element_type=F32)
            h[:, pl.ds(pl.multiple_of(i * fb, fb), size)] = (jax.nn.silu(g) * u).astype(BF16)

        def one(i):
            block(i, fb)
            serve(i)
        loop(nf, one)
        block(nf, tail)

    def d_start(j):
        for c in d_load(j):
            c.start()

    def down(ready, use, done):
        def one(j):
            @pl.when(j + 1 < 8)
            def _():
                d_start(j + 1)
            ready(j)
            for c in d_load(j):
                c.wait()
            for sub in SIDES:
                r = jnp.dot(h[...], dbuf[odd(j), sub], preferred_element_type=F32)
                use(j, slice(sub * hw, (sub + 1) * hw), r)
            done(j)
        loop(8, one)

    a_load(t - 1, 0).start()
    a_load(t + 1, 1).start()
    w_start(0)
    w_start(1)
    entry_barrier((yright, yleft, xright, xleft))

    def x_first(i):
        xsend(m_ref.at[chunk(xc - 1), :, cols(i)], 0, 0, i)
        xsend(m_ref.at[chunk(xc + 1), :, cols(4 + i)], 1, 0, i)
    loop(4, x_first)
    d_start(jnp.int32(0))
    m_load(0).start()
    load_own.start()

    for slot in SIDES:
        a_load(t, slot).wait()
        norm_rows(n2.at[pl.ds(slot * q, q)], n2.at[pl.ds(slot * q, q)], gain, q, 16)
    gate_up(lambda i: None)
    a_load(t + 2, 0).start()
    a_load(t, 1).start()
    w_start(0)
    w_start(1)

    def use1(j, part, r):
        p1[col_of(j), :, part] = r

    def done1(j):
        side = odd(j)
        ysend(p1.at[col_of(j), pl.ds(pl.multiple_of(side * q, q), q)], side, 0, j // 2)
    down(lambda j: None, use1, done1)
    d_start(jnp.int32(0))

    for slot in SIDES:
        a_load(t, slot).wait()
        norm_rows(n2.at[pl.ds(slot * q, q)], n2.at[pl.ds(slot * q, q)], gain, q, 16)

    def serve2(i):
        @pl.when(i < 8)
        def _():
            xserve(i)
    gate_up(serve2)
    for k in range(min(nf, 8), 8):
        xserve(k)

    def sent_rows(j):
        return pl.ds(pl.multiple_of(odd(j) * q, q), q)

    def ready2(j):
        arrived(yrecv, ys, yr, odd(j), 0, j // 2, yright)
        sent(yrecv, ys, yr, odd(j), 0, j // 2, yright)

    def use2(j, part, r):
        p1[col_of(j), sent_rows(j), part] = r[q:]
        yrecv[odd(j), 0, j // 2, :, part] = yrecv[odd(j), 0, j // 2, :, part] + r[:q]

    def done2(j):
        ysend(yrecv.at[odd(j), 0, j // 2], odd(j), 1, j // 2)
    down(ready2, use2, done2)

    def third(j):
        side, i = odd(j), j // 2
        xserve(8 + j)
        arrived(yrecv, ys, yr, side, 1, i, yright)
        yrecv[side, 1, i] = yrecv[side, 1, i] + p1[col_of(j), window((1 - side), q)]
        ysend(yrecv.at[side, 1, i], side, 2, i)
    loop(8, third)

    def out_local(cb):
        return pltpu.make_async_copy(n2.at[pl.ds(0, q), cols(cb)], out_ref.at[rows(t), cols(cb)], osem.at[cb])

    def gather(cb, side, dev):
        return rcopy(n2.at[pl.ds(0, q), cols(cb)], out_ref.at[rows(t), cols(cb)], gs.at[side, cb], gr.at[side, cb], dev)

    load_own.wait()

    def last(j):
        side, i = odd(j), j // 2
        cb = col_of(j)
        k = 16 + j

        @pl.when(j + 1 < 8)
        def _():
            m_load(k + 1).start()
        m_load(k).wait()
        arrived(xrecv, xs, xr, side, 2, i, xright)
        arrived(yrecv, ys, yr, side, 2, i, yright)
        b_val = a_own[:, cols(cb)].astype(F32) + (yrecv[side, 2, i] + p1[cb, sent_rows(j)])
        n2[pl.ds(0, q), cols(cb)] = (b_val + (xrecv[side, 2, i] + mbuf[odd(k)])).astype(BF16)
        out_local(cb).start()
        gather(cb, 0, yright).start()
        gather(cb, 1, yleft).start()
    loop(8, last)

    half = q // 2

    def half_rows(c, which):
        return pl.ds(pl.multiple_of(chunk(c) * q + which * half, half), half)

    def forward(c, which, cb, dev):
        ref = out_ref.at[half_rows(c, which), cols(cb)]
        return rcopy(ref, ref, fs.at[which, cb], fr.at[which, cb], dev)

    def pass_on(j):
        cb = col_of(j)
        gather(cb, 0, yright).wait_recv()
        forward(t - 1, 0, cb, yright).start()
        gather(cb, 1, yleft).wait_recv()
        forward(t + 1, 1, cb, yleft).start()
    loop(8, pass_on)

    def finish(j):
        cb = col_of(j)
        out_local(cb).wait()
        for which in SIDES:
            gather(cb, which, yright).wait_send()
            forward(t, which, cb, yright).wait_send()
            forward(t, which, cb, yright).wait_recv()
    loop(8, finish)

    def drain(k):
        step, j = k // 8, lax.rem(k, 8)

        @pl.when(step > 0)
        def _():
            sent(yrecv, ys, yr, odd(j), step, j // 2, yright)
        sent(xrecv, xs, xr, odd(j), step, j // 2, yright)
    loop(24, drain)


def ffn_call(after_attn, wg_t, wu_t, w_down, gain, m_part):
    tokens, d_model = after_attn.shape
    f_loc = wg_t.shape[0]
    fb = 256 if f_loc > 512 else 128
    q = tokens // 4
    cw = d_model // 8
    hbm = pl.BlockSpec(memory_space=pl.ANY)
    vmem = pl.BlockSpec(memory_space=pltpu.VMEM)
    dma = pltpu.SemaphoreType.DMA
    flops = 2 * tokens * d_model * f_loc * 3
    return pl.pallas_call(
        functools.partial(ffn_body, fb),
        out_shape=jax.ShapeDtypeStruct((tokens, d_model), BF16),
        in_specs=[hbm, hbm, hbm, hbm, vmem, hbm],
        out_specs=hbm,
        scratch_shapes=[
            pltpu.VMEM((q, d_model), BF16),
            pltpu.VMEM((2 * q, d_model), BF16),
            pltpu.VMEM((2 * q, f_loc), BF16),
            pltpu.VMEM((3, 2, fb, d_model), BF16),
            pltpu.VMEM((2, 2, f_loc, cw // 2), BF16),
            pltpu.VMEM((8, 2 * q, cw), F32),
            pltpu.VMEM((2, 3, RING, q, cw), F32),
            pltpu.VMEM((2, 3, RING, q, cw), F32),
            pltpu.VMEM((2, q, cw), F32),
            dma((3,)), dma((3, 2)), dma((2, 2)), dma((2,)), dma((8,)),
        ] + [dma((2, 3, RING))] * RING + [dma((2, 8))] * RING,
        compiler_params=pltpu.CompilerParams(collective_id=2, has_side_effects=True, vmem_limit_bytes=VMEM_LIMIT),
        cost_estimate=pl.CostEstimate(flops=flops, bytes_accessed=4 * tokens * d_model + 12 * f_loc * d_model, transcendentals=tokens * f_loc),
        name='ffn_ring',
    )(after_attn, wg_t, wu_t, w_down, gain, m_part)


def front_body(x_ref, wq, wk, wv, wo, eg, eu, ed, attn_gain, moe_gain, freq, ids, router,
               a_full, m_part, ctx_all, hid_all, ids_all, w_cols, og, ou, od,
               xn, ctxb, abuf, gate, idf,
               lsem, rawsem, cls, als, cs, cr, cfs, cfr, as_, ar, afs, afr, hs, hr, hfs, hfr, ws, wr, wxs, wxr, wfs, wfr,
               wds, wdr, ins, inr, es, er, csem, xsem, usem, wsem, dsem, msem):
    t = lax.axis_index('tp')
    e = lax.axis_index('ep')
    core = odd(e)
    xc = e // 2
    tokens, d_model = xn.shape
    heads, hd = wq.shape[1], wq.shape[2]
    q = tokens // RING
    half = q // 2
    width = d_model // RING
    kblk = min(512, d_model // RING)
    nk = d_model // kblk
    pair = 2 * hd
    pairs = heads // 2
    local, fe = eg.shape[0], eg.shape[1]
    top_k = ids.shape[0]
    partner = {'ep': xc * 2 + 1 - core}

    def ring(k):
        return lax.rem(k + RING, RING)

    def y_dev(k):
        return {'tp': ring(t + k)}

    def x_id(k):
        return ring(xc + k) * 2 + core

    def x_dev(k):
        return {'ep': x_id(k)}

    def w_swap(k):
        return rcopy(wo.at[window(e, hd), window(ring(t + k), width)], w_cols.at[e, t], ws.at[k - 1], wr.at[k - 1], y_dev(k))

    def w_round(side):
        return rcopy(w_cols.at[e], w_cols.at[e], wxs.at[side], wxr.at[side], x_dev(turn(side)))

    def w_forward(side):
        ref = w_cols.at[x_id(2 * side - 1), pl.ds(2 * side, 2)]
        return rcopy(ref, ref, wfs.at[side], wfr.at[side], x_dev(turn(side)))

    def w_core(k):
        return rcopy(w_cols.at[x_id(k)], w_cols.at[x_id(k)], wds.at[k], wdr.at[k], partner)

    def hid_send(part, side):
        rows = pl.ds(pl.multiple_of(t * q + part * half, half), half)
        return rcopy(x_ref.at[rows], hid_all.at[xc, part], hs.at[part, side], hr.at[part, side], x_dev(turn(side)))

    def hid_forward(part, side):
        ref = hid_all.at[ring(xc + 2 * side - 1), part, pl.ds(side * (half // 2), half // 2)]
        return rcopy(ref, ref, hfs.at[part, side], hfr.at[part, side], x_dev(turn(side)))

    def ids_send(k):
        return rcopy(ids.at[:, window(t, q)], ids_all.at[xc], ins.at[k - 1], inr.at[k - 1], x_dev(k))

    mats = ((eg, og), (eu, ou), (ed, od))

    def swap_mat(k, i):
        return rcopy(mats[i][0].at[k], mats[i][1].at[k], es.at[k, i], er.at[k, i], partner)

    def ctx_local(g):
        return pltpu.make_async_copy(ctxb.at[g], ctx_all.at[t, :, window(g, pair)], cls.at[g])

    def ctx_send(g, side):
        return rcopy(ctxb.at[g], ctx_all.at[t, :, window(g, pair)], cs.at[side, g], cr.at[side, g], y_dev(turn(side)))

    def ctx_forward(g, side):
        ref = ctx_all.at[ring(t + 2 * side - 1), pl.ds(side * (tokens // 2), tokens // 2), window(g, pair)]
        return rcopy(ref, ref, cfs.at[side, g], cfr.at[side, g], y_dev(turn(side)))

    def ctx_pass(g):
        for side in SIDES:
            ctx_send(g, side).wait_recv()
            ctx_forward(g, side).start()

    def a_local(c):
        return pltpu.make_async_copy(abuf.at[c], a_full.at[window(c, q), window(t, width)], als.at[c])

    def a_send(c, side):
        return rcopy(abuf.at[c], a_full.at[window(c, q), window(t, width)], as_.at[side, c], ar.at[side, c], y_dev(turn(side)))

    def a_forward(c, side):
        rows = pl.ds(pl.multiple_of(c * q + side * half, half), half)
        ref = a_full.at[rows, window(ring(t + 2 * side - 1), width)]
        return rcopy(ref, ref, afs.at[side, c], afr.at[side, c], y_dev(turn(side)))

    def a_pass(c):
        for side in SIDES:
            a_send(c, side).wait_recv()
            a_forward(c, side).start()

    load_x = [pltpu.make_async_copy(x_ref.at[pl.ds(k * q, q)], xn.at[pl.ds(k * q, q)], lsem.at[k]) for k in range(RING)]
    for c in load_x:
        c.start()
    w_own = pltpu.make_async_copy(wo.at[window(e, hd), window(t, width)], w_cols.at[e, t], lsem.at[RING])
    ids_own = pltpu.make_async_copy(ids.at[:, window(t, q)], ids_all.at[xc], lsem.at[RING + 1])

    def attention(rope, raw, wide, wb, qb, kb, vb):
        proj = (wq, wk, wv)

        deep = raw.shape[0]

        def raw_load(m, k):
            slot = lax.rem(k, deep)
            return pltpu.make_async_copy(proj[m].at[window(k, kblk)], raw.at[slot], rawsem.at[slot])
        for k in range(deep):
            raw_load(0, k).start()
        entry_barrier((y_dev(1), y_dev(-1), y_dev(2), x_dev(1), x_dev(-1), x_dev(2), partner))
        w_own.start()
        ids_own.start()
        for k in range(1, RING):
            w_swap(k).start()
            ids_send(k).start()
        for side in SIDES:
            hid_send(0, side).start()
        for i in range(len(mats)):
            swap_mat(0, i).start()

        sign = jnp.where(lax.broadcasted_iota(jnp.int32, (1, hd), 1) < hd // 2, -1.0, 1.0)
        steps = min(128, tokens)

        def angles(k):
            angle = (lax.broadcasted_iota(jnp.int32, (steps, 1), 0) + k * steps).astype(F32) * freq[...]
            rope[0, window(k, steps)] = jnp.cos(angle)
            rope[1, window(k, steps)] = jnp.sin(angle) * sign
        loop(tokens // steps, angles)

        for k in range(RING):
            load_x[k].wait()
            norm_rows(xn.at[pl.ds(k * q, q)], xn.at[pl.ds(k * q, q)], attn_gain, q, 16)

        for m in range(len(proj)):
            def one(k, m=m):
                raw_load(m, k).wait()
                wide[...] = raw[lax.rem(k, deep)].astype(F32).reshape(kblk * heads, hd)

                @pl.when(k + deep < nk)
                def _():
                    raw_load(m, k + deep).start()

                if m + 1 < len(proj):
                    @pl.when(k + deep >= nk)
                    def _():
                        raw_load(m + 1, k + deep - nk).start()
                for h in range(heads):
                    wb[m, window(k, kblk), h * hd:(h + 1) * hd] = wide[pl.ds(h, kblk, stride=heads), :].astype(BF16)
            loop(nk, one)

        w_own.wait()
        for k in range(1, RING):
            w_swap(k).wait_recv()
        for side in SIDES:
            w_round(side).start()
        w_core(0).start()

        scale = hd ** -0.5
        tri = lax.broadcasted_iota(jnp.int32, (q, q), 0) >= lax.broadcasted_iota(jnp.int32, (q, q), 1)

        def heads_of(g):
            for m, dst in enumerate((qb, kb, vb)):
                r = jnp.dot(xn[...], wb[m, :, window(g, pair)], preferred_element_type=F32)
                if dst is vb:
                    dst[...] = r.astype(BF16)
                else:
                    for h in SIDES:
                        part = r[:, h * hd:(h + 1) * hd]
                        turned = part * rope[0] + pltpu.roll(part, hd // 2, 1) * rope[1]
                        dst[:, h * hd:(h + 1) * hd] = turned.astype(BF16)
            for h in SIDES:
                hc = slice(h * hd, (h + 1) * hd)
                for b in range(RING):
                    s = lax.dot_general(qb[b * q:(b + 1) * q, hc], kb[0:(b + 1) * q, hc], NT, preferred_element_type=F32) * scale
                    diag = jnp.where(tri, s[:, b * q:], -1e30)
                    s = diag if b == 0 else jnp.concatenate([s[:, :b * q], diag], axis=1)
                    w = jnp.exp(s - jnp.max(s, axis=-1, keepdims=True))
                    prob = (w * (1.0 / jnp.sum(w, axis=-1, keepdims=True))).astype(BF16)
                    ctxb[g, b * q:(b + 1) * q, hc] = jnp.dot(prob, vb[0:(b + 1) * q, hc], preferred_element_type=F32).astype(BF16)
            ctx_local(g).start()
            for side in SIDES:
                ctx_send(g, side).start()

            @pl.when(g == 0)
            def _():
                for side in SIDES:
                    hid_send(0, side).wait_recv()
                    hid_forward(0, side).start()

            @pl.when(g >= 2)
            def _():
                ctx_pass(g - 2)

            @pl.when(g == 2)
            def _():
                for side in SIDES:
                    w_round(side).wait_recv()
                    w_forward(side).start()
                w_core(1).start()
                w_core(RING - 1).start()

            @pl.when(g == pairs - 1)
            def _():
                for side in SIDES:
                    hid_send(1, side).start()
        loop(pairs, heads_of)

    pl.run_scoped(attention, pltpu.VMEM((2, tokens, hd), F32), pltpu.VMEM((RING, kblk, heads, hd), BF16), pltpu.VMEM((kblk * heads, hd), F32),
                  pltpu.VMEM((len(SIDES) + 1, d_model, heads * hd), BF16), *[pltpu.VMEM((tokens, pair), BF16)] * (len(SIDES) + 1))

    fb = 256 if fe > 512 else 128
    cw = min(512, d_model // 4)

    def experts(wcv, cbuf, mv, act, wbuf, dbuf):
        sizes = [fb] * (fe // fb) + [fe % fb]
        cw = mv.shape[-1]
        nn = d_model // cw
        passes = 4 * local
        last = passes - 2

        def expert_of(p):
            late = p // last
            return (1 - late) * lax.rem(p, 3) + late * 3

        def half_of(p):
            late = p // last
            return (1 - late) * (p // 3) + late * (p - last)

        def w_load(k, own):
            k = k if own else k - local
            return [pltpu.make_async_copy(ref.at[k], wbuf.at[i], wsem.at[i]) for i, ref in enumerate((eg, eu) if own else (og, ou))]

        def d_load(k, own):
            return [pltpu.make_async_copy((ed if own else od).at[k if own else k - local], dbuf, dsem.at[0])]

        def start(p, load):
            k = expert_of(p)

            @pl.when(jnp.logical_and(p < passes, k < local))
            def _():
                for c in load(k, True):
                    c.start()

            @pl.when(jnp.logical_and(p < passes, k >= local))
            def _():
                for c in load(k, False):
                    c.start()

        def u_rows(part, k):
            return xn.at[pl.ds(pl.multiple_of((part * RING + k) * half, half), half)]

        def u_ready(part):
            for k in range(RING):
                @pl.when(k == xc)
                def _():
                    rows = pl.ds(pl.multiple_of(t * q + part * half, half), half)
                    pltpu.make_async_copy(x_ref.at[rows], u_rows(part, k), usem.at[k]).start()

                @pl.when(k != xc)
                def _():
                    pltpu.make_async_copy(hid_all.at[k, part], u_rows(part, k), usem.at[k]).start()
            for k in range(RING):
                pltpu.make_async_copy(hid_all.at[k, part], u_rows(part, k), usem.at[k]).wait()
            rows = RING * half
            u = xn.at[pl.ds(part * rows, rows)]
            norm_rows(u, u, moe_gain, rows, 16)
            logits = lax.dot_general(u[...], router[...], NT, preferred_element_type=F32)
            lane = lax.broadcasted_iota(jnp.int32, logits.shape, 1).astype(F32)
            picks = jnp.concatenate([idf[k, :, part * half:(part + 1) * half].astype(F32) for k in range(RING)], axis=1).T
            chosen = lane == picks[:, 0:1]
            for j in range(1, top_k):
                chosen = jnp.logical_or(chosen, lane == picks[:, j:j + 1])
            top = jnp.max(jnp.where(chosen, logits, -jnp.inf), axis=-1, keepdims=True)
            w = jnp.where(chosen, jnp.exp(jnp.where(chosen, logits - top, 0.0)), 0.0)
            gate[part] = w / jnp.sum(w, axis=-1, keepdims=True)

        def ctx_load(c):
            return [pltpu.make_async_copy(ctx_all.at[k, window(c, q)], cbuf.at[odd(c), :, pl.ds(k * heads * hd, heads * hd)], csem.at[odd(c), k]) for k in range(RING)]

        def x_load(c):
            return pltpu.make_async_copy(x_ref.at[window(c, q), window(t, width)], abuf.at[c], xsem.at[odd(c)])

        load_w = [pltpu.make_async_copy(w_cols.at[:, k], wcv.at[k], lsem.at[k]) for k in range(RING)]

        def attention_out():
            for side in SIDES:
                for g in range(pairs):
                    ctx_forward(g, side).wait_recv()
            for g in range(pairs):
                ctx_local(g).wait()
            for c in ctx_load(jnp.int32(0)):
                c.start()
            x_load(jnp.int32(0)).start()
            for c in load_w:
                c.wait()

            def chunk(c):
                @pl.when(c + 1 < RING)
                def _():
                    for d in ctx_load(c + 1):
                        d.start()
                    x_load(c + 1).start()
                for d in ctx_load(c):
                    d.wait()
                x_load(c).wait()
                o = jnp.dot(cbuf[odd(c)], wcv[...].reshape(RING * heads * hd, width), preferred_element_type=F32)
                abuf[c] = (abuf[c].astype(F32) + o).astype(BF16)
                a_local(c).start()
                for side in SIDES:
                    a_send(c, side).start()
            loop(RING, chunk)

        def m_out(part, n):
            return pltpu.make_async_copy(mv.at[part, n], m_part.at[:, part, :, window(n, cw)], msem.at[part, n])

        start(jnp.int32(0), w_load)
        ids_own.wait()
        for k in range(1, RING):
            ids_send(k).wait_recv()
        load_i = pltpu.make_async_copy(ids_all, idf.at[:, pl.ds(0, top_k)], lsem.at[RING + 1])
        load_i.start()
        for side in SIDES:
            hid_forward(0, side).wait_recv()
        load_i.wait()
        u_ready(0)

        def one_pass(p):
            @pl.when(p == 1)
            def _():
                ctx_pass(pairs - 2)
                for side in SIDES:
                    w_forward(side).wait_recv()
                w_core(2).start()
                for i in range(len(mats)):
                    swap_mat(1, i).start()

            @pl.when(p == 2)
            def _():
                for k in range(RING):
                    w_core(k).wait_recv()
                for c in load_w:
                    c.start()

            @pl.when(p == 3)
            def _():
                ctx_pass(pairs - 1)
                for side in SIDES:
                    hid_send(1, side).wait_recv()
                    hid_forward(1, side).start()
                attention_out()
                for side in SIDES:
                    hid_forward(1, side).wait_recv()
                u_ready(1)

            @pl.when(p >= RING)
            def _():
                a_pass(p - RING)
            k, part = expert_of(p), half_of(p)
            which = (k // local) * ((e + 1 - 2 * core) * local + k - local) + (1 - k // local) * (e * local + k)
            rows = RING * half
            u = xn.at[pl.ds(pl.multiple_of(part * rows, rows), rows)]
            lane = lax.broadcasted_iota(jnp.int32, gate.shape[1:], 1)
            weight = jnp.sum(jnp.where(lane == which, gate[part], 0.0), axis=1, keepdims=True)

            def if_new(ahead, which_mats):
                for late, when in enumerate((3, last + 1)):
                    @pl.when(ahead == when)
                    def _():
                        for i in which_mats:
                            swap_mat(late, i).wait_recv()
            if_new(p + 1, (2,))
            start(p, d_load)
            for c in w_load(0, True):
                c.wait()
            for b, size in enumerate(sizes):
                cols = slice(b * fb, b * fb + size)
                g = lax.dot_general(u[...], wbuf[0, cols], NT, preferred_element_type=F32)
                v = lax.dot_general(u[...], wbuf[1, cols], NT, preferred_element_type=F32)
                act[:, cols] = (jax.nn.silu(g) * v).astype(BF16)
            if_new(p + 2, SIDES)
            start(p + 1, w_load)
            for c in d_load(0, True):
                c.wait()
            for n in range(nn):
                y = jnp.dot(act[...], dbuf[:, n * cw:(n + 1) * cw], preferred_element_type=F32).astype(BF16)
                term = jnp.where(weight > 0.0, weight * y.astype(F32), 0.0).reshape(mv.shape[2:])
                mv[part, n] = jnp.where(k == 0, term, mv[part, n] + term)

            @pl.when(p >= last)
            def _():
                loop(nn, lambda n: m_out(part, n).start())
        loop(passes, one_pass)

        def finish(n):
            for part in SIDES:
                m_out(part, n).wait()
        loop(nn, finish)

    pl.run_scoped(experts, pltpu.VMEM((RING, 8, hd, width), BF16), pltpu.VMEM((2, q, RING * heads * hd), BF16),
                  pltpu.VMEM((2, d_model // cw, RING, half, cw), F32), pltpu.VMEM((RING * half, fe), BF16),
                  pltpu.VMEM((2, fe, d_model), BF16), pltpu.VMEM((fe, d_model), BF16))

    for side in SIDES:
        w_round(side).wait_send()
        w_forward(side).wait_send()
        for part in SIDES:
            hid_send(part, side).wait_send()
            hid_forward(part, side).wait_send()
        for g in range(pairs):
            ctx_send(g, side).wait_send()
            ctx_forward(g, side).wait_send()
        for c in range(RING):
            a_send(c, side).wait_send()
            a_forward(c, side).wait()
    for k in range(1, RING):
        w_swap(k).wait_send()
        ids_send(k).wait_send()
    for k in SIDES:
        for i in range(len(mats)):
            swap_mat(k, i).wait_send()
    for k in range(RING):
        w_core(k).wait_send()
        a_local(k).wait()


def front_call(x, wq, wk, wv, wo, eg, eu, ed, attn_gain, moe_gain, ids, router):
    tokens, d_model = x.shape
    heads, hd = wq.shape[1], wq.shape[2]
    q = tokens // RING
    local, fe = eg.shape[0], eg.shape[1]
    experts = router.shape[0]
    pairs = heads // 2
    hbm = pl.BlockSpec(memory_space=pl.ANY)
    vmem = pl.BlockSpec(memory_space=pltpu.VMEM)
    dma = pltpu.SemaphoreType.DMA
    sds = jax.ShapeDtypeStruct
    freq = ROPE_BASE ** (np.arange(hd) % (hd // 2) * (-2.0 / hd))
    freq = jnp.asarray(freq.astype(np.float32).reshape(1, hd))
    two, three, four = dma((2,)), dma((3,)), dma((RING,))
    by_pair, by_chunk, square = dma((2, pairs)), dma((2, RING)), dma((2, 2))
    outs = pl.pallas_call(
        front_body,
        out_shape=(sds((tokens, d_model), BF16), sds((RING, 2, q // 2, d_model), F32), sds((RING, tokens, heads * hd), BF16),
                   sds((RING, 2, q // 2, d_model), BF16), sds((RING, ids.shape[0], q), ids.dtype), sds((8, RING, hd, d_model // RING), BF16),
                   sds(eg.shape, BF16), sds(eu.shape, BF16), sds(ed.shape, BF16)),
        in_specs=[hbm] * 8 + [vmem] * 3 + [hbm, vmem],
        out_specs=(hbm,) * 9,
        scratch_shapes=[
            pltpu.VMEM((tokens, d_model), BF16), pltpu.VMEM((pairs, tokens, 2 * hd), BF16), pltpu.VMEM((RING, q, d_model // RING), BF16),
            pltpu.VMEM((2, tokens // 2, experts), F32), pltpu.VMEM((RING, 8, q), ids.dtype),
            dma((RING + 2,)), four, dma((pairs,)), four,
        ] + [by_pair] * RING + [by_chunk] * RING + [square] * RING + [three] * 2 + [two] * RING + [four] * 2 + [three] * 2
          + [dma((2, 3))] * 2 + [by_chunk, two, four, two, two, dma((2, 8))],
        compiler_params=pltpu.CompilerParams(collective_id=0, has_side_effects=True, vmem_limit_bytes=VMEM_LIMIT),
        cost_estimate=pl.CostEstimate(flops=2 * tokens * d_model * (heads * hd * RING + 12 * fe), bytes_accessed=24 * fe * d_model, transcendentals=heads * tokens * tokens),
        name='attn_moe',
    )(x, wq, wk, wv, wo, eg, eu, ed, attn_gain, moe_gain, freq, ids, router)
    return outs[0], outs[1]


def solution(mesh):
    tok_spec = P(('dp', 'ep'))
    col_spec = P(None, 'tp')
    in_specs = (tok_spec,) * 3 + (P(),) + (col_spec,) * 3 + (P('tp'), P(), col_spec, col_spec, P('tp'), P(), P()) + (P('ep'),) * 3

    def layer_local(hidden_in, expert_ids, slot_ids, attn_gain, w_query, w_key, w_value, w_out, ffn_gain, w_gate, w_up, w_down, moe_gain, w_router, exp_gate, exp_up, exp_down):
        num_seqs, seq_len, d_model = hidden_in.shape
        tokens = num_seqs * seq_len
        heads, head_dim = w_out.shape[0], w_out.shape[1]
        x = hidden_in.reshape(tokens, d_model)
        ids = jnp.swapaxes(expert_ids, 1, 2).reshape(expert_ids.shape[2], tokens)
        after_attn, m_part = front_call(
            x, w_query, w_key, w_value, w_out.reshape(heads * head_dim, d_model), jnp.swapaxes(exp_gate, 1, 2), jnp.swapaxes(exp_up, 1, 2), exp_down,
            attn_gain, moe_gain, ids, w_router.T)
        out = ffn_call(after_attn, w_gate.T, w_up.T, w_down, ffn_gain, m_part.reshape(-1, tokens // 4, d_model))
        return out.reshape(hidden_in.shape)

    return jax.shard_map(layer_local, mesh=mesh, in_specs=in_specs, out_specs=tok_spec, check_vma=False)
```

```python
import functools

import jax
import jax.numpy as jnp
import numpy as np
from jax import lax
from jax.experimental import pallas as pl
from jax.experimental.pallas import tpu as pltpu
from jax.sharding import PartitionSpec as P

F32 = jnp.float32
BF16 = jnp.bfloat16
EPS = 1e-6
ROPE_BASE = 10000.0
VMEM_LIMIT = 67043328
MESH = pl.DeviceIdType.MESH
NT = (((1,), (1,)), ((), ()))


RING = 4
SIDES = (0, 1)


def odd(k):
    return lax.rem(k, 2)


def turn(side):
    return 1 - 2 * side


def loop(count, body):
    def step(k, carry):
        body(k)
        return carry
    lax.fori_loop(0, count, step, 0)


def window(index, size):
    return pl.ds(pl.multiple_of(index * size, size), size)


def rcopy(src, dst, ssem, rsem, dev):
    return pltpu.make_async_remote_copy(src_ref=src, dst_ref=dst, send_sem=ssem, recv_sem=rsem, device_id=dev, device_id_type=MESH)


def entry_barrier(neighbours):
    barrier = pltpu.get_barrier_semaphore()
    for dev in neighbours:
        pl.semaphore_signal(barrier, inc=1, device_id=dev, device_id_type=MESH)
    pl.semaphore_wait(barrier, len(neighbours))


def norm_rows(src, dst, gain, rows, step):
    def one(r):
        sl = window(r, step)
        x = src[sl, :].astype(F32)
        inv = lax.rsqrt(jnp.mean(x * x, axis=-1, keepdims=True) + EPS)
        dst[sl, :] = (x * inv * gain[...].astype(F32).reshape(1, -1)).astype(BF16)
    loop(rows // step, one)


def ffn_body(fb, a_ref, wg, wu, wd, gain, m_ref, out_ref,
             a_own, n2, h, wbuf, dbuf, p1, yrecv, xrecv, mbuf,
             asem, wsem, dsem, msem, osem, ys, yr, xs, xr, gs, gr, fs, fr):
    t = lax.axis_index('tp')
    e = lax.axis_index('ep')
    big = odd(e)
    xc = e // 2
    q = a_own.shape[0]
    d_model = a_own.shape[1]
    f_loc = wg.shape[0]
    cw = d_model // 8
    hw = cw // 2
    nf = f_loc // fb
    tail = f_loc - nf * fb
    yright, yleft = {'tp': lax.rem(t + 1, RING)}, {'tp': lax.rem(t + 3, RING)}
    xright, xleft = {'ep': lax.rem(xc + 1, RING) * 2 + big}, {'ep': lax.rem(xc + 3, RING) * 2 + big}

    def cols(cb):
        return window(cb, cw)

    def chunk(c):
        return lax.rem(c + 8, RING)

    def rows(c):
        return window(chunk(c), q)

    def a_load(c, slot):
        return pltpu.make_async_copy(a_ref.at[rows(c)], n2.at[pl.ds(slot * q, q)], asem.at[slot])
    load_own = pltpu.make_async_copy(a_ref.at[rows(t)], a_own, asem.at[2])

    def w_load(i, slot, size):
        sl = pl.ds(pl.multiple_of(i * fb, fb), size)
        return (pltpu.make_async_copy(wg.at[sl], wbuf.at[slot, 0, pl.ds(0, size)], wsem.at[slot, 0]),
                pltpu.make_async_copy(wu.at[sl], wbuf.at[slot, 1, pl.ds(0, size)], wsem.at[slot, 1]))

    def w_start(i):
        slot = lax.rem(i, wbuf.shape[0])

        @pl.when(i < nf)
        def _():
            for c in w_load(i, slot, fb):
                c.start()

        @pl.when(i == nf)
        def _():
            for c in w_load(nf, slot, tail):
                c.start()

    def col_of(j):
        return odd(j) * 4 + j // 2

    def d_load(j):
        start = col_of(j) * cw
        return [pltpu.make_async_copy(wd.at[:, pl.ds(pl.multiple_of(start + sub * hw, hw), hw)], dbuf.at[odd(j), sub], dsem.at[odd(j), sub]) for sub in SIDES]

    def m_load(k):
        s, j = k // 8 + 1, lax.rem(k, 8)
        side = odd(j)
        c = lax.rem(xc + (2 * side - 1) * (1 + s) + 8, RING)
        slot = odd(k)
        return pltpu.make_async_copy(m_ref.at[c, :, cols(col_of(j))], mbuf.at[slot], msem.at[slot])

    def send(buf, ssem, rsem, src, right, left, side, step, i):
        @pl.when(side == 0)
        def _():
            rcopy(src, buf.at[0, step, i], ssem.at[0, step, i], rsem.at[0, step, i], right).start()

        @pl.when(side == 1)
        def _():
            rcopy(src, buf.at[1, step, i], ssem.at[1, step, i], rsem.at[1, step, i], left).start()

    def ysend(src, side, step, i):
        send(yrecv, ys, yr, src, yright, yleft, side, step, i)

    def xsend(src, side, step, i):
        send(xrecv, xs, xr, src, xright, xleft, side, step, i)

    def arrived(buf, ssem, rsem, side, step, i, dev):
        rcopy(buf.at[side, step, i], buf.at[side, step, i], ssem.at[side, step, i], rsem.at[side, step, i], dev).wait_recv()

    def sent(buf, ssem, rsem, side, step, i, dev):
        rcopy(buf.at[side, step, i], buf.at[side, step, i], ssem.at[side, step, i], rsem.at[side, step, i], dev).wait_send()

    def xserve(k):
        s, j = k // 8, lax.rem(k, 8)
        side, i = odd(j), j // 2
        m_load(k + 1).start()
        m_load(k).wait()
        arrived(xrecv, xs, xr, side, s, i, xright)
        xrecv[side, s, i] = xrecv[side, s, i] + mbuf[odd(k)]
        xsend(xrecv.at[side, s, i], side, s + 1, i)

    def gate_up(serve):
        def block(i, size):
            slot = lax.rem(i, wbuf.shape[0])
            w_start(i + 2)
            for c in w_load(i, slot, size):
                c.wait()
            g = lax.dot_general(n2[...], wbuf[slot, 0, pl.ds(0, size)], NT, preferred_element_type=F32)
            u = lax.dot_general(n2[...], wbuf[slot, 1, pl.ds(0, size)], NT, preferred_element_type=F32)
            h[:, pl.ds(pl.multiple_of(i * fb, fb), size)] = (jax.nn.silu(g) * u).astype(BF16)

        def one(i):
            block(i, fb)
            serve(i)
        loop(nf, one)
        block(nf, tail)

    def d_start(j):
        for c in d_load(j):
            c.start()

    def down(ready, use, done):
        def one(j):
            @pl.when(j + 1 < 8)
            def _():
                d_start(j + 1)
            ready(j)
            for c in d_load(j):
                c.wait()
            for sub in SIDES:
                r = jnp.dot(h[...], dbuf[odd(j), sub], preferred_element_type=F32)
                use(j, slice(sub * hw, (sub + 1) * hw), r)
            done(j)
        loop(8, one)

    a_load(t - 1, 0).start()
    a_load(t + 1, 1).start()
    w_start(0)
    w_start(1)
    entry_barrier((yright, yleft, xright, xleft))

    def x_first(i):
        xsend(m_ref.at[chunk(xc - 1), :, cols(i)], 0, 0, i)
        xsend(m_ref.at[chunk(xc + 1), :, cols(4 + i)], 1, 0, i)
    loop(4, x_first)
    d_start(jnp.int32(0))
    m_load(0).start()
    load_own.start()

    for slot in SIDES:
        a_load(t, slot).wait()
        norm_rows(n2.at[pl.ds(slot * q, q)], n2.at[pl.ds(slot * q, q)], gain, q, 16)
    gate_up(lambda i: None)
    a_load(t + 2, 0).start()
    a_load(t, 1).start()
    w_start(0)
    w_start(1)

    def use1(j, part, r):
        p1[col_of(j), :, part] = r

    def done1(j):
        side = odd(j)
        ysend(p1.at[col_of(j), pl.ds(pl.multiple_of(side * q, q), q)], side, 0, j // 2)
    down(lambda j: None, use1, done1)
    d_start(jnp.int32(0))

    for slot in SIDES:
        a_load(t, slot).wait()
        norm_rows(n2.at[pl.ds(slot * q, q)], n2.at[pl.ds(slot * q, q)], gain, q, 16)

    def serve2(i):
        @pl.when(i < 8)
        def _():
            xserve(i)
    gate_up(serve2)
    for k in range(min(nf, 8), 8):
        xserve(k)

    def sent_rows(j):
        return pl.ds(pl.multiple_of(odd(j) * q, q), q)

    def ready2(j):
        arrived(yrecv, ys, yr, odd(j), 0, j // 2, yright)
        sent(yrecv, ys, yr, odd(j), 0, j // 2, yright)

    def use2(j, part, r):
        p1[col_of(j), sent_rows(j), part] = r[q:]
        yrecv[odd(j), 0, j // 2, :, part] = yrecv[odd(j), 0, j // 2, :, part] + r[:q]

    def done2(j):
        ysend(yrecv.at[odd(j), 0, j // 2], odd(j), 1, j // 2)
    down(ready2, use2, done2)

    def third(j):
        side, i = odd(j), j // 2
        xserve(8 + j)
        arrived(yrecv, ys, yr, side, 1, i, yright)
        yrecv[side, 1, i] = yrecv[side, 1, i] + p1[col_of(j), window((1 - side), q)]
        ysend(yrecv.at[side, 1, i], side, 2, i)
    loop(8, third)

    def out_local(cb):
        return pltpu.make_async_copy(n2.at[pl.ds(0, q), cols(cb)], out_ref.at[rows(t), cols(cb)], osem.at[cb])

    def gather(cb, side, dev):
        return rcopy(n2.at[pl.ds(0, q), cols(cb)], out_ref.at[rows(t), cols(cb)], gs.at[side, cb], gr.at[side, cb], dev)

    load_own.wait()

    def last(j):
        side, i = odd(j), j // 2
        cb = col_of(j)
        k = 16 + j

        @pl.when(j + 1 < 8)
        def _():
            m_load(k + 1).start()
        m_load(k).wait()
        arrived(xrecv, xs, xr, side, 2, i, xright)
        arrived(yrecv, ys, yr, side, 2, i, yright)
        b_val = a_own[:, cols(cb)].astype(F32) + (yrecv[side, 2, i] + p1[cb, sent_rows(j)])
        n2[pl.ds(0, q), cols(cb)] = (b_val + (xrecv[side, 2, i] + mbuf[odd(k)])).astype(BF16)
        out_local(cb).start()
        gather(cb, 0, yright).start()
        gather(cb, 1, yleft).start()
    loop(8, last)

    half = q // 2

    def half_rows(c, which):
        return pl.ds(pl.multiple_of(chunk(c) * q + which * half, half), half)

    def forward(c, which, cb, dev):
        ref = out_ref.at[half_rows(c, which), cols(cb)]
        return rcopy(ref, ref, fs.at[which, cb], fr.at[which, cb], dev)

    def pass_on(j):
        cb = col_of(j)
        gather(cb, 0, yright).wait_recv()
        forward(t - 1, 0, cb, yright).start()
        gather(cb, 1, yleft).wait_recv()
        forward(t + 1, 1, cb, yleft).start()
    loop(8, pass_on)

    def finish(j):
        cb = col_of(j)
        out_local(cb).wait()
        for which in SIDES:
            gather(cb, which, yright).wait_send()
            forward(t, which, cb, yright).wait_send()
            forward(t, which, cb, yright).wait_recv()
    loop(8, finish)

    def drain(k):
        step, j = k // 8, lax.rem(k, 8)

        @pl.when(step > 0)
        def _():
            sent(yrecv, ys, yr, odd(j), step, j // 2, yright)
        sent(xrecv, xs, xr, odd(j), step, j // 2, yright)
    loop(24, drain)


def ffn_call(after_attn, wg_t, wu_t, w_down, gain, m_part):
    tokens, d_model = after_attn.shape
    f_loc = wg_t.shape[0]
    fb = 256 if f_loc > 512 else 128
    q = tokens // 4
    cw = d_model // 8
    hbm = pl.BlockSpec(memory_space=pl.ANY)
    vmem = pl.BlockSpec(memory_space=pltpu.VMEM)
    dma = pltpu.SemaphoreType.DMA
    flops = 2 * tokens * d_model * f_loc * 3
    return pl.pallas_call(
        functools.partial(ffn_body, fb),
        out_shape=jax.ShapeDtypeStruct((tokens, d_model), BF16),
        in_specs=[hbm, hbm, hbm, hbm, vmem, hbm],
        out_specs=hbm,
        scratch_shapes=[
            pltpu.VMEM((q, d_model), BF16),
            pltpu.VMEM((2 * q, d_model), BF16),
            pltpu.VMEM((2 * q, f_loc), BF16),
            pltpu.VMEM((3, 2, fb, d_model), BF16),
            pltpu.VMEM((2, 2, f_loc, cw // 2), BF16),
            pltpu.VMEM((8, 2 * q, cw), F32),
            pltpu.VMEM((2, 3, RING, q, cw), F32),
            pltpu.VMEM((2, 3, RING, q, cw), F32),
            pltpu.VMEM((2, q, cw), F32),
            dma((3,)), dma((3, 2)), dma((2, 2)), dma((2,)), dma((8,)),
        ] + [dma((2, 3, RING))] * RING + [dma((2, 8))] * RING,
        compiler_params=pltpu.CompilerParams(collective_id=2, has_side_effects=True, vmem_limit_bytes=VMEM_LIMIT),
        cost_estimate=pl.CostEstimate(flops=flops, bytes_accessed=4 * tokens * d_model + 12 * f_loc * d_model, transcendentals=tokens * f_loc),
        name='ffn_ring',
    )(after_attn, wg_t, wu_t, w_down, gain, m_part)


def front_body(x_ref, wq, wk, wv, wo, eg, eu, ed, attn_gain, moe_gain, freq, ids, router,
               a_full, m_part, ctx_all, hid_all, ids_all, w_cols, og, ou, od,
               xn, ctxb, abuf, gate, idf,
               lsem, rawsem, cls, als, cs, cr, cfs, cfr, as_, ar, afs, afr, hs, hr, hfs, hfr, ws, wr, wxs, wxr, wfs, wfr,
               wds, wdr, ins, inr, es, er, csem, xsem, usem, wsem, dsem, msem):
    t = lax.axis_index('tp')
    e = lax.axis_index('ep')
    core = odd(e)
    xc = e // 2
    tokens, d_model = xn.shape
    heads, hd = wq.shape[1], wq.shape[2]
    q = tokens // RING
    half = q // 2
    width = d_model // RING
    kblk = min(512, d_model // RING)
    nk = d_model // kblk
    pair = 2 * hd
    pairs = heads // 2
    local, fe = eg.shape[0], eg.shape[1]
    top_k = ids.shape[0]
    partner = {'ep': xc * 2 + 1 - core}

    def ring(k):
        return lax.rem(k + RING, RING)

    def y_dev(k):
        return {'tp': ring(t + k)}

    def x_id(k):
        return ring(xc + k) * 2 + core

    def x_dev(k):
        return {'ep': x_id(k)}

    def w_swap(k):
        return rcopy(wo.at[window(e, hd), window(ring(t + k), width)], w_cols.at[e, t], ws.at[k - 1], wr.at[k - 1], y_dev(k))

    def w_round(side):
        return rcopy(w_cols.at[e], w_cols.at[e], wxs.at[side], wxr.at[side], x_dev(turn(side)))

    def w_forward(side):
        ref = w_cols.at[x_id(2 * side - 1), pl.ds(2 * side, 2)]
        return rcopy(ref, ref, wfs.at[side], wfr.at[side], x_dev(turn(side)))

    def w_core(k):
        return rcopy(w_cols.at[x_id(k)], w_cols.at[x_id(k)], wds.at[k], wdr.at[k], partner)

    def hid_send(part, side):
        return rcopy(hid_all.at[xc, part], hid_all.at[xc, part], hs.at[part, side], hr.at[part, side], x_dev(turn(side)))

    def hid_forward(part, side):
        ref = hid_all.at[ring(xc + 2 * side - 1), part, pl.ds(side * (half // 2), half // 2)]
        return rcopy(ref, ref, hfs.at[part, side], hfr.at[part, side], x_dev(turn(side)))

    def ids_send(k):
        return rcopy(ids.at[:, window(t, q)], ids_all.at[xc], ins.at[k - 1], inr.at[k - 1], x_dev(k))

    mats = ((eg, og), (eu, ou), (ed, od))

    def swap_mat(k, i):
        return rcopy(mats[i][0].at[k], mats[i][1].at[k], es.at[k, i], er.at[k, i], partner)

    def ctx_local(g):
        return pltpu.make_async_copy(ctxb.at[g], ctx_all.at[t, :, window(g, pair)], cls.at[g])

    def ctx_send(g, side):
        return rcopy(ctxb.at[g], ctx_all.at[t, :, window(g, pair)], cs.at[side, g], cr.at[side, g], y_dev(turn(side)))

    def ctx_forward(g, side):
        ref = ctx_all.at[ring(t + 2 * side - 1), pl.ds(side * (tokens // 2), tokens // 2), window(g, pair)]
        return rcopy(ref, ref, cfs.at[side, g], cfr.at[side, g], y_dev(turn(side)))

    def ctx_pass(g):
        for side in SIDES:
            ctx_send(g, side).wait_recv()
            ctx_forward(g, side).start()

    def a_local(c):
        return pltpu.make_async_copy(abuf.at[c], a_full.at[window(c, q), window(t, width)], als.at[c])

    def a_send(c, side):
        return rcopy(abuf.at[c], a_full.at[window(c, q), window(t, width)], as_.at[side, c], ar.at[side, c], y_dev(turn(side)))

    def a_forward(c, side):
        rows = pl.ds(pl.multiple_of(c * q + side * half, half), half)
        ref = a_full.at[rows, window(ring(t + 2 * side - 1), width)]
        return rcopy(ref, ref, afs.at[side, c], afr.at[side, c], y_dev(turn(side)))

    def a_pass(c):
        for side in SIDES:
            a_send(c, side).wait_recv()
            a_forward(c, side).start()

    load_x = [pltpu.make_async_copy(x_ref.at[pl.ds(k * q, q)], xn.at[pl.ds(k * q, q)], lsem.at[k]) for k in range(RING)]
    for c in load_x:
        c.start()
    w_own = pltpu.make_async_copy(wo.at[window(e, hd), window(t, width)], w_cols.at[e, t], lsem.at[RING])
    ids_own = pltpu.make_async_copy(ids.at[:, window(t, q)], ids_all.at[xc], lsem.at[RING + 1])

    def attention(rope, raw, wide, wide2, wb, qb, kb, vb, ub):
        proj = (wq, wk, wv)
        deep = raw.shape[0]
        share = tokens // nk
        step = min(16, share)

        def raw_load(m, k):
            slot = lax.rem(k, deep)
            return pltpu.make_async_copy(proj[m].at[window(k, kblk)], raw.at[slot], rawsem.at[slot])

        def rows_of(m, k):
            slot = lax.rem(k, deep)
            part = kblk // 2
            for i, buf in enumerate((wide, wide2)):
                buf[...] = raw[slot, i * part:(i + 1) * part].astype(F32).reshape(part * heads, hd)
            for i, buf in enumerate((wide, wide2)):
                rows = pl.ds(pl.multiple_of(k * kblk + i * part, part), part)
                for h in range(heads):
                    wb[m, rows, h * hd:(h + 1) * hd] = buf[pl.ds(h, part, stride=heads), :].astype(BF16)

        def raw_next(m, k):
            @pl.when(k + deep < nk)
            def _():
                raw_load(m, k + deep).start()

            if m + 1 < len(proj):
                @pl.when(k + deep >= nk)
                def _():
                    raw_load(m + 1, k + deep - nk).start()

        own = pltpu.make_async_copy(x_ref.at[window(t, q)], ub, lsem.at[RING + 2])
        own.start()
        for k in range(deep):
            raw_load(0, k).start()
        entry_barrier((y_dev(1), y_dev(-1), y_dev(2), x_dev(1), x_dev(-1), x_dev(2), partner))
        w_own.start()
        ids_own.start()
        for k in range(1, RING):
            w_swap(k).start()
            ids_send(k).start()
        for i in range(len(mats)):
            swap_mat(0, i).start()

        own.wait()
        norm_rows(ub, ub, moe_gain, q, 16)
        keep = [pltpu.make_async_copy(ub.at[pl.ds(part * half, half)], hid_all.at[xc, part], lsem.at[RING + 2 + part]) for part in SIDES]
        for c in keep:
            c.start()

        sign = jnp.where(lax.broadcasted_iota(jnp.int32, (1, hd), 1) < hd // 2, -1.0, 1.0)
        steps = min(128, tokens)

        def angles(k):
            angle = (lax.broadcasted_iota(jnp.int32, (steps, 1), 0) + k * steps).astype(F32) * freq[...]
            rope[0, window(k, steps)] = jnp.cos(angle)
            rope[1, window(k, steps)] = jnp.sin(angle) * sign
        loop(tokens // steps, angles)
        for c in keep:
            c.wait()
        for side in SIDES:
            hid_send(0, side).start()
        for k in range(RING):
            load_x[k].wait()

        for m in range(len(proj)):
            def one(k, m=m):
                raw_load(m, k).wait()
                rows_of(m, k)
                if m == 0:
                    for i in range(0, share, step):
                        rows = pl.ds(pl.multiple_of(k * share + i, step), step)
                        x = xn[rows, :].astype(F32)
                        inv = lax.rsqrt(jnp.mean(x * x, axis=-1, keepdims=True) + EPS)
                        xn[rows, :] = (x * inv * attn_gain[...].astype(F32).reshape(1, -1)).astype(BF16)
                raw_next(m, k)
            loop(nk, one)

        def turned(r):
            for h in SIDES:
                part = r[:, h * hd:(h + 1) * hd]
                yield (part * rope[0] + pltpu.roll(part, hd // 2, 1) * rope[1]).astype(BF16)

        def project(m, g):
            return jnp.dot(xn[...], wb[m, :, window(g, pair)], preferred_element_type=F32)

        w_own.wait()
        for k in range(1, RING):
            w_swap(k).wait_recv()
        for side in SIDES:
            w_round(side).start()
        w_core(0).start()

        scale = hd ** -0.5
        tri = lax.broadcasted_iota(jnp.int32, (q, q), 0) >= lax.broadcasted_iota(jnp.int32, (q, q), 1)

        def heads_of(g):
            for m, dst in enumerate((qb, kb)):
                for h, part in enumerate(turned(project(m, g))):
                    dst[:, h * hd:(h + 1) * hd] = part
            vb[...] = project(2, g).astype(BF16)
            for h in SIDES:
                hc = slice(h * hd, (h + 1) * hd)
                for b in range(RING):
                    s = lax.dot_general(qb[b * q:(b + 1) * q, hc], kb[0:(b + 1) * q, hc], NT, preferred_element_type=F32) * scale
                    diag = jnp.where(tri, s[:, b * q:], -1e30)
                    s = diag if b == 0 else jnp.concatenate([s[:, :b * q], diag], axis=1)
                    w = jnp.exp(s - jnp.max(s, axis=-1, keepdims=True))
                    prob = (w * (1.0 / jnp.sum(w, axis=-1, keepdims=True))).astype(BF16)
                    ctxb[g, b * q:(b + 1) * q, hc] = jnp.dot(prob, vb[0:(b + 1) * q, hc], preferred_element_type=F32).astype(BF16)
            ctx_local(g).start()
            for side in SIDES:
                ctx_send(g, side).start()

            @pl.when(g == 0)
            def _():
                for side in SIDES:
                    hid_send(0, side).wait_recv()
                    hid_forward(0, side).start()

            @pl.when(g >= 2)
            def _():
                ctx_pass(g - 2)

            @pl.when(g == 2)
            def _():
                for side in SIDES:
                    w_round(side).wait_recv()
                    w_forward(side).start()
                w_core(1).start()
                w_core(RING - 1).start()

            @pl.when(g == pairs - 1)
            def _():
                for side in SIDES:
                    hid_send(1, side).start()
        loop(pairs, heads_of)

    pl.run_scoped(attention, pltpu.VMEM((2, tokens, hd), F32), pltpu.VMEM((RING, kblk, heads, hd), BF16), *[pltpu.VMEM((kblk // 2 * heads, hd), F32)] * 2,
                  pltpu.VMEM((3, d_model, heads * hd), BF16), *[pltpu.VMEM((tokens, pair), BF16)] * 3, pltpu.VMEM((q, d_model), BF16))

    fb = 256 if fe > 512 else 128
    cw = min(512, d_model // 4)

    def experts(wcv, cbuf, mv, act, wbuf, dbuf):
        sizes = [fb] * (fe // fb) + [fe % fb]
        cw = mv.shape[-1]
        nn = d_model // cw
        passes = 4 * local
        last = passes - 2

        def expert_of(p):
            late = p // last
            return (1 - late) * lax.rem(p, 3) + late * 3

        def half_of(p):
            late = p // last
            return (1 - late) * (p // 3) + late * (p - last)

        def w_load(k, own):
            k = k if own else k - local
            return [pltpu.make_async_copy(ref.at[k], wbuf.at[i], wsem.at[i]) for i, ref in enumerate((eg, eu) if own else (og, ou))]

        def d_load(k, own):
            return [pltpu.make_async_copy((ed if own else od).at[k if own else k - local], dbuf, dsem.at[0])]

        def start(p, load):
            k = expert_of(p)

            @pl.when(jnp.logical_and(p < passes, k < local))
            def _():
                for c in load(k, True):
                    c.start()

            @pl.when(jnp.logical_and(p < passes, k >= local))
            def _():
                for c in load(k, False):
                    c.start()

        def u_rows(part, k):
            return xn.at[pl.ds(pl.multiple_of((part * RING + k) * half, half), half)]

        def u_ready(part):
            for k in range(RING):
                pltpu.make_async_copy(hid_all.at[k, part], u_rows(part, k), usem.at[k]).start()
            for k in range(RING):
                pltpu.make_async_copy(hid_all.at[k, part], u_rows(part, k), usem.at[k]).wait()
            rows = RING * half
            u = xn.at[pl.ds(part * rows, rows)]
            logits = lax.dot_general(u[...], router[...], NT, preferred_element_type=F32)
            lane = lax.broadcasted_iota(jnp.int32, logits.shape, 1).astype(F32)
            picks = jnp.concatenate([idf[k, :, part * half:(part + 1) * half].astype(F32) for k in range(RING)], axis=1).T
            chosen = lane == picks[:, 0:1]
            for j in range(1, top_k):
                chosen = jnp.logical_or(chosen, lane == picks[:, j:j + 1])
            top = jnp.max(jnp.where(chosen, logits, -jnp.inf), axis=-1, keepdims=True)
            w = jnp.where(chosen, jnp.exp(jnp.where(chosen, logits - top, 0.0)), 0.0)
            gate[part] = w / jnp.sum(w, axis=-1, keepdims=True)

        def ctx_load(c):
            return [pltpu.make_async_copy(ctx_all.at[k, window(c, q)], cbuf.at[odd(c), :, pl.ds(k * heads * hd, heads * hd)], csem.at[odd(c), k]) for k in range(RING)]

        def x_load(c):
            return pltpu.make_async_copy(x_ref.at[window(c, q), window(t, width)], abuf.at[c], xsem.at[odd(c)])

        load_w = [pltpu.make_async_copy(w_cols.at[:, k], wcv.at[k], lsem.at[k]) for k in range(RING)]

        def attention_out():
            for side in SIDES:
                for g in range(pairs):
                    ctx_forward(g, side).wait_recv()
            for g in range(pairs):
                ctx_local(g).wait()
            for c in ctx_load(jnp.int32(0)):
                c.start()
            x_load(jnp.int32(0)).start()
            for c in load_w:
                c.wait()

            def chunk(c):
                @pl.when(c + 1 < RING)
                def _():
                    for d in ctx_load(c + 1):
                        d.start()
                    x_load(c + 1).start()
                for d in ctx_load(c):
                    d.wait()
                x_load(c).wait()
                o = jnp.dot(cbuf[odd(c)], wcv[...].reshape(RING * heads * hd, width), preferred_element_type=F32)
                abuf[c] = (abuf[c].astype(F32) + o).astype(BF16)
                a_local(c).start()
                for side in SIDES:
                    a_send(c, side).start()
            loop(RING, chunk)

        def m_out(part, n):
            return pltpu.make_async_copy(mv.at[part, n], m_part.at[:, part, :, window(n, cw)], msem.at[part, n])

        start(jnp.int32(0), w_load)
        ids_own.wait()
        for k in range(1, RING):
            ids_send(k).wait_recv()
        load_i = pltpu.make_async_copy(ids_all, idf.at[:, pl.ds(0, top_k)], lsem.at[RING + 1])
        load_i.start()
        for side in SIDES:
            hid_forward(0, side).wait_recv()
        load_i.wait()
        u_ready(0)

        def one_pass(p):
            @pl.when(p == 1)
            def _():
                ctx_pass(pairs - 2)
                for side in SIDES:
                    w_forward(side).wait_recv()
                w_core(2).start()
                for i in range(len(mats)):
                    swap_mat(1, i).start()

            @pl.when(p == 2)
            def _():
                for k in range(RING):
                    w_core(k).wait_recv()
                for c in load_w:
                    c.start()

            @pl.when(p == 3)
            def _():
                ctx_pass(pairs - 1)
                for side in SIDES:
                    hid_send(1, side).wait_recv()
                    hid_forward(1, side).start()
                attention_out()
                for side in SIDES:
                    hid_forward(1, side).wait_recv()
                u_ready(1)

            @pl.when(p >= RING)
            def _():
                a_pass(p - RING)
            k, part = expert_of(p), half_of(p)
            which = (k // local) * ((e + 1 - 2 * core) * local + k - local) + (1 - k // local) * (e * local + k)
            rows = RING * half
            u = xn.at[pl.ds(pl.multiple_of(part * rows, rows), rows)]
            lane = lax.broadcasted_iota(jnp.int32, gate.shape[1:], 1)
            weight = jnp.sum(jnp.where(lane == which, gate[part], 0.0), axis=1, keepdims=True)

            def if_new(ahead, which_mats):
                for late, when in enumerate((3, last + 1)):
                    @pl.when(ahead == when)
                    def _():
                        for i in which_mats:
                            swap_mat(late, i).wait_recv()
            if_new(p + 1, (2,))
            start(p, d_load)
            for c in w_load(0, True):
                c.wait()
            for b, size in enumerate(sizes):
                cols = slice(b * fb, b * fb + size)
                g = lax.dot_general(u[...], wbuf[0, cols], NT, preferred_element_type=F32)
                v = lax.dot_general(u[...], wbuf[1, cols], NT, preferred_element_type=F32)
                act[:, cols] = (jax.nn.silu(g) * v).astype(BF16)
            if_new(p + 2, SIDES)
            start(p + 1, w_load)
            for c in d_load(0, True):
                c.wait()
            for n in range(nn):
                y = jnp.dot(act[...], dbuf[:, n * cw:(n + 1) * cw], preferred_element_type=F32).astype(BF16)
                term = jnp.where(weight > 0.0, weight * y.astype(F32), 0.0).reshape(mv.shape[2:])
                mv[part, n] = jnp.where(k == 0, term, mv[part, n] + term)

            @pl.when(p >= last)
            def _():
                loop(nn, lambda n: m_out(part, n).start())
        loop(passes, one_pass)

        def finish(n):
            for part in SIDES:
                m_out(part, n).wait()
        loop(nn, finish)

    pl.run_scoped(experts, pltpu.VMEM((RING, 8, hd, width), BF16), pltpu.VMEM((2, q, RING * heads * hd), BF16),
                  pltpu.VMEM((2, d_model // cw, RING, half, cw), F32), pltpu.VMEM((RING * half, fe), BF16),
                  pltpu.VMEM((2, fe, d_model), BF16), pltpu.VMEM((fe, d_model), BF16))

    for side in SIDES:
        w_round(side).wait_send()
        w_forward(side).wait_send()
        for part in SIDES:
            hid_send(part, side).wait_send()
            hid_forward(part, side).wait_send()
        for g in range(pairs):
            ctx_send(g, side).wait_send()
            ctx_forward(g, side).wait_send()
        for c in range(RING):
            a_send(c, side).wait_send()
            a_forward(c, side).wait()
    for k in range(1, RING):
        w_swap(k).wait_send()
        ids_send(k).wait_send()
    for k in SIDES:
        for i in range(len(mats)):
            swap_mat(k, i).wait_send()
    for k in range(RING):
        w_core(k).wait_send()
        a_local(k).wait()


def front_call(x, wq, wk, wv, wo, eg, eu, ed, attn_gain, moe_gain, ids, router):
    tokens, d_model = x.shape
    heads, hd = wq.shape[1], wq.shape[2]
    q = tokens // RING
    local, fe = eg.shape[0], eg.shape[1]
    experts = router.shape[0]
    pairs = heads // 2
    hbm = pl.BlockSpec(memory_space=pl.ANY)
    vmem = pl.BlockSpec(memory_space=pltpu.VMEM)
    dma = pltpu.SemaphoreType.DMA
    sds = jax.ShapeDtypeStruct
    freq = ROPE_BASE ** (np.arange(hd) % (hd // 2) * (-2.0 / hd))
    freq = jnp.asarray(freq.astype(np.float32).reshape(1, hd))
    two, three, four = dma((2,)), dma((3,)), dma((RING,))
    by_pair, by_chunk, square = dma((2, pairs)), dma((2, RING)), dma((2, 2))
    outs = pl.pallas_call(
        front_body,
        out_shape=(sds((tokens, d_model), BF16), sds((RING, 2, q // 2, d_model), F32), sds((RING, tokens, heads * hd), BF16),
                   sds((RING, 2, q // 2, d_model), BF16), sds((RING, ids.shape[0], q), ids.dtype), sds((8, RING, hd, d_model // RING), BF16),
                   sds(eg.shape, BF16), sds(eu.shape, BF16), sds(ed.shape, BF16)),
        in_specs=[hbm] * 8 + [vmem] * 3 + [hbm, vmem],
        out_specs=(hbm,) * 9,
        scratch_shapes=[
            pltpu.VMEM((tokens, d_model), BF16), pltpu.VMEM((pairs, tokens, 2 * hd), BF16), pltpu.VMEM((RING, q, d_model // RING), BF16),
            pltpu.VMEM((2, tokens // 2, experts), F32), pltpu.VMEM((RING, 8, q), ids.dtype),
            dma((RING + RING,)), four, dma((pairs,)), four,
        ] + [by_pair] * RING + [by_chunk] * RING + [square] * RING + [three] * 2 + [two] * RING + [four] * 2 + [three] * 2
          + [dma((2, 3))] * 2 + [by_chunk, two, four, two, two, dma((2, 8))],
        compiler_params=pltpu.CompilerParams(collective_id=0, has_side_effects=True, vmem_limit_bytes=VMEM_LIMIT),
        cost_estimate=pl.CostEstimate(flops=2 * tokens * d_model * (heads * hd * RING + 12 * fe), bytes_accessed=24 * fe * d_model, transcendentals=heads * tokens * tokens),
        name='attn_moe',
    )(x, wq, wk, wv, wo, eg, eu, ed, attn_gain, moe_gain, freq, ids, router)
    return outs[0], outs[1]


def copy_body(src, dst):
    dst[...] = src[...]


def copy_out(x):
    rows = x.shape[0] // 8
    spec = pl.BlockSpec((rows, x.shape[1]), lambda i: (i, 0))
    return pl.pallas_call(copy_body, out_shape=jax.ShapeDtypeStruct(x.shape, x.dtype), grid=(8,), in_specs=[spec], out_specs=spec, name='copy_out')(x)


def solution(mesh):
    tok_spec = P(('dp', 'ep'))
    col_spec = P(None, 'tp')
    in_specs = (tok_spec,) * 3 + (P(),) + (col_spec,) * 3 + (P('tp'), P(), col_spec, col_spec, P('tp'), P(), P()) + (P('ep'),) * 3

    def layer_local(hidden_in, expert_ids, slot_ids, attn_gain, w_query, w_key, w_value, w_out, ffn_gain, w_gate, w_up, w_down, moe_gain, w_router, exp_gate, exp_up, exp_down):
        num_seqs, seq_len, d_model = hidden_in.shape
        tokens = num_seqs * seq_len
        heads, head_dim = w_out.shape[0], w_out.shape[1]
        x = hidden_in.reshape(tokens, d_model)
        ids = jnp.swapaxes(expert_ids, 1, 2).reshape(expert_ids.shape[2], tokens)
        after_attn, m_part = front_call(
            x, w_query, w_key, w_value, w_out.reshape(heads * head_dim, d_model), jnp.swapaxes(exp_gate, 1, 2), jnp.swapaxes(exp_up, 1, 2), exp_down,
            attn_gain, moe_gain, ids, w_router.T)
        out = ffn_call(after_attn, w_gate.T, w_up.T, w_down, ffn_gain, m_part.reshape(-1, tokens // 4, d_model))
        return copy_out(out).reshape(hidden_in.shape)

    return jax.shard_map(layer_local, mesh=mesh, in_specs=in_specs, out_specs=tok_spec, check_vma=False)
```

```python
import functools

import jax
import jax.numpy as jnp
import numpy as np
from jax import lax
from jax.experimental import pallas as pl
from jax.experimental.pallas import tpu as pltpu
from jax.sharding import PartitionSpec as P

F32 = jnp.float32
BF16 = jnp.bfloat16
EPS = 1e-6
ROPE_BASE = 10000.0
VMEM_LIMIT = 67043328
MESH = pl.DeviceIdType.MESH
NT = (((1,), (1,)), ((), ()))


RING = 4
SIDES = (0, 1)


def odd(k):
    return lax.rem(k, 2)


def turn(side):
    return 1 - 2 * side


def loop(count, body):
    def step(k, carry):
        body(k)
        return carry
    lax.fori_loop(0, count, step, 0)


def window(index, size):
    return pl.ds(pl.multiple_of(index * size, size), size)


def rcopy(src, dst, ssem, rsem, dev):
    return pltpu.make_async_remote_copy(src_ref=src, dst_ref=dst, send_sem=ssem, recv_sem=rsem, device_id=dev, device_id_type=MESH)


def entry_barrier(neighbours):
    barrier = pltpu.get_barrier_semaphore()
    for dev in neighbours:
        pl.semaphore_signal(barrier, inc=1, device_id=dev, device_id_type=MESH)
    pl.semaphore_wait(barrier, len(neighbours))


def norm_rows(src, dst, gain, rows, step):
    def one(r):
        sl = window(r, step)
        x = src[sl, :].astype(F32)
        inv = lax.rsqrt(jnp.mean(x * x, axis=-1, keepdims=True) + EPS)
        dst[sl, :] = (x * inv * gain[...].astype(F32).reshape(1, -1)).astype(BF16)
    loop(rows // step, one)


def ffn_body(fb, a_ref, wg, wu, wd, gain, m_ref, out_ref,
             a_own, n2, h, wbuf, dbuf, p1, yrecv, xrecv, mbuf,
             asem, wsem, dsem, msem, osem, ys, yr, xs, xr, gs, gr, fs, fr):
    t = lax.axis_index('tp')
    e = lax.axis_index('ep')
    big = odd(e)
    xc = e // 2
    q = a_own.shape[0]
    d_model = a_own.shape[1]
    f_loc = wg.shape[0]
    cw = d_model // 8
    hw = cw // 2
    nf = f_loc // fb
    tail = f_loc - nf * fb
    yright, yleft = {'tp': lax.rem(t + 1, RING)}, {'tp': lax.rem(t + 3, RING)}
    xright, xleft = {'ep': lax.rem(xc + 1, RING) * 2 + big}, {'ep': lax.rem(xc + 3, RING) * 2 + big}

    def cols(cb):
        return window(cb, cw)

    def chunk(c):
        return lax.rem(c + 8, RING)

    def rows(c):
        return window(chunk(c), q)

    def a_load(c, slot):
        return pltpu.make_async_copy(a_ref.at[rows(c)], n2.at[pl.ds(slot * q, q)], asem.at[slot])
    load_own = pltpu.make_async_copy(a_ref.at[rows(t)], a_own, asem.at[2])

    def w_load(i, slot, size):
        sl = pl.ds(pl.multiple_of(i * fb, fb), size)
        return (pltpu.make_async_copy(wg.at[sl], wbuf.at[slot, 0, pl.ds(0, size)], wsem.at[slot, 0]),
                pltpu.make_async_copy(wu.at[sl], wbuf.at[slot, 1, pl.ds(0, size)], wsem.at[slot, 1]))

    def w_start(i):
        slot = lax.rem(i, wbuf.shape[0])

        @pl.when(i < nf)
        def _():
            for c in w_load(i, slot, fb):
                c.start()

        @pl.when(i == nf)
        def _():
            for c in w_load(nf, slot, tail):
                c.start()

    def col_of(j):
        return odd(j) * 4 + j // 2

    def d_load(j):
        start = col_of(j) * cw
        return [pltpu.make_async_copy(wd.at[:, pl.ds(pl.multiple_of(start + sub * hw, hw), hw)], dbuf.at[odd(j), sub], dsem.at[odd(j), sub]) for sub in SIDES]

    def m_load(k):
        s, j = k // 8 + 1, lax.rem(k, 8)
        side = odd(j)
        c = lax.rem(xc + (2 * side - 1) * (1 + s) + 8, RING)
        slot = odd(k)
        return pltpu.make_async_copy(m_ref.at[c, :, cols(col_of(j))], mbuf.at[slot], msem.at[slot])

    def send(buf, ssem, rsem, src, right, left, side, step, i):
        @pl.when(side == 0)
        def _():
            rcopy(src, buf.at[0, step, i], ssem.at[0, step, i], rsem.at[0, step, i], right).start()

        @pl.when(side == 1)
        def _():
            rcopy(src, buf.at[1, step, i], ssem.at[1, step, i], rsem.at[1, step, i], left).start()

    def ysend(src, side, step, i):
        send(yrecv, ys, yr, src, yright, yleft, side, step, i)

    def xsend(src, side, step, i):
        send(xrecv, xs, xr, src, xright, xleft, side, step, i)

    def arrived(buf, ssem, rsem, side, step, i, dev):
        rcopy(buf.at[side, step, i], buf.at[side, step, i], ssem.at[side, step, i], rsem.at[side, step, i], dev).wait_recv()

    def sent(buf, ssem, rsem, side, step, i, dev):
        rcopy(buf.at[side, step, i], buf.at[side, step, i], ssem.at[side, step, i], rsem.at[side, step, i], dev).wait_send()

    def xserve(k):
        s, j = k // 8, lax.rem(k, 8)
        side, i = odd(j), j // 2
        m_load(k + 1).start()
        m_load(k).wait()
        arrived(xrecv, xs, xr, side, s, i, xright)
        xrecv[side, s, i] = xrecv[side, s, i] + mbuf[odd(k)]
        xsend(xrecv.at[side, s, i], side, s + 1, i)

    def gate_up(serve):
        def block(i, size):
            slot = lax.rem(i, wbuf.shape[0])
            w_start(i + 2)
            for c in w_load(i, slot, size):
                c.wait()
            g = lax.dot_general(n2[...], wbuf[slot, 0, pl.ds(0, size)], NT, preferred_element_type=F32)
            u = lax.dot_general(n2[...], wbuf[slot, 1, pl.ds(0, size)], NT, preferred_element_type=F32)
            h[:, pl.ds(pl.multiple_of(i * fb, fb), size)] = (jax.nn.silu(g) * u).astype(BF16)

        def one(i):
            block(i, fb)
            serve(i)
        loop(nf, one)
        block(nf, tail)

    def d_start(j):
        for c in d_load(j):
            c.start()

    def down(ready, use, done):
        def one(j):
            @pl.when(j + 1 < 8)
            def _():
                d_start(j + 1)
            ready(j)
            for c in d_load(j):
                c.wait()
            for sub in SIDES:
                r = jnp.dot(h[...], dbuf[odd(j), sub], preferred_element_type=F32)
                use(j, slice(sub * hw, (sub + 1) * hw), r)
            done(j)
        loop(8, one)

    a_load(t - 1, 0).start()
    a_load(t + 1, 1).start()
    w_start(0)
    w_start(1)
    entry_barrier((yright, yleft, xright, xleft))

    def x_first(i):
        xsend(m_ref.at[chunk(xc - 1), :, cols(i)], 0, 0, i)
        xsend(m_ref.at[chunk(xc + 1), :, cols(4 + i)], 1, 0, i)
    loop(4, x_first)
    d_start(jnp.int32(0))
    m_load(0).start()
    load_own.start()

    for slot in SIDES:
        a_load(t, slot).wait()
        norm_rows(n2.at[pl.ds(slot * q, q)], n2.at[pl.ds(slot * q, q)], gain, q, 16)
    gate_up(lambda i: None)
    a_load(t + 2, 0).start()
    a_load(t, 1).start()
    w_start(0)
    w_start(1)

    def use1(j, part, r):
        p1[col_of(j), :, part] = r

    def done1(j):
        side = odd(j)
        ysend(p1.at[col_of(j), pl.ds(pl.multiple_of(side * q, q), q)], side, 0, j // 2)
    down(lambda j: None, use1, done1)
    d_start(jnp.int32(0))

    for slot in SIDES:
        a_load(t, slot).wait()
        norm_rows(n2.at[pl.ds(slot * q, q)], n2.at[pl.ds(slot * q, q)], gain, q, 16)

    def serve2(i):
        @pl.when(i < 8)
        def _():
            xserve(i)
    gate_up(serve2)
    for k in range(min(nf, 8), 8):
        xserve(k)

    def sent_rows(j):
        return pl.ds(pl.multiple_of(odd(j) * q, q), q)

    def ready2(j):
        arrived(yrecv, ys, yr, odd(j), 0, j // 2, yright)
        sent(yrecv, ys, yr, odd(j), 0, j // 2, yright)

    def use2(j, part, r):
        p1[col_of(j), sent_rows(j), part] = r[q:]
        yrecv[odd(j), 0, j // 2, :, part] = yrecv[odd(j), 0, j // 2, :, part] + r[:q]

    def done2(j):
        ysend(yrecv.at[odd(j), 0, j // 2], odd(j), 1, j // 2)
    down(ready2, use2, done2)

    def third(j):
        side, i = odd(j), j // 2
        xserve(8 + j)
        arrived(yrecv, ys, yr, side, 1, i, yright)
        yrecv[side, 1, i] = yrecv[side, 1, i] + p1[col_of(j), window((1 - side), q)]
        ysend(yrecv.at[side, 1, i], side, 2, i)
    loop(8, third)

    def out_local(cb):
        return pltpu.make_async_copy(n2.at[pl.ds(0, q), cols(cb)], out_ref.at[rows(t), cols(cb)], osem.at[cb])

    def gather(cb, side, dev):
        return rcopy(n2.at[pl.ds(0, q), cols(cb)], out_ref.at[rows(t), cols(cb)], gs.at[side, cb], gr.at[side, cb], dev)

    load_own.wait()

    def last(j):
        side, i = odd(j), j // 2
        cb = col_of(j)
        k = 16 + j

        @pl.when(j + 1 < 8)
        def _():
            m_load(k + 1).start()
        m_load(k).wait()
        arrived(xrecv, xs, xr, side, 2, i, xright)
        arrived(yrecv, ys, yr, side, 2, i, yright)
        b_val = a_own[:, cols(cb)].astype(F32) + (yrecv[side, 2, i] + p1[cb, sent_rows(j)])
        n2[pl.ds(0, q), cols(cb)] = (b_val + (xrecv[side, 2, i] + mbuf[odd(k)])).astype(BF16)
        out_local(cb).start()
        gather(cb, 0, yright).start()
        gather(cb, 1, yleft).start()
    loop(8, last)

    half = q // 2

    def half_rows(c, which):
        return pl.ds(pl.multiple_of(chunk(c) * q + which * half, half), half)

    def forward(c, which, cb, dev):
        ref = out_ref.at[half_rows(c, which), cols(cb)]
        return rcopy(ref, ref, fs.at[which, cb], fr.at[which, cb], dev)

    def pass_on(j):
        cb = col_of(j)
        gather(cb, 0, yright).wait_recv()
        forward(t - 1, 0, cb, yright).start()
        gather(cb, 1, yleft).wait_recv()
        forward(t + 1, 1, cb, yleft).start()
    loop(8, pass_on)

    def finish(j):
        cb = col_of(j)
        out_local(cb).wait()
        for which in SIDES:
            gather(cb, which, yright).wait_send()
            forward(t, which, cb, yright).wait_send()
            forward(t, which, cb, yright).wait_recv()
    loop(8, finish)

    def drain(k):
        step, j = k // 8, lax.rem(k, 8)

        @pl.when(step > 0)
        def _():
            sent(yrecv, ys, yr, odd(j), step, j // 2, yright)
        sent(xrecv, xs, xr, odd(j), step, j // 2, yright)
    loop(24, drain)


def ffn_call(after_attn, wg_t, wu_t, w_down, gain, m_part):
    tokens, d_model = after_attn.shape
    f_loc = wg_t.shape[0]
    fb = 256 if f_loc > 512 else 128
    q = tokens // 4
    cw = d_model // 8
    hbm = pl.BlockSpec(memory_space=pl.ANY)
    vmem = pl.BlockSpec(memory_space=pltpu.VMEM)
    dma = pltpu.SemaphoreType.DMA
    flops = 2 * tokens * d_model * f_loc * 3
    return pl.pallas_call(
        functools.partial(ffn_body, fb),
        out_shape=jax.ShapeDtypeStruct((tokens, d_model), BF16),
        in_specs=[hbm, hbm, hbm, hbm, vmem, hbm],
        out_specs=hbm,
        scratch_shapes=[
            pltpu.VMEM((q, d_model), BF16),
            pltpu.VMEM((2 * q, d_model), BF16),
            pltpu.VMEM((2 * q, f_loc), BF16),
            pltpu.VMEM((3, 2, fb, d_model), BF16),
            pltpu.VMEM((2, 2, f_loc, cw // 2), BF16),
            pltpu.VMEM((8, 2 * q, cw), F32),
            pltpu.VMEM((2, 3, RING, q, cw), F32),
            pltpu.VMEM((2, 3, RING, q, cw), F32),
            pltpu.VMEM((2, q, cw), F32),
            dma((3,)), dma((3, 2)), dma((2, 2)), dma((2,)), dma((8,)),
        ] + [dma((2, 3, RING))] * RING + [dma((2, 8))] * RING,
        compiler_params=pltpu.CompilerParams(collective_id=2, has_side_effects=True, vmem_limit_bytes=VMEM_LIMIT),
        cost_estimate=pl.CostEstimate(flops=flops, bytes_accessed=4 * tokens * d_model + 12 * f_loc * d_model, transcendentals=tokens * f_loc),
        name='ffn_ring',
    )(after_attn, wg_t, wu_t, w_down, gain, m_part)


def front_body(x_ref, wq, wk, wv, wo, eg, eu, ed, attn_gain, moe_gain, freq, ids, router,
               a_full, m_part, ctx_all, hid_all, ids_all, w_cols, og, ou, od,
               xn, ctxb, abuf, gate, idf,
               lsem, rawsem, cls, als, cs, cr, cfs, cfr, as_, ar, afs, afr, hs, hr, hfs, hfr, ws, wr, wxs, wxr, wfs, wfr,
               wds, wdr, ins, inr, es, er, csem, xsem, usem, wsem, dsem, msem):
    t = lax.axis_index('tp')
    e = lax.axis_index('ep')
    core = odd(e)
    xc = e // 2
    tokens, d_model = xn.shape
    heads, hd = wq.shape[1], wq.shape[2]
    q = tokens // RING
    half = q // 2
    width = d_model // RING
    kblk = min(512, d_model // RING)
    nk = d_model // kblk
    pair = 2 * hd
    pairs = heads // 2
    local, fe = eg.shape[0], eg.shape[1]
    top_k = ids.shape[0]
    partner = {'ep': xc * 2 + 1 - core}

    def ring(k):
        return lax.rem(k + RING, RING)

    def y_dev(k):
        return {'tp': ring(t + k)}

    def x_id(k):
        return ring(xc + k) * 2 + core

    def x_dev(k):
        return {'ep': x_id(k)}

    def w_swap(k):
        return rcopy(wo.at[window(e, hd), window(ring(t + k), width)], w_cols.at[e, t], ws.at[k - 1], wr.at[k - 1], y_dev(k))

    def w_round(side):
        return rcopy(w_cols.at[e], w_cols.at[e], wxs.at[side], wxr.at[side], x_dev(turn(side)))

    def w_forward(side):
        ref = w_cols.at[x_id(2 * side - 1), pl.ds(2 * side, 2)]
        return rcopy(ref, ref, wfs.at[side], wfr.at[side], x_dev(turn(side)))

    def w_core(k):
        return rcopy(w_cols.at[x_id(k)], w_cols.at[x_id(k)], wds.at[k], wdr.at[k], partner)

    def hid_send(part, side):
        return rcopy(hid_all.at[xc, part], hid_all.at[xc, part], hs.at[part, side], hr.at[part, side], x_dev(turn(side)))

    def hid_forward(part, side):
        ref = hid_all.at[ring(xc + 2 * side - 1), part, pl.ds(side * (half // 2), half // 2)]
        return rcopy(ref, ref, hfs.at[part, side], hfr.at[part, side], x_dev(turn(side)))

    def ids_send(k):
        return rcopy(ids.at[:, window(t, q)], ids_all.at[xc], ins.at[k - 1], inr.at[k - 1], x_dev(k))

    mats = ((eg, og), (eu, ou), (ed, od))

    def swap_mat(k, i):
        return rcopy(mats[i][0].at[k], mats[i][1].at[k], es.at[k, i], er.at[k, i], partner)

    def ctx_local(g):
        return pltpu.make_async_copy(ctxb.at[g], ctx_all.at[t, :, window(g, pair)], cls.at[g])

    def ctx_send(g, side):
        return rcopy(ctxb.at[g], ctx_all.at[t, :, window(g, pair)], cs.at[side, g], cr.at[side, g], y_dev(turn(side)))

    def ctx_forward(g, side):
        ref = ctx_all.at[ring(t + 2 * side - 1), pl.ds(side * (tokens // 2), tokens // 2), window(g, pair)]
        return rcopy(ref, ref, cfs.at[side, g], cfr.at[side, g], y_dev(turn(side)))

    def ctx_pass(g):
        for side in SIDES:
            ctx_send(g, side).wait_recv()
            ctx_forward(g, side).start()

    def a_local(c):
        return pltpu.make_async_copy(abuf.at[c], a_full.at[window(c, q), window(t, width)], als.at[c])

    def a_send(c, side):
        return rcopy(abuf.at[c], a_full.at[window(c, q), window(t, width)], as_.at[side, c], ar.at[side, c], y_dev(turn(side)))

    def a_forward(c, side):
        rows = pl.ds(pl.multiple_of(c * q + side * half, half), half)
        ref = a_full.at[rows, window(ring(t + 2 * side - 1), width)]
        return rcopy(ref, ref, afs.at[side, c], afr.at[side, c], y_dev(turn(side)))

    def a_pass(c):
        for side in SIDES:
            a_send(c, side).wait_recv()
            a_forward(c, side).start()

    load_x = [pltpu.make_async_copy(x_ref.at[pl.ds(k * q, q)], xn.at[pl.ds(k * q, q)], lsem.at[k]) for k in range(RING)]
    for c in load_x:
        c.start()
    w_own = pltpu.make_async_copy(wo.at[window(e, hd), window(t, width)], w_cols.at[e, t], lsem.at[RING])
    ids_own = pltpu.make_async_copy(ids.at[:, window(t, q)], ids_all.at[xc], lsem.at[RING + 1])

    def attention(rope, raw, wide, wide2, wb, qb, kb, vb, ub):
        proj = (wq, wk, wv)
        deep = raw.shape[0]
        share = tokens // nk
        step = min(16, share)

        def raw_load(m, k):
            slot = lax.rem(k, deep)
            return pltpu.make_async_copy(proj[m].at[window(k, kblk)], raw.at[slot], rawsem.at[slot])

        def rows_of(m, k):
            slot = lax.rem(k, deep)
            part = kblk // 2
            for i, buf in enumerate((wide, wide2)):
                buf[...] = raw[slot, i * part:(i + 1) * part].astype(F32).reshape(part * heads, hd)
            for i, buf in enumerate((wide, wide2)):
                rows = pl.ds(pl.multiple_of(k * kblk + i * part, part), part)
                for h in range(heads):
                    wb[m, rows, h * hd:(h + 1) * hd] = buf[pl.ds(h, part, stride=heads), :].astype(BF16)

        def raw_next(m, k):
            @pl.when(k + deep < nk)
            def _():
                raw_load(m, k + deep).start()

            if m + 1 < len(proj):
                @pl.when(k + deep >= nk)
                def _():
                    raw_load(m + 1, k + deep - nk).start()

        own = pltpu.make_async_copy(x_ref.at[window(t, q)], ub, lsem.at[RING + 2])
        own.start()
        for k in range(deep):
            raw_load(0, k).start()
        entry_barrier((y_dev(1), y_dev(-1), y_dev(2), x_dev(1), x_dev(-1), x_dev(2), partner))
        w_own.start()
        ids_own.start()
        for k in range(1, RING):
            w_swap(k).start()
            ids_send(k).start()
        for i in range(len(mats)):
            swap_mat(0, i).start()

        sign = jnp.where(lax.broadcasted_iota(jnp.int32, (1, hd), 1) < hd // 2, -1.0, 1.0)
        steps = min(128, tokens)

        def angles(k):
            angle = (lax.broadcasted_iota(jnp.int32, (steps, 1), 0) + k * steps).astype(F32) * freq[...]
            rope[0, window(k, steps)] = jnp.cos(angle)
            rope[1, window(k, steps)] = jnp.sin(angle) * sign
        loop(tokens // steps, angles)
        own.wait()
        norm_rows(ub, ub, moe_gain, q, 16)
        keep = [pltpu.make_async_copy(ub.at[pl.ds(part * half, half)], hid_all.at[xc, part], lsem.at[RING + 2 + part]) for part in SIDES]
        for c in keep:
            c.start()

        for c in keep:
            c.wait()
        for side in SIDES:
            hid_send(0, side).start()
        for k in range(RING):
            load_x[k].wait()

        for m in range(len(proj)):
            def one(k, m=m):
                raw_load(m, k).wait()
                rows_of(m, k)
                if m == 0:
                    for i in range(0, share, step):
                        rows = pl.ds(pl.multiple_of(k * share + i, step), step)
                        x = xn[rows, :].astype(F32)
                        inv = lax.rsqrt(jnp.mean(x * x, axis=-1, keepdims=True) + EPS)
                        xn[rows, :] = (x * inv * attn_gain[...].astype(F32).reshape(1, -1)).astype(BF16)
                raw_next(m, k)
            loop(nk, one)

        def turned(r):
            for h in SIDES:
                part = r[:, h * hd:(h + 1) * hd]
                yield (part * rope[0] + pltpu.roll(part, hd // 2, 1) * rope[1]).astype(BF16)

        def project(m, g):
            return jnp.dot(xn[...], wb[m, :, window(g, pair)], preferred_element_type=F32)

        w_own.wait()
        for k in range(1, RING):
            w_swap(k).wait_recv()
        for side in SIDES:
            w_round(side).start()
        w_core(0).start()

        scale = hd ** -0.5
        tri = lax.broadcasted_iota(jnp.int32, (q, q), 0) >= lax.broadcasted_iota(jnp.int32, (q, q), 1)

        def heads_of(g):
            for m, dst in enumerate((qb, kb)):
                for h, part in enumerate(turned(project(m, g))):
                    dst[:, h * hd:(h + 1) * hd] = part
            vb[...] = project(2, g).astype(BF16)
            for h in SIDES:
                hc = slice(h * hd, (h + 1) * hd)
                for b in range(RING):
                    s = lax.dot_general(qb[b * q:(b + 1) * q, hc], kb[0:(b + 1) * q, hc], NT, preferred_element_type=F32) * scale
                    diag = jnp.where(tri, s[:, b * q:], -1e30)
                    s = diag if b == 0 else jnp.concatenate([s[:, :b * q], diag], axis=1)
                    w = jnp.exp(s - jnp.max(s, axis=-1, keepdims=True))
                    prob = (w * (1.0 / jnp.sum(w, axis=-1, keepdims=True))).astype(BF16)
                    ctxb[g, b * q:(b + 1) * q, hc] = jnp.dot(prob, vb[0:(b + 1) * q, hc], preferred_element_type=F32).astype(BF16)
            ctx_local(g).start()
            for side in SIDES:
                ctx_send(g, side).start()

            @pl.when(g == 0)
            def _():
                for side in SIDES:
                    hid_send(0, side).wait_recv()
                    hid_forward(0, side).start()

            @pl.when(g >= 2)
            def _():
                ctx_pass(g - 2)

            @pl.when(g == 2)
            def _():
                for side in SIDES:
                    w_round(side).wait_recv()
                    w_forward(side).start()
                w_core(1).start()
                w_core(RING - 1).start()

            @pl.when(g == pairs - 1)
            def _():
                for side in SIDES:
                    hid_send(1, side).start()
        loop(pairs, heads_of)

    pl.run_scoped(attention, pltpu.VMEM((2, tokens, hd), F32), pltpu.VMEM((RING, kblk, heads, hd), BF16), *[pltpu.VMEM((kblk // 2 * heads, hd), F32)] * 2,
                  pltpu.VMEM((3, d_model, heads * hd), BF16), *[pltpu.VMEM((tokens, pair), BF16)] * 3, pltpu.VMEM((q, d_model), BF16))

    fb = 256 if fe > 512 else 128
    cw = min(512, d_model // 4)

    def experts(wcv, cbuf, mv, act, wbuf, dbuf):
        sizes = [fb] * (fe // fb) + [fe % fb]
        cw = mv.shape[-1]
        nn = d_model // cw
        each = 2 * local
        passes = 2 * each

        def expert_of(p):
            return lax.rem(p, each)

        def w_load(k, own):
            k = k if own else k - local
            return [pltpu.make_async_copy(ref.at[k], wbuf.at[i], wsem.at[i]) for i, ref in enumerate((eg, eu) if own else (og, ou))]

        def d_load(k, own):
            return [pltpu.make_async_copy((ed if own else od).at[k if own else k - local], dbuf, dsem.at[0])]

        def start(p, load):
            k = expert_of(p)

            @pl.when(jnp.logical_and(p < passes, k < local))
            def _():
                for c in load(k, True):
                    c.start()

            @pl.when(jnp.logical_and(p < passes, k >= local))
            def _():
                for c in load(k, False):
                    c.start()

        def u_rows(part, k):
            return xn.at[pl.ds(pl.multiple_of((part * RING + k) * half, half), half)]

        def u_load(part, k):
            return pltpu.make_async_copy(hid_all.at[k, part], u_rows(part, k), usem.at[k])

        def u_start(part):
            for side in SIDES:
                hid_forward(part, side).wait_recv()
            for k in range(RING):
                u_load(part, k).start()

        def u_ready(part):
            for k in range(RING):
                u_load(part, k).wait()
            rows = RING * half
            u = xn.at[pl.ds(part * rows, rows)]
            logits = lax.dot_general(u[...], router[...], NT, preferred_element_type=F32)
            lane = lax.broadcasted_iota(jnp.int32, logits.shape, 1).astype(F32)
            picks = jnp.concatenate([idf[k, :, part * half:(part + 1) * half].astype(F32) for k in range(RING)], axis=1).T
            chosen = lane == picks[:, 0:1]
            for j in range(1, top_k):
                chosen = jnp.logical_or(chosen, lane == picks[:, j:j + 1])
            top = jnp.max(jnp.where(chosen, logits, -jnp.inf), axis=-1, keepdims=True)
            w = jnp.where(chosen, jnp.exp(jnp.where(chosen, logits - top, 0.0)), 0.0)
            gate[part] = w / jnp.sum(w, axis=-1, keepdims=True)

        def ctx_load(c):
            return [pltpu.make_async_copy(ctx_all.at[k, window(c, q)], cbuf.at[odd(c), :, pl.ds(k * heads * hd, heads * hd)], csem.at[odd(c), k]) for k in range(RING)]

        def x_load(c):
            return pltpu.make_async_copy(x_ref.at[window(c, q), window(t, width)], abuf.at[c], xsem.at[odd(c)])

        load_w = [pltpu.make_async_copy(w_cols.at[:, k], wcv.at[k], lsem.at[k]) for k in range(RING)]

        def attention_out():
            for side in SIDES:
                for g in range(pairs):
                    ctx_forward(g, side).wait_recv()
            for g in range(pairs):
                ctx_local(g).wait()
            for c in ctx_load(jnp.int32(0)):
                c.start()
            x_load(jnp.int32(0)).start()
            for c in load_w:
                c.wait()

            def chunk(c):
                @pl.when(c + 1 < RING)
                def _():
                    for d in ctx_load(c + 1):
                        d.start()
                    x_load(c + 1).start()
                for d in ctx_load(c):
                    d.wait()
                x_load(c).wait()
                o = jnp.dot(cbuf[odd(c)], wcv[...].reshape(RING * heads * hd, width), preferred_element_type=F32)
                abuf[c] = (abuf[c].astype(F32) + o).astype(BF16)
                a_local(c).start()
                for side in SIDES:
                    a_send(c, side).start()
            loop(RING, chunk)

        def m_out(part, n):
            return pltpu.make_async_copy(mv.at[part, n], m_part.at[:, part, :, window(n, cw)], msem.at[part, n])

        start(jnp.int32(0), w_load)
        ids_own.wait()
        for k in range(1, RING):
            ids_send(k).wait_recv()
        load_i = pltpu.make_async_copy(ids_all, idf.at[:, pl.ds(0, top_k)], lsem.at[RING + 1])
        load_i.start()
        u_start(0)
        for i in SIDES:
            swap_mat(1, i).start()
        load_i.wait()
        u_ready(0)

        def one_pass(p):
            @pl.when(p == 1)
            def _():
                ctx_pass(pairs - 2)
                for side in SIDES:
                    w_forward(side).wait_recv()
                w_core(2).start()
                swap_mat(1, 2).start()

            @pl.when(p == 2)
            def _():
                for k in range(RING):
                    w_core(k).wait_recv()
                for c in load_w:
                    c.start()

            @pl.when(p == 3)
            def _():
                ctx_pass(pairs - 1)
                for side in SIDES:
                    hid_send(1, side).wait_recv()
                    hid_forward(1, side).start()
                attention_out()
                u_start(1)

            @pl.when(p == each)
            def _():
                u_ready(1)

            @pl.when(p >= RING)
            def _():
                a_pass(p - RING)
            k, part = expert_of(p), p // each
            which = (k // local) * ((e + 1 - 2 * core) * local + k - local) + (1 - k // local) * (e * local + k)
            rows = RING * half
            u = xn.at[pl.ds(pl.multiple_of(part * rows, rows), rows)]
            lane = lax.broadcasted_iota(jnp.int32, gate.shape[1:], 1)
            weight = jnp.sum(jnp.where(lane == which, gate[part], 0.0), axis=1, keepdims=True)

            def if_new(ahead, which_mats):
                for late, when in enumerate((3, 4)):
                    @pl.when(ahead == when)
                    def _():
                        for i in which_mats:
                            swap_mat(late, i).wait_recv()
            if_new(p + 1, (2,))
            start(p, d_load)
            for c in w_load(0, True):
                c.wait()
            for b, size in enumerate(sizes):
                cols = slice(b * fb, b * fb + size)
                g = lax.dot_general(u[...], wbuf[0, cols], NT, preferred_element_type=F32)
                v = lax.dot_general(u[...], wbuf[1, cols], NT, preferred_element_type=F32)
                act[:, cols] = (jax.nn.silu(g) * v).astype(BF16)
            if_new(p + 2, SIDES)
            start(p + 1, w_load)
            for c in d_load(0, True):
                c.wait()
            for n in range(nn):
                y = jnp.dot(act[...], dbuf[:, n * cw:(n + 1) * cw], preferred_element_type=F32).astype(BF16)
                term = jnp.where(weight > 0.0, weight * y.astype(F32), 0.0).reshape(mv.shape[2:])
                mv[part, n] = jnp.where(k == 0, term, mv[part, n] + term)

            @pl.when(k == each - 1)
            def _():
                loop(nn, lambda n: m_out(part, n).start())
        loop(passes, one_pass)

        def finish(n):
            for part in SIDES:
                m_out(part, n).wait()
        loop(nn, finish)

    pl.run_scoped(experts, pltpu.VMEM((RING, 8, hd, width), BF16), pltpu.VMEM((2, q, RING * heads * hd), BF16),
                  pltpu.VMEM((2, d_model // cw, RING, half, cw), F32), pltpu.VMEM((RING * half, fe), BF16),
                  pltpu.VMEM((2, fe, d_model), BF16), pltpu.VMEM((fe, d_model), BF16))

    for side in SIDES:
        w_round(side).wait_send()
        w_forward(side).wait_send()
        for part in SIDES:
            hid_send(part, side).wait_send()
            hid_forward(part, side).wait_send()
        for g in range(pairs):
            ctx_send(g, side).wait_send()
            ctx_forward(g, side).wait_send()
        for c in range(RING):
            a_send(c, side).wait_send()
            a_forward(c, side).wait()
    for k in range(1, RING):
        w_swap(k).wait_send()
        ids_send(k).wait_send()
    for k in SIDES:
        for i in range(len(mats)):
            swap_mat(k, i).wait_send()
    for k in range(RING):
        w_core(k).wait_send()
        a_local(k).wait()


def front_call(x, wq, wk, wv, wo, eg, eu, ed, attn_gain, moe_gain, ids, router):
    tokens, d_model = x.shape
    heads, hd = wq.shape[1], wq.shape[2]
    q = tokens // RING
    local, fe = eg.shape[0], eg.shape[1]
    experts = router.shape[0]
    pairs = heads // 2
    hbm = pl.BlockSpec(memory_space=pl.ANY)
    vmem = pl.BlockSpec(memory_space=pltpu.VMEM)
    dma = pltpu.SemaphoreType.DMA
    sds = jax.ShapeDtypeStruct
    freq = ROPE_BASE ** (np.arange(hd) % (hd // 2) * (-2.0 / hd))
    freq = jnp.asarray(freq.astype(np.float32).reshape(1, hd))
    two, three, four = dma((2,)), dma((3,)), dma((RING,))
    by_pair, by_chunk, square = dma((2, pairs)), dma((2, RING)), dma((2, 2))
    outs = pl.pallas_call(
        front_body,
        out_shape=(sds((tokens, d_model), BF16), sds((RING, 2, q // 2, d_model), F32), sds((RING, tokens, heads * hd), BF16),
                   sds((RING, 2, q // 2, d_model), BF16), sds((RING, ids.shape[0], q), ids.dtype), sds((8, RING, hd, d_model // RING), BF16),
                   sds(eg.shape, BF16), sds(eu.shape, BF16), sds(ed.shape, BF16)),
        in_specs=[hbm] * 8 + [vmem] * 3 + [hbm, vmem],
        out_specs=(hbm,) * 9,
        scratch_shapes=[
            pltpu.VMEM((tokens, d_model), BF16), pltpu.VMEM((pairs, tokens, 2 * hd), BF16), pltpu.VMEM((RING, q, d_model // RING), BF16),
            pltpu.VMEM((2, tokens // 2, experts), F32), pltpu.VMEM((RING, 8, q), ids.dtype),
            dma((RING + RING,)), four, dma((pairs,)), four,
        ] + [by_pair] * RING + [by_chunk] * RING + [square] * RING + [three] * 2 + [two] * RING + [four] * 2 + [three] * 2
          + [dma((2, 3))] * 2 + [by_chunk, two, four, two, two, dma((2, 8))],
        compiler_params=pltpu.CompilerParams(collective_id=0, has_side_effects=True, vmem_limit_bytes=VMEM_LIMIT),
        cost_estimate=pl.CostEstimate(flops=2 * tokens * d_model * (heads * hd * RING + 12 * fe), bytes_accessed=24 * fe * d_model, transcendentals=heads * tokens * tokens),
        name='attn_moe',
    )(x, wq, wk, wv, wo, eg, eu, ed, attn_gain, moe_gain, freq, ids, router)
    return outs[0], outs[1]


def solution(mesh):
    tok_spec = P(('dp', 'ep'))
    col_spec = P(None, 'tp')
    in_specs = (tok_spec,) * 3 + (P(),) + (col_spec,) * 3 + (P('tp'), P(), col_spec, col_spec, P('tp'), P(), P()) + (P('ep'),) * 3

    def layer_local(hidden_in, expert_ids, slot_ids, attn_gain, w_query, w_key, w_value, w_out, ffn_gain, w_gate, w_up, w_down, moe_gain, w_router, exp_gate, exp_up, exp_down):
        num_seqs, seq_len, d_model = hidden_in.shape
        tokens = num_seqs * seq_len
        heads, head_dim = w_out.shape[0], w_out.shape[1]
        x = hidden_in.reshape(tokens, d_model)
        ids = jnp.swapaxes(expert_ids, 1, 2).reshape(expert_ids.shape[2], tokens)
        after_attn, m_part = front_call(
            x, w_query, w_key, w_value, w_out.reshape(heads * head_dim, d_model), jnp.swapaxes(exp_gate, 1, 2), jnp.swapaxes(exp_up, 1, 2), exp_down,
            attn_gain, moe_gain, ids, w_router.T)
        out = ffn_call(after_attn, w_gate.T, w_up.T, w_down, ffn_gain, m_part.reshape(-1, tokens // 4, d_model))
        return out.reshape(hidden_in.shape)

    return jax.shard_map(layer_local, mesh=mesh, in_specs=in_specs, out_specs=tok_spec, check_vma=False)
```
